128 devices in a mesh: dp: 32 (over x_lo, z, y), tr: 2 (over core), tc: 2 (over x_hi).
Axes of the slice: x: 4 (x_hi: 2, x_lo: 2; x = x_hi * 2 + x_lo), y: 4, z: 4, core: 2. Of those that a mesh axis runs over, the one named last changes fastest.
Arguments:
- activations: bfloat16 [16384, 4096], P('dp', ('tr', 'tc')), may hold values from -16.8 to 16.8, as said below
- gradients: bfloat16 [16384, 7168], P('dp', ('tr', 'tc')), may hold values from -16.8 to 16.8, as said below
- old_inputs: float32 [4096, 4096], P(('dp', 'tr', 'tc')), may hold values from -3 to 3
- old_gradients: float32 [7168, 7168], P(('dp', 'tr', 'tc')), may hold values from -3 to 3
Outputs:
- input_factor: float32 [4096, 4096], P(('dp', 'tr', 'tc'))
- grad_factor: float32 [7168, 7168], P(('dp', 'tr', 'tc'))
The draws below stay inside these ranges and needn't reach their ends.
Inputs may be any that keep to these rules, and one draw needn't show every extreme that they name: `activations`: real-valued samples. `gradients`: real-valued samples.
All inputs are finite; a program needn't handle non-finite values.
Results may differ from the reference program's by a relative error of at most 0.0045.
Values may be sent and summed in bfloat16 or wider, within the bound.
A program may use at most 192 MiB of HBM per device.

```python
import jax
import jax.numpy as jnp
from jax import lax

D = 4096
FF = 7168
TOK_DEV = 512
N_DP = 32


def spiked(key, width):
    first = jax.random.fold_in(key, 0)
    third = jax.random.fold_in(key, 2)
    rows_total = TOK_DEV * N_DP
    base = jnp.clip(jax.random.normal(first, (rows_total, width), jnp.float32), -6.0, 6.0)
    pairing = jax.random.permutation(third, N_DP).astype(jnp.int32)
    replica = jnp.arange(rows_total, dtype=jnp.int32) // TOK_DEV
    block = jnp.arange(width, dtype=jnp.int32) // (width // N_DP)
    target = jnp.take(pairing, replica)
    boost = jnp.where(target[:, None] == block[None, :], 2.0, 1.0)
    return (base * boost).astype(jnp.bfloat16)


def draw_activations(key, part):
    return spiked(jax.random.fold_in(key, 11), D)


def draw_gradients(key, part):
    return spiked(jax.random.fold_in(key, 23), FF)


def levels(key, dims, cuts, low, largest):
    factor_of, own = 1.0, jax.random.fold_in(key, 6)
    for axis_at, blocks in cuts:
        heights = jnp.exp(jax.random.uniform(jax.random.fold_in(own, axis_at), (blocks,), jnp.float32, low / len(cuts), largest / len(cuts)))
        factor_of = factor_of * jnp.repeat(heights, dims[axis_at] // blocks).reshape([-1 if axis == axis_at else 1 for axis in range(len(dims))])
    return factor_of


def bell_draw(own_key, shape, scale, most, cuts=(), kind=jnp.bfloat16):
    entries = scale * jax.random.normal(own_key, shape, jnp.float32)
    if cuts:
        entries = entries * levels(own_key, shape, cuts, -0.22, 0.18)
    return jnp.clip(entries, -most, most).astype(kind)


def setup_inputs(seed: int = 0) -> dict:
    key_list = jax.random.split(jax.random.key(seed), 5)
    activations = draw_activations(jax.random.fold_in(key_list[4], 71), 0)
    gradients = draw_gradients(jax.random.fold_in(key_list[4], 71), 0)
    old_inputs = bell_draw(key_list[2], (D, D), 0.5, 3.0, ((0, 128),), jnp.float32)
    old_gradients = bell_draw(key_list[3], (FF, FF), 0.5, 3.0, ((0, 128),), jnp.float32)
    return {"activations": activations, "gradients": gradients, "old_inputs": old_inputs, "old_gradients": old_gradients}


def replica_sum(samples, tokens_all):
    columns = samples.shape[1]
    replicas = samples.reshape(N_DP, TOK_DEV, columns)

    def accumulate(running, replica_rows):
        partial_value = (jnp.dot(replica_rows.T, replica_rows, preferred_element_type=jnp.float32) / tokens_all).astype(jnp.bfloat16)
        return running + partial_value.astype(jnp.float32), None

    running, _ = lax.scan(accumulate, jnp.zeros((columns, columns), jnp.float32), replicas)
    return running


def reference(activations, gradients, old_inputs, old_gradients):
    tokens_all = N_DP * TOK_DEV
    input_new = replica_sum(activations, tokens_all)
    gradient_new = replica_sum(gradients, tokens_all)
    return (0.5 * old_inputs + 0.5 * input_new, 0.5 * old_gradients + 0.5 * gradient_new)
```

```python
import functools

import jax
import jax.numpy as jnp
from jax import lax
from jax.experimental import pallas as pl
from jax.experimental.pallas import tpu as pltpu
from jax.sharding import Mesh
from jax.sharding import PartitionSpec as P

MESH = pl.DeviceIdType.MESH
DP = ("dp_0", "dp_1", "dp_2")
DP_TR_TC = ("dp_0", "dp_1", "dp_2", "tr", "tc")
AXES = DP_TR_TC

ACT, GRAD = 0, 1
PIECES = (
    (ACT, 0, 512, 0),
    (ACT, 512, 512, 1),
    (GRAD, 0, 512, 0),
    (GRAD, 512, 384, 0),
    (GRAD, 896, 512, 1),
    (GRAD, 1408, 384, 1),
)


def pieces_of(m, half):
    return [i for i, p in enumerate(PIECES) if p[0] == m and p[3] == half]


def kernel(
    act, grad, out_a, out_g,
    buf_a, buf_g, prod_a, prod_g, recv_a, recv_g, fin_a, fin_g,
    own_sem, a_send, a_recv, b_send, b_recv, d_send, d_recv,
    s_send, s_recv, f_send, f_recv, o_sem,
):
    h = lax.axis_index("dp_0")
    z = lax.axis_index("dp_1")
    y = lax.axis_index("dp_2")
    tr = lax.axis_index("tr")
    tc = lax.axis_index("tc")
    is_n = (tr + h) % 2

    src = (act, grad)
    out = (out_a, out_g)
    buf = (buf_a, buf_g)
    prod = (prod_a, prod_g)
    recv = (recv_a, recv_g)
    fin = (fin_a, fin_g)

    def flip1(v):
        return v + 1 - 2 * (v % 2)

    def flip3(v):
        return 3 - v

    x1 = (1 - h, z, y, tr, tc)
    x3 = (1 - h, z, y, tr, 1 - tc)
    core = (h, z, y, 1 - tr, tc)
    others = ((h, z, y, tr, 1 - tc), core, (h, z, y, 1 - tr, 1 - tc))

    def partner(d):
        f = flip1 if d % 2 == 0 else flip3
        on_y = (1 - tr) if d < 2 else tr
        return (
            h,
            on_y * z + (1 - on_y) * f(z),
            on_y * f(y) + (1 - on_y) * y,
            tr,
            tc,
        )

    barrier = pltpu.get_barrier_semaphore()
    peers = [x1, x3, *others, *(partner(d) for d in range(4))]
    for peer in peers:
        pl.semaphore_signal(barrier, inc=1, device_id=peer, device_id_type=MESH)

    own = [pltpu.make_async_copy(src[m], buf[m].at[0], own_sem.at[m]) for m in (ACT, GRAD)]
    for copy in own:
        copy.start()
    pl.semaphore_wait(barrier, len(peers))

    def cols(i):
        return pl.ds(PIECES[i][1], PIECES[i][2])

    def remote(a, b, ss, rs, to):
        return pltpu.make_async_remote_copy(
            src_ref=a, dst_ref=b, send_sem=ss, recv_sem=rs, device_id=to, device_id_type=MESH
        )

    def along_a(i):
        m = PIECES[i][0]
        return remote(
            src[m].at[:, cols(i)], buf[m].at[1, :, cols(i)], a_send.at[i], a_recv.at[i], x1
        )

    def along_b(k, i):
        m = PIECES[i][0]
        source = src[m].at[:, cols(i)] if k == 0 else buf[m].at[1, :, cols(i)]
        return remote(
            source, buf[m].at[3 - k, :, cols(i)], b_send.at[k, i], b_recv.at[k, i], x3
        )

    def to_core(k, i):
        m = PIECES[i][0]
        source = src[m].at[:, cols(i)] if k == 0 else buf[m].at[k, :, cols(i)]
        slot = k + 4 if k < 2 else k
        return remote(
            source, buf[m].at[slot, :, cols(i)], d_send.at[k, i], d_recv.at[k, i], core
        )

    every = range(len(PIECES))
    for i in every:
        along_a(i).start()

    @pl.when(is_n == 1)
    def _():
        for i in every:
            along_b(0, i).start()

    @pl.when(is_n == 0)
    def _():
        for i in every:
            to_core(0, i).start()

    def step_a(m, half):
        for i in pieces_of(m, half):
            along_a(i).wait_recv()

            @pl.when(is_n == 1)
            def _(i=i):
                along_b(1, i).start()

            @pl.when(is_n == 0)
            def _(i=i):
                to_core(1, i).start()

        @pl.when(is_n == 1)
        def _():
            for i in pieces_of(m, half):
                to_core(0, i).wait_recv()
                to_core(1, i).wait_recv()

    def step_b(m, half):
        @pl.when(is_n == 0)
        def _():
            for i in pieces_of(m, half):
                along_b(0, i).wait_recv()
                to_core(3, i).start()
            for i in pieces_of(m, half):
                along_b(1, i).wait_recv()
                to_core(2, i).start()

        @pl.when(is_n == 1)
        def _():
            for i in pieces_of(m, half):
                to_core(3, i).wait_recv()
                to_core(2, i).wait_recv()

    zb = z // 2
    za = (z + zb) % 2
    yb = y // 2
    ya = (y + yb) % 2

    def weight(d0, d1, s):
        w = [[2 ** ((d - k) % 4) for k in (0, 1)] for d in (d0, d1)]
        on0 = w[0][0] + s * (w[0][1] - w[0][0])
        on1 = w[1][0] + s * (w[1][1] - w[1][0])
        return on0 + tr * (on1 - on0)

    def first_partner(s):
        def f(v):
            return (1 - s) * flip1(v) + s * flip3(v)

        return (h, (1 - tr) * z + tr * f(z), (1 - tr) * f(y) + tr * y, tr, tc)

    def stream_copy(m, s, q, to):
        return remote(
            prod[m].at[s, q], recv[m].at[s, q], s_send.at[m, s, q], s_recv.at[m, s, q], to
        )

    def product(m, e, c, s):
        half = buf[m].shape[2] // 2
        rows = half // 4
        tokens = 2 * buf[m].shape[1]
        base = e * 2 + (1 - e) * 4 * is_n
        left = buf[m][pl.ds(base, 2), :, pl.ds(pl.multiple_of(c * half, 128), half)]
        right = buf[m][pl.ds(0, 2), :, pl.ds(pl.multiple_of(s * half, 128), half)]
        value = lax.dot_general(
            left.reshape(tokens, half),
            right.reshape(tokens, half),
            (((0,), (0,)), ((), ())),
            preferred_element_type=jnp.float32,
        )
        block = (tc + e) % 2
        rza = (c + block + za) % 2
        rzb = (block + zb) % 2
        zq = rza * weight(2, 0, s) + rzb * weight(3, 1, s)
        for yy in range(4):
            rya = ((yy ^ (yy >> 1)) % 2 + ya) % 2
            ryb = (yy // 2 + yb) % 2
            q = zq + rya * weight(0, 2, s) + ryb * weight(1, 3, s)
            prod[m][s, q] = value[yy * rows : (yy + 1) * rows].astype(jnp.bfloat16)

            @pl.when(q % 2 == 1)
            def _(q=q):
                stream_copy(m, s, q, first_partner(s)).start()

    def arrived(m, s, q):
        stream_copy(m, s, q, core).wait_recv()

    def total(m, s, q, parts):
        value = prod[m][s, q].astype(jnp.float32)
        for p in parts:
            value = value + recv[m][s, p].astype(jnp.float32)
        return value

    def stage(m, s, k):
        to = partner((k + s) % 4)

        def one(i, carry):
            q = i * 2 ** (k + 1) + 2**k
            parts = [q + 2**j for j in range(k)]
            for p in parts:
                arrived(m, s, p)
            prod[m][s, q] = total(m, s, q, parts).astype(jnp.bfloat16)
            stream_copy(m, s, q, to).start()
            return carry

        lax.fori_loop(0, 2 ** (3 - k), one, 0)

    def place(m, s):
        width = buf[m].shape[2]
        half = width // 2
        first = pl.multiple_of((2 * tr + tc) * width + s * half, 128)
        return out[m].at[:, pl.ds(first, half)]

    def last_copy(m, s, k):
        half = buf[m].shape[2] // 2
        to = others[k]
        return remote(
            fin[m].at[2 * to[3] + to[4], :, pl.ds(s * half, half)],
            place(m, s),
            f_send.at[m, s, k],
            f_recv.at[m, s, k],
            to,
        )

    def own_copy(m, s):
        half = buf[m].shape[2] // 2
        return pltpu.make_async_copy(
            fin[m].at[2 * tr + tc, :, pl.ds(s * half, half)], place(m, s), o_sem.at[m, s]
        )

    def finish(m, s):
        parts = [1, 2, 4, 8]
        for p in parts:
            arrived(m, s, p)
        half = buf[m].shape[2] // 2
        rows = half // 16
        value = total(m, s, 0, parts)
        for k in range(4):
            fin[m][k, :, pl.ds(s * half, half)] = value[k * rows : (k + 1) * rows].astype(
                jnp.bfloat16
            )
        for k in range(3):
            last_copy(m, s, k).start()
        own_copy(m, s).start()

    def loop(m, first, last, which):
        def one(j, carry):
            product(m, *which(j))
            return carry

        lax.fori_loop(first, last, one, 0)

    for copy in own:
        copy.wait()

    def products_a(m):
        step_a(m, 0)
        step_a(m, 1)
        loop(m, 0, 4, lambda j: (0, j % 2, j // 2))

    def products_b(m):
        step_b(m, 0)
        step_b(m, 1)
        loop(m, 0, 4, lambda j: (1, j // 2, j % 2))

    products_a(ACT)
    products_b(ACT)
    step_a(GRAD, 0)
    for k in (1, 2):
        for s in (0, 1):
            stage(ACT, s, k)
    step_a(GRAD, 1)
    loop(GRAD, 0, 4, lambda j: (0, j % 2, j // 2))
    for s in (0, 1):
        stage(ACT, s, 3)
    for s in (0, 1):
        finish(ACT, s)
    products_b(GRAD)
    for k in (1, 2, 3):
        for s in (0, 1):
            stage(GRAD, s, k)
    for s in (0, 1):
        finish(GRAD, s)

    for i in every:
        along_a(i).wait_send()

    @pl.when(is_n == 1)
    def _():
        for i in every:
            for k in (0, 1):
                along_b(k, i).wait_send()

    @pl.when(is_n == 0)
    def _():
        for i in every:
            for k in range(4):
                to_core(k, i).wait_send()

    for m in (ACT, GRAD):
        for s in (0, 1):
            for q in range(1, 16):
                stream_copy(m, s, q, core).wait_send()
            own_copy(m, s).wait()
            for k in range(3):
                last_copy(m, s, k).wait()


def sums(activations, gradients, rows_a, rows_g):
    tokens = activations.shape[0]
    wide = (activations.shape[1], gradients.shape[1])
    rows = (rows_a, rows_g)
    bf16 = jnp.bfloat16
    vmem = [
        *(pltpu.VMEM((6, tokens, w), bf16) for w in wide),
        *(pltpu.VMEM((2, 16, w // 8, w // 2), bf16) for w in wide),
        *(pltpu.VMEM((2, 16, w // 8, w // 2), bf16) for w in wide),
        *(pltpu.VMEM((4, r, w), bf16) for r, w in zip(rows, wide)),
    ]
    n = len(PIECES)
    dma = pltpu.SemaphoreType.DMA
    sems = [
        dma((2,)), dma((n,)), dma((n,)), dma((2, n)), dma((2, n)), dma((4, n)), dma((4, n)),
        dma((2, 2, 16)), dma((2, 2, 16)), dma((2, 2, 3)), dma((2, 2, 3)), dma((2, 2)),
    ]
    anywhere = pl.BlockSpec(memory_space=pl.ANY)
    return pl.pallas_call(
        kernel,
        out_shape=[jax.ShapeDtypeStruct((r, 4 * w), bf16) for r, w in zip(rows, wide)],
        in_specs=[anywhere] * 2,
        out_specs=[anywhere] * 2,
        scratch_shapes=[*vmem, *sems],
        compiler_params=pltpu.CompilerParams(
            collective_id=0, has_side_effects=True, vmem_limit_bytes=66_000_000
        ),
    )(activations, gradients)


def body(activations, gradients, old_inputs, old_gradients):
    tokens_all = activations.shape[0] * lax.axis_size(DP)
    sum_a, sum_g = sums(activations, gradients, old_inputs.shape[0], old_gradients.shape[0])
    scale = 0.5 / tokens_all
    return (
        0.5 * old_inputs + scale * sum_a.astype(jnp.float32),
        0.5 * old_gradients + scale * sum_g.astype(jnp.float32),
    )


def solution(mesh):
    finer = Mesh(mesh.devices.reshape(2, 4, 4, mesh.shape["tr"], mesh.shape["tc"]), AXES)
    return jax.shard_map(
        body,
        mesh=finer,
        in_specs=(P(DP, ("tr", "tc")), P(DP, ("tr", "tc")), P(DP_TR_TC, None), P(DP_TR_TC, None)),
        out_specs=(P(DP_TR_TC, None), P(DP_TR_TC, None)),
        check_vma=False,
    )
```

```python
import functools

import jax
import jax.numpy as jnp
from jax import lax
from jax.experimental import pallas as pl
from jax.experimental.pallas import tpu as pltpu
from jax.sharding import Mesh
from jax.sharding import PartitionSpec as P

MESH = pl.DeviceIdType.MESH
DP = ("dp_0", "dp_1", "dp_2")
DP_TR_TC = ("dp_0", "dp_1", "dp_2", "tr", "tc")
AXES = DP_TR_TC

ACT, GRAD = 0, 1
PIECES = (
    (GRAD, 0, 512, 0),
    (GRAD, 512, 384, 0),
    (GRAD, 896, 512, 1),
    (GRAD, 1408, 384, 1),
    (ACT, 0, 512, 0),
    (ACT, 512, 512, 1),
)
EARLY = 3


def pieces_of(m, half):
    return [i for i, p in enumerate(PIECES) if p[0] == m and p[3] == half]


def scoped(name, f):
    def g(*a):
        with jax.named_scope(name + "#" + "_".join(str(x) for x in a if isinstance(x, int))):
            return f(*a)

    return g


def kernel(
    act, grad, out_a, out_g,
    buf_a, buf_g, prod_a, prod_g, recv_a, recv_g, prox_a, prox_g, recx_a, recx_g,
    fin_a, fin_g, finx_a, finx_g, turn_a, turn_g, mir_a, mir_g, row_a, row_g,
    own_sem, a_send, a_recv, b_send, b_recv, d_send, d_recv,
    s_send, s_recv, x_send, x_recv, f_send, f_recv, g_send, g_recv, m_send, m_recv, o_sem,
):
    h = lax.axis_index("dp_0")
    z = lax.axis_index("dp_1")
    y = lax.axis_index("dp_2")
    tr = lax.axis_index("tr")
    tc = lax.axis_index("tc")
    is_n = (tr + h) % 2

    src = (act, grad)
    out = (out_a, out_g)
    buf = (buf_a, buf_g)
    prod = (prod_a, prod_g)
    recv = (recv_a, recv_g)
    prox = (prox_a, prox_g)
    recx = (recx_a, recx_g)
    fin = (fin_a, fin_g)
    finx = (finx_a, finx_g)
    turn = (turn_a, turn_g)
    mir = (mir_a, mir_g)
    row = (row_a, row_g)

    def flip1(v):
        return v + 1 - 2 * (v % 2)

    def flip3(v):
        return 3 - v

    x1 = (1 - h, z, y, tr, tc)
    x3 = (1 - h, z, y, tr, 1 - tc)
    core = (h, z, y, 1 - tr, tc)
    others = ((h, z, y, tr, 1 - tc), core, (h, z, y, 1 - tr, 1 - tc))
    y_a, y_b = (h, z, flip1(y), tr, tc), (h, z, flip3(y), tr, tc)
    z_a, z_b = (h, flip1(z), y, tr, tc), (h, flip3(z), y, tr, tc)

    def partner(d):
        f = flip1 if d % 2 == 0 else flip3
        on_y = (1 - tr) if d < 2 else tr
        return (
            h,
            on_y * z + (1 - on_y) * f(z),
            on_y * f(y) + (1 - on_y) * y,
            tr,
            tc,
        )

    half_z = z // 2
    c_mine = z % 2
    apart = (half_z + tc) % 2
    side = (c_mine + apart * tc + (1 - apart) * is_n * h) % 2
    mirrors = 1 - (1 - is_n) * (1 - apart)
    kind = is_n * (1 + apart)
    turned_rows = (
        4 * h + 2 * (1 - half_z) + (c_mine + half_z) % 2,
        4 * (1 - h) + 2 * half_z + (c_mine + 1 - h) % 2,
        4 * (1 - h) + 2 * (1 - half_z) + (c_mine + half_z) % 2,
    )

    def quarters():
        for yy in range(4):
            for aa in range(2):
                for bb in range(2):
                    yield yy * 4 + aa * 2 + bb, (tr, 2 * tc + side, yy, aa, bb)

    barrier = pltpu.get_barrier_semaphore()
    peers = [x1, x3, *others, y_a, y_b, z_a, z_b]

    def greet(peer):
        pl.semaphore_signal(barrier, inc=1, device_id=peer, device_id_type=MESH)

    for peer in peers:
        greet(peer)
    for chunk in turned_rows:
        for yy in range(4):
            greet((chunk // 4, chunk % 4, yy, h, half_z))

    own = [pltpu.make_async_copy(src[m], buf[m].at[0], own_sem.at[m]) for m in (ACT, GRAD)]
    for copy in own:
        copy.start()
    pl.semaphore_wait(barrier, len(peers) + 16 * mirrors)

    def cols(i):
        return pl.ds(PIECES[i][1], PIECES[i][2])

    def remote(a, b, ss, rs, to):
        return pltpu.make_async_remote_copy(
            src_ref=a, dst_ref=b, send_sem=ss, recv_sem=rs, device_id=to, device_id_type=MESH
        )

    def along_a(i):
        m = PIECES[i][0]
        return remote(
            src[m].at[:, cols(i)], buf[m].at[1, :, cols(i)], a_send.at[i], a_recv.at[i], x1
        )

    def along_b(k, i):
        m = PIECES[i][0]
        source = src[m].at[:, cols(i)] if k == 0 else buf[m].at[1, :, cols(i)]
        return remote(
            source, buf[m].at[3 - k, :, cols(i)], b_send.at[k, i], b_recv.at[k, i], x3
        )

    def to_core(k, i):
        m = PIECES[i][0]
        source = src[m].at[:, cols(i)] if k == 0 else buf[m].at[k, :, cols(i)]
        slot = k + 4 if k < 2 else k
        return remote(
            source, buf[m].at[slot, :, cols(i)], d_send.at[k, i], d_recv.at[k, i], core
        )

    every = range(len(PIECES))
    for i in every:
        along_a(i).start()

    @pl.when(is_n == 1)
    def _():
        for i in range(EARLY):
            along_b(0, i).start()

    @pl.when(is_n == 0)
    def _():
        for i in every:
            to_core(0, i).start()

    def step_a(m, half):
        for i in pieces_of(m, half):
            along_a(i).wait_recv()

            @pl.when(is_n == 1)
            def _(i=i):
                along_b(1, i).start()
                if 1 <= i and i + EARLY - 1 in every:
                    along_b(0, i + EARLY - 1).start()

            @pl.when(is_n == 0)
            def _(i=i):
                to_core(1, i).start()

        @pl.when(is_n == 1)
        def _():
            for i in pieces_of(m, half):
                to_core(0, i).wait_recv()
                to_core(1, i).wait_recv()

    def step_b(m, half):
        @pl.when(is_n == 0)
        def _():
            for i in pieces_of(m, half):
                along_b(0, i).wait_recv()
                to_core(3, i).start()
            for i in pieces_of(m, half):
                along_b(1, i).wait_recv()
                to_core(2, i).start()

        @pl.when(is_n == 1)
        def _():
            for i in pieces_of(m, half):
                to_core(3, i).wait_recv()
                to_core(2, i).wait_recv()

    zb = z // 2
    za = (z + zb) % 2
    yb = y // 2
    ya = (y + yb) % 2

    def weight(d0, d1, k):
        on0, on1 = 2 ** ((d0 - k) % 4), 2 ** ((d1 - k) % 4)
        return on0 + tr * (on1 - on0)

    def stream_copy(m, k, q, to):
        return remote(
            prod[m].at[k, q], recv[m].at[k, q], s_send.at[m, k, q], s_recv.at[m, k, q], to
        )

    def extra_copy(m, k, q, to):
        return remote(
            prox[m].at[k, q], recx[m].at[k, q], x_send.at[m, k, q], x_recv.at[m, k, q], to
        )

    def dot(m, e, c, s):
        half = buf[m].shape[2] // 2
        tokens = 2 * buf[m].shape[1]
        base = e * 2 + (1 - e) * 4 * is_n
        left = buf[m][pl.ds(base, 2), :, pl.ds(pl.multiple_of(c * half, 128), half)]
        right = buf[m][pl.ds(0, 2), :, pl.ds(pl.multiple_of(s * half, 128), half)]
        return lax.dot_general(
            left.reshape(tokens, half),
            right.reshape(tokens, half),
            (((0,), (0,)), ((), ())),
            preferred_element_type=jnp.float32,
        )

    def bits_of(yy):
        return ((yy ^ (yy >> 1)) % 2 + ya) % 2, (yy // 2 + yb) % 2

    def product(m, e, c):
        value = dot(m, e, c, (c + (e * tc if e else is_n * h)) % 2)
        rows = value.shape[0] // 8
        block = (tc + e) % 2
        rza = (c + block + za) % 2
        rzb = (block + zb) % 2
        for yy in range(4):
            rya, ryb = bits_of(yy)
            for k in range(2):
                q = rza * weight(2, 0, k) + rzb * weight(3, 1, k)
                q = q + rya * weight(0, 2, k) + ryb * weight(1, 3, k)
                first = (2 * yy + k) * rows
                prod[m][k, q] = value[first : first + rows].astype(jnp.bfloat16)

                @pl.when(q % 2 == 1)
                def _(k=k, q=q):
                    stream_copy(m, k, q, partner(k)).start()

    EXTRA = ((y_a, y_b, z_a), (z_a, y_b, y_a))

    def product_extra(m, c):
        value = dot(m, 0, c, 1 - c)
        rows = value.shape[0] // 8
        rza = (c + tc + za) % 2
        for yy in range(4):
            rya, ryb = bits_of(yy)
            for k in range(2):
                q = rya + 2 * ryb + 4 * rza if k == 0 else rza + 2 * ryb + 4 * rya
                first = (2 * yy + k) * rows
                prox[m][k, q] = value[first : first + rows].astype(jnp.bfloat16)

                @pl.when(q % 2 == 1)
                def _(k=k, q=q):
                    extra_copy(m, k, q, EXTRA[k][0]).start()

    def total(own_ref, got_ref, k, q, parts):
        value = own_ref[k, q].astype(jnp.float32)
        for p in parts:
            value = value + got_ref[k, p].astype(jnp.float32)
        return value

    def stage(m, j):
        for k in range(2):
            to = partner((j + k) % 4)

            def one(i, carry, k=k, to=to):
                q = i * 2 ** (j + 1) + 2**j
                parts = [q + 2**b for b in range(j)]
                for p in parts:
                    stream_copy(m, k, p, core).wait_recv()
                prod[m][k, q] = total(prod[m], recv[m], k, q, parts).astype(jnp.bfloat16)
                stream_copy(m, k, q, to).start()
                return carry

            lax.fori_loop(0, 2 ** (3 - j), one, 0)

    def stage_extra(m, j):
        @pl.when(is_n == 0)
        def _():
            for k in range(2):
                if j < 3:

                    def one(i, carry, k=k):
                        q = i * 2 ** (j + 1) + 2**j
                        parts = [q + 2**b for b in range(j)]
                        for p in parts:
                            extra_copy(m, k, p, core).wait_recv()
                        prox[m][k, q] = total(prox[m], recx[m], k, q, parts).astype(
                            jnp.bfloat16
                        )
                        extra_copy(m, k, q, EXTRA[k][j]).start()
                        return carry

                    lax.fori_loop(0, 2 ** (2 - j), one, 0)
                else:
                    for p in (1, 2, 4):
                        extra_copy(m, k, p, core).wait_recv()

                    @pl.when(apart == 1)
                    def _(k=k):
                        prox[m][k, 0] = total(prox[m], recx[m], k, 0, (1, 2, 4)).astype(
                            jnp.bfloat16
                        )
                        extra_copy(m, k, 0, z_b).start()

    def at(m, block, s):
        width = buf[m].shape[2]
        half = width // 2
        first = pl.multiple_of(block * width + s * half, 128)
        return pl.ds(first, half)

    def last_copy(m, k):
        to = others[k]
        return remote(
            fin[m].at[2 * to[3] + to[4]],
            row[m].at[:, at(m, 2 * tr + tc, side)],
            f_send.at[m, k],
            f_recv.at[m, k],
            to,
        )

    def last_extra(m, k):
        to = others[k]
        return remote(
            finx[m].at[2 * to[3] + to[4]],
            row[m].at[:, at(m, 2 * tr + tc, 1 - c_mine)],
            g_send.at[m, k],
            g_recv.at[m],
            to,
        )

    def turned_copy(m, i, to):
        return remote(
            turn[m].at[i], mir[m].at[kind, y], m_send.at[m, i], m_recv.at[m, kind, y], to
        )

    def by_quarter(m, ref, value, s):
        rows = value.shape[0] // 4
        for i in range(4):
            ref[m][i] = value[i * rows : (i + 1) * rows].astype(jnp.bfloat16)
        row[m][:, at(m, 2 * tr + tc, s)] = ref[m][2 * tr + tc]

    def finish(m):
        parts = (1, 2, 4, 8)
        for k in range(2):
            for p in parts:
                stream_copy(m, k, p, core).wait_recv()
        value = jnp.concatenate(
            [total(prod[m], recv[m], k, 0, parts) for k in range(2)], axis=0
        )
        by_quarter(m, fin, value, side)
        for k in range(3):
            last_copy(m, k).start()

        @pl.when(mirrors == 1)
        def _():
            lanes = turn[m].shape[2]
            tall = value
            if lanes != value.shape[0]:
                fill = jnp.zeros((lanes - value.shape[0], value.shape[1]), jnp.float32)
                tall = jnp.concatenate([value, fill], axis=0)
            turned = tall.T
            rows = turned.shape[0] // 16
            for i, to in quarters():
                turn[m][i] = turned[i * rows : (i + 1) * rows].astype(jnp.bfloat16)
                turned_copy(m, i, to).start()

    def finish_extra(m):
        @pl.when(mirrors == 0)
        def _():
            for k in range(2):
                extra_copy(m, k, 0, core).wait_recv()
            value = jnp.concatenate(
                [total(prox[m], recx[m], k, 0, (1, 2, 4, 0)) for k in range(2)], axis=0
            )
            by_quarter(m, finx, value, 1 - c_mine)
            for k in range(3):
                last_extra(m, k).start()

    def gather_rows(m):
        width = buf[m].shape[2]
        rows = width // 8
        for t in range(3):
            for yy in range(4):
                remote(
                    turn[m].at[0], mir[m].at[t, yy], m_send.at[m, 0], m_recv.at[m, t, yy], core
                ).wait_recv()
            value = jnp.concatenate(
                [mir[m][t, yy].astype(jnp.float32)[:, :rows] for yy in range(4)], axis=1
            )
            chunk = turned_rows[t]
            row[m][:, at(m, chunk // 2, chunk % 2)] = value.astype(jnp.bfloat16)
        for k in range(3):
            last_copy(m, k).wait_recv()

        @pl.when(mirrors == 1)
        def _():
            last_extra(m, 0).wait_recv()

        own_out(m).start()

    def own_out(m):
        return pltpu.make_async_copy(row[m], out[m], o_sem.at[m])

    def products(m, e, first, last):
        def one(c, carry):
            product(m, e, c)
            return carry

        lax.fori_loop(first, last, one, 0)

    def extras(m):
        @pl.when(is_n == 0)
        def _():
            def one(c, carry):
                product_extra(m, c)
                return carry

            lax.fori_loop(0, 2, one, 0)

    step_a = scoped("step_a", step_a)
    step_b = scoped("step_b", step_b)
    products = scoped("products", products)
    extras = scoped("extras", extras)
    stage = scoped("stage", stage)
    stage_extra = scoped("stage_extra", stage_extra)
    finish = scoped("finish", finish)
    finish_extra = scoped("finish_extra", finish_extra)
    gather_rows = scoped("gather_rows", gather_rows)

    early_0 = 1 - is_n * h
    early_1 = 1 - tc

    for copy in own:
        copy.wait()
    step_a(GRAD, 0)
    products(GRAD, 0, 0, early_0)
    step_b(GRAD, 0)
    products(GRAD, 1, 0, early_1)
    step_a(GRAD, 1)
    products(GRAD, 0, early_0, 2)
    products(GRAD, 1, early_1, 1)
    extras(GRAD)
    step_b(GRAD, 1)
    products(GRAD, 1, 1, 2)
    step_a(ACT, 0)
    stage(GRAD, 1)
    stage_extra(GRAD, 1)
    step_a(ACT, 1)
    products(ACT, 0, 0, 2)
    extras(ACT)
    stage(GRAD, 2)
    stage_extra(GRAD, 2)
    step_b(ACT, 0)
    step_b(ACT, 1)
    products(ACT, 1, 0, 2)
    stage(GRAD, 3)
    stage_extra(GRAD, 3)
    stage(ACT, 1)
    stage_extra(ACT, 1)
    finish(GRAD)
    stage(ACT, 2)
    stage_extra(ACT, 2)
    finish_extra(GRAD)
    stage(ACT, 3)
    stage_extra(ACT, 3)
    finish(ACT)
    finish_extra(ACT)
    gather_rows(GRAD)
    gather_rows(ACT)

    with jax.named_scope("drain"):
        for i in every:
            along_a(i).wait_send()

        @pl.when(is_n == 1)
        def _():
            for i in every:
                for k in (0, 1):
                    along_b(k, i).wait_send()

        @pl.when(is_n == 0)
        def _():
            for i in every:
                for k in range(4):
                    to_core(k, i).wait_send()
            for m in (ACT, GRAD):
                for k in range(2):
                    for q in range(1, 8):
                        extra_copy(m, k, q, core).wait_send()

                    @pl.when(apart == 1)
                    def _(m=m, k=k):
                        extra_copy(m, k, 0, core).wait_send()

        for m in (ACT, GRAD):
            for k in range(2):
                for q in range(1, 16):
                    stream_copy(m, k, q, core).wait_send()
            for k in range(3):
                last_copy(m, k).wait_send()

            @pl.when(mirrors == 1)
            def _(m=m):
                for i, to in quarters():
                    turned_copy(m, i, to).wait_send()

            @pl.when(mirrors == 0)
            def _(m=m):
                for k in range(3):
                    last_extra(m, k).wait_send()

            own_out(m).wait()


def sums(activations, gradients, rows_a, rows_g):
    tokens = activations.shape[0]
    wide = (activations.shape[1], gradients.shape[1])
    rows = (rows_a, rows_g)
    bf16 = jnp.bfloat16
    lanes = [-(-w // 1024) * 128 for w in wide]
    vmem = [
        *(pltpu.VMEM((6, tokens, w), bf16) for w in wide),
        *(pltpu.VMEM((2, 16, w // 16, w // 2), bf16) for w in wide),
        *(pltpu.VMEM((2, 16, w // 16, w // 2), bf16) for w in wide),
        *(pltpu.VMEM((2, 8, w // 16, w // 2), bf16) for w in wide),
        *(pltpu.VMEM((2, 8, w // 16, w // 2), bf16) for w in wide),
        *(pltpu.VMEM((4, r, w // 2), bf16) for r, w in zip(rows, wide)),
        *(pltpu.VMEM((4, r, w // 2), bf16) for r, w in zip(rows, wide)),
        *(pltpu.VMEM((16, r, n), bf16) for r, n in zip(rows, lanes)),
        *(pltpu.VMEM((3, 4, r, n), bf16) for r, n in zip(rows, lanes)),
        *(pltpu.VMEM((r, 4 * w), bf16) for r, w in zip(rows, wide)),
    ]
    n = len(PIECES)
    dma = pltpu.SemaphoreType.DMA
    sems = [
        dma((2,)), dma((n,)), dma((n,)), dma((2, n)), dma((2, n)), dma((4, n)), dma((4, n)),
        dma((2, 2, 16)), dma((2, 2, 16)), dma((2, 2, 8)), dma((2, 2, 8)),
        dma((2, 3)), dma((2, 3)), dma((2, 3)), dma((2,)),
        dma((2, 16)), dma((2, 3, 4)), dma((2,)),
    ]
    anywhere = pl.BlockSpec(memory_space=pl.ANY)
    return pl.pallas_call(
        kernel,
        out_shape=[jax.ShapeDtypeStruct((r, 4 * w), bf16) for r, w in zip(rows, wide)],
        in_specs=[anywhere] * 2,
        out_specs=[anywhere] * 2,
        scratch_shapes=[*vmem, *sems],
        compiler_params=pltpu.CompilerParams(
            collective_id=0, has_side_effects=True, vmem_limit_bytes=66_000_000
        ),
    )(activations, gradients)


def body(activations, gradients, old_inputs, old_gradients):
    tokens_all = activations.shape[0] * lax.axis_size(DP)
    sum_a, sum_g = sums(activations, gradients, old_inputs.shape[0], old_gradients.shape[0])
    scale = 0.5 / tokens_all
    return (
        0.5 * old_inputs + scale * sum_a.astype(jnp.float32),
        0.5 * old_gradients + scale * sum_g.astype(jnp.float32),
    )


def solution(mesh):
    finer = Mesh(mesh.devices.reshape(2, 4, 4, mesh.shape["tr"], mesh.shape["tc"]), AXES)
    return jax.shard_map(
        body,
        mesh=finer,
        in_specs=(P(DP, ("tr", "tc")), P(DP, ("tr", "tc")), P(DP_TR_TC, None), P(DP_TR_TC, None)),
        out_specs=(P(DP_TR_TC, None), P(DP_TR_TC, None)),
        check_vma=False,
    )
```

```python
import functools

import jax
import jax.numpy as jnp
from jax import lax
from jax.experimental import pallas as pl
from jax.experimental.pallas import tpu as pltpu
from jax.sharding import Mesh
from jax.sharding import PartitionSpec as P

MESH = pl.DeviceIdType.MESH
DP = ("dp_0", "dp_1", "dp_2")
DP_TR_TC = ("dp_0", "dp_1", "dp_2", "tr", "tc")
AXES = DP_TR_TC

ACT, GRAD = 0, 1
PIECES = (
    (GRAD, 0, 512, 0),
    (GRAD, 512, 384, 0),
    (GRAD, 0, 512, 1),
    (GRAD, 512, 384, 1),
    (ACT, 0, 512, 0),
    (ACT, 0, 512, 1),
)
AT_ONCE = (0, 1, 2)
AFTER = {1: (3,), 3: (4, 5)}


def pieces_of(m, half):
    return [i for i, p in enumerate(PIECES) if p[0] == m and p[3] == half]


def scoped(name, f):
    def g(*a):
        with jax.named_scope(name + "#" + "_".join(str(x) for x in a if isinstance(x, int))):
            return f(*a)

    return g


def kernel(
    act, grad, out_a, out_g,
    buf_a, buf_g, prod_a, prod_g, recv_a, recv_g, prox_a, prox_g, recx_a, recx_g,
    fin_a, fin_g, finx_a, finx_g, turn_a, turn_g, mir_a, mir_g, row_a, row_g,
    own_sem, a_send, a_recv, b_send, b_recv, d_send, d_recv,
    s_send, s_recv, x_send, x_recv, f_send, f_recv, g_send, g_recv, m_send, m_recv, o_sem,
):
    h = lax.axis_index("dp_0")
    z = lax.axis_index("dp_1")
    y = lax.axis_index("dp_2")
    tr = lax.axis_index("tr")
    tc = lax.axis_index("tc")
    is_n = (tr + h) % 2
    odd = (h + tc) % 2
    shift = (is_n * odd, (1 - is_n) * odd + is_n * tc)

    src = (act, grad)
    out = (out_a, out_g)
    buf = (buf_a, buf_g)
    prod = (prod_a, prod_g)
    recv = (recv_a, recv_g)
    prox = (prox_a, prox_g)
    recx = (recx_a, recx_g)
    fin = (fin_a, fin_g)
    finx = (finx_a, finx_g)
    turn = (turn_a, turn_g)
    mir = (mir_a, mir_g)
    row = (row_a, row_g)

    def flip1(v):
        return v + 1 - 2 * (v % 2)

    def flip3(v):
        return 3 - v

    x1 = (1 - h, z, y, tr, tc)
    x3 = (1 - h, z, y, tr, 1 - tc)
    core = (h, z, y, 1 - tr, tc)
    others = ((h, z, y, tr, 1 - tc), core, (h, z, y, 1 - tr, 1 - tc))
    y_a, y_b = (h, z, flip1(y), tr, tc), (h, z, flip3(y), tr, tc)
    z_a, z_b = (h, flip1(z), y, tr, tc), (h, flip3(z), y, tr, tc)

    def partner(d):
        f = flip1 if d % 2 == 0 else flip3
        on_y = (1 - tr) if d < 2 else tr
        return (
            h,
            on_y * z + (1 - on_y) * f(z),
            on_y * f(y) + (1 - on_y) * y,
            tr,
            tc,
        )

    half_z = z // 2
    c_mine = z % 2
    apart = (half_z + tc) % 2
    side = (c_mine + apart * shift[1] + (1 - apart) * shift[0]) % 2
    mirrors = 1 - (1 - is_n) * (1 - apart)
    kind = is_n * (1 + apart)
    turned_rows = (
        4 * h + 2 * (1 - half_z) + (c_mine + h + half_z) % 2,
        4 * (1 - h) + 2 * half_z + (c_mine + 1 + h + half_z) % 2,
        4 * (1 - h) + 2 * (1 - half_z) + (c_mine + half_z) % 2,
    )

    def quarters():
        for yy in range(4):
            for aa in range(2):
                for bb in range(2):
                    yield yy * 4 + aa * 2 + bb, (tr, 2 * tc + side, yy, aa, bb)

    barrier = pltpu.get_barrier_semaphore()
    peers = [x1, x3, *others, y_a, y_b, z_a, z_b]

    def greet(peer):
        pl.semaphore_signal(barrier, inc=1, device_id=peer, device_id_type=MESH)

    for peer in peers:
        greet(peer)
    for chunk in turned_rows:
        for yy in range(4):
            greet((chunk // 4, chunk % 4, yy, h, half_z))

    own = [pltpu.make_async_copy(src[m], buf[m].at[0], own_sem.at[m]) for m in (ACT, GRAD)]
    for copy in own:
        copy.start()
    pl.semaphore_wait(barrier, len(peers) + 16 * mirrors)

    def cols(i, first):
        m, offset, size, later = PIECES[i]
        start = (first + later) % 2 * (buf[m].shape[2] // 2) + offset
        return pl.ds(pl.multiple_of(start, 128), size)

    def remote(a, b, ss, rs, to):
        return pltpu.make_async_remote_copy(
            src_ref=a, dst_ref=b, send_sem=ss, recv_sem=rs, device_id=to, device_id_type=MESH
        )

    def along_a(i):
        m = PIECES[i][0]
        to = (1 - is_n) * (1 - odd)
        return remote(
            src[m].at[:, cols(i, to)], buf[m].at[1, :, cols(i, to)], a_send.at[i], a_recv.at[i], x1
        )

    def along_b(k, i):
        m = PIECES[i][0]
        part = cols(i, odd)
        source = src[m].at[:, part] if k == 0 else buf[m].at[1, :, part]
        return remote(source, buf[m].at[3 - k, :, part], b_send.at[k, i], b_recv.at[k, i], x3)

    def to_core(k, i):
        m = PIECES[i][0]
        part = cols(i, 0 if k < 2 else odd)
        source = src[m].at[:, part] if k == 0 else buf[m].at[k, :, part]
        slot = k + 4 if k < 2 else k
        return remote(source, buf[m].at[slot, :, part], d_send.at[k, i], d_recv.at[k, i], core)

    every = range(len(PIECES))
    for i in every:
        along_a(i).start()

    @pl.when(is_n == 1)
    def _():
        for i in AT_ONCE:
            along_b(0, i).start()

    @pl.when(is_n == 0)
    def _():
        for i in every:
            to_core(0, i).start()

    def step_a(m, half):
        for i in pieces_of(m, half):
            along_a(i).wait_recv()

            @pl.when(is_n == 1)
            def _(i=i):
                along_b(1, i).start()
                for j in AFTER.get(i, ()):
                    along_b(0, j).start()

            @pl.when(is_n == 0)
            def _(i=i):
                to_core(1, i).start()

        @pl.when(is_n == 1)
        def _():
            for i in pieces_of(m, half):
                to_core(0, i).wait_recv()
                to_core(1, i).wait_recv()

    def step_b(m, half):
        @pl.when(is_n == 0)
        def _():
            for i in pieces_of(m, half):
                along_b(0, i).wait_recv()
                to_core(3, i).start()
            for i in pieces_of(m, half):
                along_b(1, i).wait_recv()
                to_core(2, i).start()

        @pl.when(is_n == 1)
        def _():
            for i in pieces_of(m, half):
                to_core(3, i).wait_recv()
                to_core(2, i).wait_recv()

    zb = z // 2
    za = (z + zb) % 2
    yb = y // 2
    ya = (y + yb) % 2

    def weight(d0, d1, k):
        on0, on1 = 2 ** ((d0 - k) % 4), 2 ** ((d1 - k) % 4)
        return on0 + tr * (on1 - on0)

    def stream_copy(m, k, q, to):
        return remote(
            prod[m].at[k, q], recv[m].at[k, q], s_send.at[m, k, q], s_recv.at[m, k, q], to
        )

    def extra_copy(m, k, q, to):
        return remote(
            prox[m].at[k, q], recx[m].at[k, q], x_send.at[m, k, q], x_recv.at[m, k, q], to
        )

    def dot(m, e, c, s):
        half = buf[m].shape[2] // 2
        tokens = 2 * buf[m].shape[1]
        base = e * 2 + (1 - e) * 4 * is_n
        left = buf[m][pl.ds(base, 2), :, pl.ds(pl.multiple_of(c * half, 128), half)]
        right = buf[m][pl.ds(0, 2), :, pl.ds(pl.multiple_of(s * half, 128), half)]
        return lax.dot_general(
            left.reshape(tokens, half),
            right.reshape(tokens, half),
            (((0,), (0,)), ((), ())),
            preferred_element_type=jnp.float32,
        )

    def bits_of(yy):
        return ((yy ^ (yy >> 1)) % 2 + ya) % 2, (yy // 2 + yb) % 2

    def product(m, e, order):
        c = (order + odd) % 2 if e else order
        value = dot(m, e, c, (c + shift[e]) % 2)
        rows = value.shape[0] // 8
        block = (tc + e) % 2
        rza = (c + block + za) % 2
        rzb = (block + zb) % 2
        for yy in range(4):
            rya, ryb = bits_of(yy)
            for k in range(2):
                q = rza * weight(2, 0, k) + rzb * weight(3, 1, k)
                q = q + rya * weight(0, 2, k) + ryb * weight(1, 3, k)
                first = (2 * yy + k) * rows
                prod[m][k, q] = value[first : first + rows].astype(jnp.bfloat16)

                @pl.when(q % 2 == 1)
                def _(k=k, q=q):
                    stream_copy(m, k, q, partner(k)).start()

    def pick(a, b):
        return tuple(v + odd * (w - v) for v, w in zip(a, b))

    EXTRA = ((y_a, y_b, z_a), (pick(z_a, y_b), pick(y_b, z_a), y_a))

    def product_extra(m, c):
        value = dot(m, 0, c, 1 - c)
        rows = value.shape[0] // 8
        rza = (c + tc + za) % 2
        for yy in range(4):
            rya, ryb = bits_of(yy)
            for k in range(2):
                q = rya + 2 * ryb + 4 * rza if k == 0 else (1 + odd) * rza + (2 - odd) * ryb + 4 * rya
                first = (2 * yy + k) * rows
                prox[m][k, q] = value[first : first + rows].astype(jnp.bfloat16)

                @pl.when(q % 2 == 1)
                def _(k=k, q=q):
                    extra_copy(m, k, q, EXTRA[k][0]).start()

    def total(own_ref, got_ref, k, q, parts):
        value = own_ref[k, q].astype(jnp.float32)
        for p in parts:
            value = value + got_ref[k, p].astype(jnp.float32)
        return value

    early_0 = 1
    early_1 = 1 - is_n * tc

    def is_early(k, q):
        def bit(d0, d1):
            at0, at1 = 2 ** ((d0 - k) % 4), 2 ** ((d1 - k) % 4)
            return (1 - tr) * (q // at0 % 2) + tr * (q // at1 % 2)

        block = (bit(3, 1) + zb) % 2
        c = (bit(2, 0) + za + block) % 2
        e = (block + tc) % 2
        return (1 - e) * (1 - c) + e * ((c + odd + 1) % 2) * early_1

    def stage(m, j, early=None):
        def move(k, q, parts):
            for p in parts:
                stream_copy(m, k, p, core).wait_recv()
            prod[m][k, q] = total(prod[m], recv[m], k, q, parts).astype(jnp.bfloat16)
            stream_copy(m, k, q, partner((j + k) % 4)).start()

        def one(i, carry):
            q = i * 2 ** (j + 1) + 2**j
            parts = [q + 2**b for b in range(j)]
            for k in range(2):
                if early is None:
                    move(k, q, parts)
                else:
                    pl.when(is_early(k, q) == early)(functools.partial(move, k, q, parts))
            return carry

        lax.fori_loop(0, 2 ** (3 - j), one, 0)

    def stage_extra(m, j):
        @pl.when(is_n == 0)
        def _():
            for k in range(2):
                if j < 3:

                    def one(i, carry, k=k):
                        q = i * 2 ** (j + 1) + 2**j
                        parts = [q + 2**b for b in range(j)]
                        for p in parts:
                            extra_copy(m, k, p, core).wait_recv()
                        prox[m][k, q] = total(prox[m], recx[m], k, q, parts).astype(
                            jnp.bfloat16
                        )
                        extra_copy(m, k, q, EXTRA[k][j]).start()
                        return carry

                    lax.fori_loop(0, 2 ** (2 - j), one, 0)
                else:
                    for p in (1, 2, 4):
                        extra_copy(m, k, p, core).wait_recv()

                    @pl.when(apart == 1)
                    def _(k=k):
                        prox[m][k, 0] = total(prox[m], recx[m], k, 0, (1, 2, 4)).astype(
                            jnp.bfloat16
                        )
                        extra_copy(m, k, 0, z_b).start()

    def at(m, block, s):
        width = buf[m].shape[2]
        half = width // 2
        first = pl.multiple_of(block * width + s * half, 128)
        return pl.ds(first, half)

    def last_copy(m, k):
        to = others[k]
        return remote(
            fin[m].at[2 * to[3] + to[4]],
            row[m].at[:, at(m, 2 * tr + tc, side)],
            f_send.at[m, k],
            f_recv.at[m, k],
            to,
        )

    def last_extra(m, k):
        to = others[k]
        return remote(
            finx[m].at[2 * to[3] + to[4]],
            row[m].at[:, at(m, 2 * tr + tc, 1 - c_mine)],
            g_send.at[m, k],
            g_recv.at[m],
            to,
        )

    def turned_copy(m, i, to):
        return remote(
            turn[m].at[i], mir[m].at[kind, y], m_send.at[m, i], m_recv.at[m, kind, y], to
        )

    def by_quarter(m, ref, value, s):
        rows = value.shape[0] // 4
        for i in range(4):
            ref[m][i] = value[i * rows : (i + 1) * rows].astype(jnp.bfloat16)
        row[m][:, at(m, 2 * tr + tc, s)] = ref[m][2 * tr + tc]

    def finish(m):
        parts = (1, 2, 4, 8)
        for k in range(2):
            for p in parts:
                stream_copy(m, k, p, core).wait_recv()
        value = jnp.concatenate(
            [total(prod[m], recv[m], k, 0, parts) for k in range(2)], axis=0
        )
        by_quarter(m, fin, value, side)
        for k in range(3):
            last_copy(m, k).start()

        @pl.when(mirrors == 1)
        def _():
            lanes = turn[m].shape[2]
            tall = value
            if lanes != value.shape[0]:
                fill = jnp.zeros((lanes - value.shape[0], value.shape[1]), jnp.float32)
                tall = jnp.concatenate([value, fill], axis=0)
            turned = tall.T
            rows = turned.shape[0] // 16
            for i, to in quarters():
                turn[m][i] = turned[i * rows : (i + 1) * rows].astype(jnp.bfloat16)
                turned_copy(m, i, to).start()

    def finish_extra(m):
        @pl.when(mirrors == 0)
        def _():
            for k in range(2):
                extra_copy(m, k, 0, core).wait_recv()
            value = jnp.concatenate(
                [total(prox[m], recx[m], k, 0, (1, 2, 4, 0)) for k in range(2)], axis=0
            )
            by_quarter(m, finx, value, 1 - c_mine)
            for k in range(3):
                last_extra(m, k).start()

    def gather_rows(m):
        width = buf[m].shape[2]
        rows = width // 8
        for t in range(3):
            for yy in range(4):
                remote(
                    turn[m].at[0], mir[m].at[t, yy], m_send.at[m, 0], m_recv.at[m, t, yy], core
                ).wait_recv()
            value = jnp.concatenate(
                [mir[m][t, yy].astype(jnp.float32)[:, :rows] for yy in range(4)], axis=1
            )
            chunk = turned_rows[t]
            row[m][:, at(m, chunk // 2, chunk % 2)] = value.astype(jnp.bfloat16)
        for k in range(3):
            last_copy(m, k).wait_recv()

        @pl.when(mirrors == 1)
        def _():
            last_extra(m, 0).wait_recv()

        own_out(m).start()

    def own_out(m):
        return pltpu.make_async_copy(row[m], out[m], o_sem.at[m])

    def products(m, e, first, last):
        def one(c, carry):
            product(m, e, c)
            return carry

        lax.fori_loop(first, last, one, 0)

    def extras(m):
        @pl.when(is_n == 0)
        def _():
            def one(c, carry):
                product_extra(m, c)
                return carry

            lax.fori_loop(0, 2, one, 0)

    step_a = scoped("step_a", step_a)
    step_b = scoped("step_b", step_b)
    products = scoped("products", products)
    extras = scoped("extras", extras)
    stage = scoped("stage", stage)
    stage_extra = scoped("stage_extra", stage_extra)
    finish = scoped("finish", finish)
    finish_extra = scoped("finish_extra", finish_extra)
    gather_rows = scoped("gather_rows", gather_rows)

    for copy in own:
        copy.wait()
    step_a(GRAD, 0)
    products(GRAD, 0, 0, early_0)
    step_b(GRAD, 0)
    products(GRAD, 1, 0, early_1)
    step_a(GRAD, 1)
    products(GRAD, 0, early_0, 2)
    products(GRAD, 1, early_1, 1)
    extras(GRAD)
    stage(GRAD, 1, 1)
    step_b(GRAD, 1)
    products(GRAD, 1, 1, 2)
    step_a(ACT, 0)
    step_a(ACT, 1)
    products(ACT, 0, 0, 2)
    extras(ACT)
    stage(GRAD, 1, 0)
    stage_extra(GRAD, 1)
    step_b(ACT, 0)
    step_b(ACT, 1)
    products(ACT, 1, 0, 2)
    stage(GRAD, 2)
    stage_extra(GRAD, 2)
    stage(ACT, 1)
    stage_extra(ACT, 1)
    stage(GRAD, 3)
    stage_extra(GRAD, 3)
    stage(ACT, 2)
    stage_extra(ACT, 2)
    finish(GRAD)
    finish_extra(GRAD)
    stage(ACT, 3)
    stage_extra(ACT, 3)
    finish(ACT)
    finish_extra(ACT)
    gather_rows(GRAD)
    gather_rows(ACT)

    with jax.named_scope("drain"):
        for i in every:
            along_a(i).wait_send()

        @pl.when(is_n == 1)
        def _():
            for i in every:
                for k in (0, 1):
                    along_b(k, i).wait_send()

        @pl.when(is_n == 0)
        def _():
            for i in every:
                for k in range(4):
                    to_core(k, i).wait_send()
            for m in (ACT, GRAD):
                for k in range(2):
                    for q in range(1, 8):
                        extra_copy(m, k, q, core).wait_send()

                    @pl.when(apart == 1)
                    def _(m=m, k=k):
                        extra_copy(m, k, 0, core).wait_send()

        for m in (ACT, GRAD):
            for k in range(2):
                for q in range(1, 16):
                    stream_copy(m, k, q, core).wait_send()
            for k in range(3):
                last_copy(m, k).wait_send()

            @pl.when(mirrors == 1)
            def _(m=m):
                for i, to in quarters():
                    turned_copy(m, i, to).wait_send()

            @pl.when(mirrors == 0)
            def _(m=m):
                for k in range(3):
                    last_extra(m, k).wait_send()

            own_out(m).wait()


def sums(activations, gradients, rows_a, rows_g):
    tokens = activations.shape[0]
    wide = (activations.shape[1], gradients.shape[1])
    rows = (rows_a, rows_g)
    bf16 = jnp.bfloat16
    lanes = [-(-w // 1024) * 128 for w in wide]
    vmem = [
        *(pltpu.VMEM((6, tokens, w), bf16) for w in wide),
        *(pltpu.VMEM((2, 16, w // 16, w // 2), bf16) for w in wide),
        *(pltpu.VMEM((2, 16, w // 16, w // 2), bf16) for w in wide),
        *(pltpu.VMEM((2, 8, w // 16, w // 2), bf16) for w in wide),
        *(pltpu.VMEM((2, 8, w // 16, w // 2), bf16) for w in wide),
        *(pltpu.VMEM((4, r, w // 2), bf16) for r, w in zip(rows, wide)),
        *(pltpu.VMEM((4, r, w // 2), bf16) for r, w in zip(rows, wide)),
        *(pltpu.VMEM((16, r, n), bf16) for r, n in zip(rows, lanes)),
        *(pltpu.VMEM((3, 4, r, n), bf16) for r, n in zip(rows, lanes)),
        *(pltpu.VMEM((r, 4 * w), bf16) for r, w in zip(rows, wide)),
    ]
    n = len(PIECES)
    dma = pltpu.SemaphoreType.DMA
    sems = [
        dma((2,)), dma((n,)), dma((n,)), dma((2, n)), dma((2, n)), dma((4, n)), dma((4, n)),
        dma((2, 2, 16)), dma((2, 2, 16)), dma((2, 2, 8)), dma((2, 2, 8)),
        dma((2, 3)), dma((2, 3)), dma((2, 3)), dma((2,)),
        dma((2, 16)), dma((2, 3, 4)), dma((2,)),
    ]
    anywhere = pl.BlockSpec(memory_space=pl.ANY)
    return pl.pallas_call(
        kernel,
        out_shape=[jax.ShapeDtypeStruct((r, 4 * w), bf16) for r, w in zip(rows, wide)],
        in_specs=[anywhere] * 2,
        out_specs=[anywhere] * 2,
        scratch_shapes=[*vmem, *sems],
        compiler_params=pltpu.CompilerParams(
            collective_id=0, has_side_effects=True, vmem_limit_bytes=66_000_000
        ),
    )(activations, gradients)


def body(activations, gradients, old_inputs, old_gradients):
    tokens_all = activations.shape[0] * lax.axis_size(DP)
    sum_a, sum_g = sums(activations, gradients, old_inputs.shape[0], old_gradients.shape[0])
    scale = 0.5 / tokens_all
    return (
        0.5 * old_inputs + scale * sum_a.astype(jnp.float32),
        0.5 * old_gradients + scale * sum_g.astype(jnp.float32),
    )


def solution(mesh):
    finer = Mesh(mesh.devices.reshape(2, 4, 4, mesh.shape["tr"], mesh.shape["tc"]), AXES)
    return jax.shard_map(
        body,
        mesh=finer,
        in_specs=(P(DP, ("tr", "tc")), P(DP, ("tr", "tc")), P(DP_TR_TC, None), P(DP_TR_TC, None)),
        out_specs=(P(DP_TR_TC, None), P(DP_TR_TC, None)),
        check_vma=False,
    )
```

```python
import functools

import jax
import jax.numpy as jnp
from jax import lax
from jax.experimental import pallas as pl
from jax.experimental.pallas import tpu as pltpu
from jax.sharding import Mesh
from jax.sharding import PartitionSpec as P

MESH = pl.DeviceIdType.MESH
DP = ("dp_0", "dp_1", "dp_2")
DP_TR_TC = ("dp_0", "dp_1", "dp_2", "tr", "tc")
AXES = DP_TR_TC

ACT, GRAD = 0, 1
PIECES = (
    (GRAD, 0, 512, 0),
    (GRAD, 512, 384, 0),
    (GRAD, 0, 512, 1),
    (GRAD, 512, 384, 1),
    (ACT, 0, 512, 0),
    (ACT, 0, 512, 1),
)
AT_ONCE = (0, 1, 2)
AFTER = {1: (3,), 3: (4, 5)}


def pieces_of(m, half):
    return [i for i, p in enumerate(PIECES) if p[0] == m and p[3] == half]


def scoped(name, f):
    def g(*a):
        with jax.named_scope(name + "#" + "_".join(str(x) for x in a if isinstance(x, int))):
            return f(*a)

    return g


def kernel(
    act, grad, out_a, out_g,
    buf_a, buf_g, prod_a, prod_g, recv_a, recv_g, prox_a, prox_g, recx_a, recx_g,
    fin_a, fin_g, finx_a, finx_g, turn_a, turn_g, mir_a, mir_g, row_a, row_g,
    own_sem, a_send, a_recv, b_send, b_recv, d_send, d_recv,
    s_send, s_recv, x_send, x_recv, f_send, f_recv, g_send, g_recv, m_send, m_recv, o_sem,
):
    h = lax.axis_index("dp_0")
    z = lax.axis_index("dp_1")
    y = lax.axis_index("dp_2")
    tr = lax.axis_index("tr")
    tc = lax.axis_index("tc")
    is_n = (tr + h) % 2
    odd = (h + tc) % 2
    shift = (is_n * odd, (1 - is_n) * odd + is_n * tc)

    src = (act, grad)
    out = (out_a, out_g)
    buf = (buf_a, buf_g)
    prod = (prod_a, prod_g)
    recv = (recv_a, recv_g)
    prox = (prox_a, prox_g)
    recx = (recx_a, recx_g)
    fin = (fin_a, fin_g)
    finx = (finx_a, finx_g)
    turn = (turn_a, turn_g)
    mir = (mir_a, mir_g)
    row = (row_a, row_g)

    def flip1(v):
        return v + 1 - 2 * (v % 2)

    def flip3(v):
        return 3 - v

    x1 = (1 - h, z, y, tr, tc)
    x3 = (1 - h, z, y, tr, 1 - tc)
    core = (h, z, y, 1 - tr, tc)
    others = ((h, z, y, tr, 1 - tc), core, (h, z, y, 1 - tr, 1 - tc))
    y_a, y_b = (h, z, flip1(y), tr, tc), (h, z, flip3(y), tr, tc)
    z_a, z_b = (h, flip1(z), y, tr, tc), (h, flip3(z), y, tr, tc)

    def partner(d):
        f = flip1 if d % 2 == 0 else flip3
        on_y = (1 - tr) if d < 2 else tr
        return (
            h,
            on_y * z + (1 - on_y) * f(z),
            on_y * f(y) + (1 - on_y) * y,
            tr,
            tc,
        )

    half_z = z // 2
    c_mine = z % 2
    apart = (half_z + tc) % 2
    side = (c_mine + apart * shift[1] + (1 - apart) * shift[0]) % 2
    mirrors = 1 - (1 - is_n) * (1 - apart)
    kind = is_n * (1 + apart)
    turned_rows = (
        4 * h + 2 * (1 - half_z) + (c_mine + h + half_z) % 2,
        4 * (1 - h) + 2 * half_z + (c_mine + 1 + h + half_z) % 2,
        4 * (1 - h) + 2 * (1 - half_z) + (c_mine + half_z) % 2,
    )

    def quarters():
        for yy in range(4):
            for aa in range(2):
                for bb in range(2):
                    yield yy * 4 + aa * 2 + bb, (tr, 2 * tc + side, yy, aa, bb)

    barrier = pltpu.get_barrier_semaphore()
    peers = [x1, x3, *others, y_a, y_b, z_a, z_b]

    def greet(peer):
        pl.semaphore_signal(barrier, inc=1, device_id=peer, device_id_type=MESH)

    for peer in peers:
        greet(peer)

    own = [pltpu.make_async_copy(src[m], buf[m].at[0], own_sem.at[m]) for m in (ACT, GRAD)]
    for copy in own:
        copy.start()
    pl.semaphore_wait(barrier, len(peers))

    def cols(i, first):
        m, offset, size, later = PIECES[i]
        start = (first + later) % 2 * (buf[m].shape[2] // 2) + offset
        return pl.ds(pl.multiple_of(start, 128), size)

    def remote(a, b, ss, rs, to):
        return pltpu.make_async_remote_copy(
            src_ref=a, dst_ref=b, send_sem=ss, recv_sem=rs, device_id=to, device_id_type=MESH
        )

    def along_a(i):
        m = PIECES[i][0]
        to = (1 - is_n) * (1 - odd)
        return remote(
            src[m].at[:, cols(i, to)], buf[m].at[1, :, cols(i, to)], a_send.at[i], a_recv.at[i], x1
        )

    def along_b(k, i):
        m = PIECES[i][0]
        part = cols(i, odd)
        source = src[m].at[:, part] if k == 0 else buf[m].at[1, :, part]
        return remote(source, buf[m].at[3 - k, :, part], b_send.at[k, i], b_recv.at[k, i], x3)

    def to_core(k, i):
        m = PIECES[i][0]
        part = cols(i, 0 if k < 2 else odd)
        source = src[m].at[:, part] if k == 0 else buf[m].at[k, :, part]
        slot = k + 4 if k < 2 else k
        return remote(source, buf[m].at[slot, :, part], d_send.at[k, i], d_recv.at[k, i], core)

    every = range(len(PIECES))
    for i in every:
        along_a(i).start()

    @pl.when(is_n == 1)
    def _():
        for i in AT_ONCE:
            along_b(0, i).start()

    @pl.when(is_n == 0)
    def _():
        for i in every:
            to_core(0, i).start()

    def step_a(m, half):
        for i in pieces_of(m, half):
            along_a(i).wait_recv()

            @pl.when(is_n == 1)
            def _(i=i):
                along_b(1, i).start()
                for j in AFTER.get(i, ()):
                    along_b(0, j).start()

            @pl.when(is_n == 0)
            def _(i=i):
                to_core(1, i).start()

        @pl.when(is_n == 1)
        def _():
            for i in pieces_of(m, half):
                to_core(0, i).wait_recv()
                to_core(1, i).wait_recv()

    def step_b(m, half):
        @pl.when(is_n == 0)
        def _():
            for i in pieces_of(m, half):
                along_b(0, i).wait_recv()
                to_core(3, i).start()
            for i in pieces_of(m, half):
                along_b(1, i).wait_recv()
                to_core(2, i).start()

        @pl.when(is_n == 1)
        def _():
            for i in pieces_of(m, half):
                to_core(3, i).wait_recv()
                to_core(2, i).wait_recv()

    zb = z // 2
    za = (z + zb) % 2
    yb = y // 2
    ya = (y + yb) % 2

    def weight(d0, d1, k):
        on0, on1 = 2 ** ((d0 - k) % 4), 2 ** ((d1 - k) % 4)
        return on0 + tr * (on1 - on0)

    def stream_copy(m, k, q, to):
        return remote(
            prod[m].at[k, q], recv[m].at[k, q], s_send.at[m, k, q], s_recv.at[m, k, q], to
        )

    def extra_copy(m, k, q, to):
        return remote(
            prox[m].at[k, q], recx[m].at[k, q], x_send.at[m, k, q], x_recv.at[m, k, q], to
        )

    def dot(m, e, c, s):
        half = buf[m].shape[2] // 2
        tokens = 2 * buf[m].shape[1]
        base = e * 2 + (1 - e) * 4 * is_n
        left = buf[m][pl.ds(base, 2), :, pl.ds(pl.multiple_of(c * half, 128), half)]
        right = buf[m][pl.ds(0, 2), :, pl.ds(pl.multiple_of(s * half, 128), half)]
        return lax.dot_general(
            left.reshape(tokens, half),
            right.reshape(tokens, half),
            (((0,), (0,)), ((), ())),
            preferred_element_type=jnp.float32,
        )

    def bits_of(yy):
        return ((yy ^ (yy >> 1)) % 2 + ya) % 2, (yy // 2 + yb) % 2

    def product(m, e, order):
        c = (order + odd) % 2 if e else order
        value = dot(m, e, c, (c + shift[e]) % 2)
        rows = value.shape[0] // 8
        block = (tc + e) % 2
        rza = (c + block + za) % 2
        rzb = (block + zb) % 2
        for yy in range(4):
            rya, ryb = bits_of(yy)
            for k in range(2):
                q = rza * weight(2, 0, k) + rzb * weight(3, 1, k)
                q = q + rya * weight(0, 2, k) + ryb * weight(1, 3, k)
                first = (2 * yy + k) * rows
                prod[m][k, q] = value[first : first + rows].astype(jnp.bfloat16)

                @pl.when(q % 2 == 1)
                def _(k=k, q=q):
                    stream_copy(m, k, q, partner(k)).start()

    def pick(a, b):
        return tuple(v + odd * (w - v) for v, w in zip(a, b))

    EXTRA = ((y_a, y_b, z_a), (pick(z_a, y_b), pick(y_b, z_a), y_a))

    def product_extra(m, c):
        value = dot(m, 0, c, 1 - c)
        rows = value.shape[0] // 8
        rza = (c + tc + za) % 2
        for yy in range(4):
            rya, ryb = bits_of(yy)
            for k in range(2):
                q = rya + 2 * ryb + 4 * rza if k == 0 else (1 + odd) * rza + (2 - odd) * ryb + 4 * rya
                first = (2 * yy + k) * rows
                prox[m][k, q] = value[first : first + rows].astype(jnp.bfloat16)

                @pl.when(q % 2 == 1)
                def _(k=k, q=q):
                    extra_copy(m, k, q, EXTRA[k][0]).start()

    def total(own_ref, got_ref, k, q, parts):
        value = own_ref[k, q].astype(jnp.float32)
        for p in parts:
            value = value + got_ref[k, p].astype(jnp.float32)
        return value

    early_0 = 1
    early_1 = 1 - is_n * tc

    def is_early(k, q):
        def bit(d0, d1):
            at0, at1 = 2 ** ((d0 - k) % 4), 2 ** ((d1 - k) % 4)
            return (1 - tr) * (q // at0 % 2) + tr * (q // at1 % 2)

        block = (bit(3, 1) + zb) % 2
        c = (bit(2, 0) + za + block) % 2
        e = (block + tc) % 2
        return (1 - e) * (1 - c) + e * ((c + odd + 1) % 2) * early_1

    def stage(m, j, early=None):
        def move(k, q, parts):
            for p in parts:
                stream_copy(m, k, p, core).wait_recv()
            prod[m][k, q] = total(prod[m], recv[m], k, q, parts).astype(jnp.bfloat16)
            stream_copy(m, k, q, partner((j + k) % 4)).start()

        def one(i, carry):
            q = i * 2 ** (j + 1) + 2**j
            parts = [q + 2**b for b in range(j)]
            for k in range(2):
                if early is None:
                    move(k, q, parts)
                else:
                    pl.when(is_early(k, q) == early)(functools.partial(move, k, q, parts))
            return carry

        lax.fori_loop(0, 2 ** (3 - j), one, 0)

    def stage_extra(m, j):
        @pl.when(is_n == 0)
        def _():
            for k in range(2):
                if j < 3:

                    def one(i, carry, k=k):
                        q = i * 2 ** (j + 1) + 2**j
                        parts = [q + 2**b for b in range(j)]
                        for p in parts:
                            extra_copy(m, k, p, core).wait_recv()
                        prox[m][k, q] = total(prox[m], recx[m], k, q, parts).astype(
                            jnp.bfloat16
                        )
                        extra_copy(m, k, q, EXTRA[k][j]).start()
                        return carry

                    lax.fori_loop(0, 2 ** (2 - j), one, 0)
                else:
                    for p in (1, 2, 4):
                        extra_copy(m, k, p, core).wait_recv()

                    @pl.when(apart == 1)
                    def _(k=k):
                        prox[m][k, 0] = total(prox[m], recx[m], k, 0, (1, 2, 4)).astype(
                            jnp.bfloat16
                        )
                        extra_copy(m, k, 0, z_b).start()

    def at(m, block, s):
        width = buf[m].shape[2]
        half = width // 2
        first = pl.multiple_of(block * width + s * half, 128)
        return pl.ds(first, half)

    def last_copy(m, k):
        to = others[k]
        return remote(
            fin[m].at[2 * to[3] + to[4]],
            row[m].at[:, at(m, 2 * tr + tc, side)],
            f_send.at[m, k],
            f_recv.at[m, k],
            to,
        )

    def last_extra(m, k):
        to = others[k]
        return remote(
            finx[m].at[2 * to[3] + to[4]],
            row[m].at[:, at(m, 2 * tr + tc, 1 - c_mine)],
            g_send.at[m, k],
            g_recv.at[m],
            to,
        )

    def turned_copy(m, i, to):
        return remote(
            turn[m].at[i], mir[m].at[kind, y], m_send.at[m, i], m_recv.at[m, kind, y], to
        )

    def by_quarter(m, ref, value, s):
        rows = value.shape[0] // 4
        for i in range(4):
            ref[m][i] = value[i * rows : (i + 1) * rows].astype(jnp.bfloat16)
        row[m][:, at(m, 2 * tr + tc, s)] = ref[m][2 * tr + tc]

    def finish(m):
        parts = (1, 2, 4, 8)
        for k in range(2):
            for p in parts:
                stream_copy(m, k, p, core).wait_recv()
        value = jnp.concatenate(
            [total(prod[m], recv[m], k, 0, parts) for k in range(2)], axis=0
        )
        by_quarter(m, fin, value, side)
        for k in range(3):
            last_copy(m, k).start()

        @pl.when(mirrors == 1)
        def _():
            lanes = turn[m].shape[2]
            tall = value
            if lanes != value.shape[0]:
                fill = jnp.zeros((lanes - value.shape[0], value.shape[1]), jnp.float32)
                tall = jnp.concatenate([value, fill], axis=0)
            turned = tall.T
            rows = turned.shape[0] // 16
            for i, to in quarters():
                turn[m][i] = turned[i * rows : (i + 1) * rows].astype(jnp.bfloat16)
                turned_copy(m, i, to).start()

    def finish_extra(m):
        @pl.when(mirrors == 0)
        def _():
            for k in range(2):
                extra_copy(m, k, 0, core).wait_recv()
            value = jnp.concatenate(
                [total(prox[m], recx[m], k, 0, (1, 2, 4, 0)) for k in range(2)], axis=0
            )
            by_quarter(m, finx, value, 1 - c_mine)
            for k in range(3):
                last_extra(m, k).start()

    def gather_rows(m):
        width = buf[m].shape[2]
        rows = width // 8
        for t in range(3):
            for yy in range(4):
                remote(
                    turn[m].at[0], mir[m].at[t, yy], m_send.at[m, 0], m_recv.at[m, t, yy], core
                ).wait_recv()
            value = jnp.concatenate(
                [mir[m][t, yy].astype(jnp.float32)[:, :rows] for yy in range(4)], axis=1
            )
            chunk = turned_rows[t]
            row[m][:, at(m, chunk // 2, chunk % 2)] = value.astype(jnp.bfloat16)
        for k in range(3):
            last_copy(m, k).wait_recv()

        @pl.when(mirrors == 1)
        def _():
            last_extra(m, 0).wait_recv()

        own_out(m).start()

    def own_out(m):
        return pltpu.make_async_copy(row[m], out[m], o_sem.at[m])

    def products(m, e, first, last):
        def one(c, carry):
            product(m, e, c)
            return carry

        lax.fori_loop(first, last, one, 0)

    def extras(m):
        @pl.when(is_n == 0)
        def _():
            def one(c, carry):
                product_extra(m, c)
                return carry

            lax.fori_loop(0, 2, one, 0)

    step_a = scoped("step_a", step_a)
    step_b = scoped("step_b", step_b)
    products = scoped("products", products)
    extras = scoped("extras", extras)
    stage = scoped("stage", stage)
    stage_extra = scoped("stage_extra", stage_extra)
    finish = scoped("finish", finish)
    finish_extra = scoped("finish_extra", finish_extra)
    gather_rows = scoped("gather_rows", gather_rows)

    for copy in own:
        copy.wait()
    step_a(GRAD, 0)
    products(GRAD, 0, 0, early_0)
    step_b(GRAD, 0)
    products(GRAD, 1, 0, early_1)
    step_a(GRAD, 1)
    products(GRAD, 0, early_0, 2)
    products(GRAD, 1, early_1, 1)
    extras(GRAD)
    stage(GRAD, 1, 1)
    step_b(GRAD, 1)
    products(GRAD, 1, 1, 2)
    step_a(ACT, 0)
    step_a(ACT, 1)
    products(ACT, 0, 0, 2)
    extras(ACT)
    stage(GRAD, 1, 0)
    stage_extra(GRAD, 1)
    step_b(ACT, 0)
    step_b(ACT, 1)
    products(ACT, 1, 0, 2)
    stage(GRAD, 2)
    stage_extra(GRAD, 2)
    stage(ACT, 1)
    stage_extra(ACT, 1)
    stage(GRAD, 3)
    stage_extra(GRAD, 3)
    stage(ACT, 2)
    stage_extra(ACT, 2)
    finish(GRAD)
    finish_extra(GRAD)
    stage(ACT, 3)
    stage_extra(ACT, 3)
    finish(ACT)
    finish_extra(ACT)
    gather_rows(GRAD)
    gather_rows(ACT)

    with jax.named_scope("drain"):
        for i in every:
            along_a(i).wait_send()

        @pl.when(is_n == 1)
        def _():
            for i in every:
                for k in (0, 1):
                    along_b(k, i).wait_send()

        @pl.when(is_n == 0)
        def _():
            for i in every:
                for k in range(4):
                    to_core(k, i).wait_send()
            for m in (ACT, GRAD):
                for k in range(2):
                    for q in range(1, 8):
                        extra_copy(m, k, q, core).wait_send()

                    @pl.when(apart == 1)
                    def _(m=m, k=k):
                        extra_copy(m, k, 0, core).wait_send()

        for m in (ACT, GRAD):
            for k in range(2):
                for q in range(1, 16):
                    stream_copy(m, k, q, core).wait_send()
            for k in range(3):
                last_copy(m, k).wait_send()

            @pl.when(mirrors == 1)
            def _(m=m):
                for i, to in quarters():
                    turned_copy(m, i, to).wait_send()

            @pl.when(mirrors == 0)
            def _(m=m):
                for k in range(3):
                    last_extra(m, k).wait_send()

            own_out(m).wait()


def sums(activations, gradients, rows_a, rows_g):
    tokens = activations.shape[0]
    wide = (activations.shape[1], gradients.shape[1])
    rows = (rows_a, rows_g)
    bf16 = jnp.bfloat16
    lanes = [-(-w // 1024) * 128 for w in wide]
    vmem = [
        *(pltpu.VMEM((6, tokens, w), bf16) for w in wide),
        *(pltpu.VMEM((2, 16, w // 16, w // 2), bf16) for w in wide),
        *(pltpu.VMEM((2, 16, w // 16, w // 2), bf16) for w in wide),
        *(pltpu.VMEM((2, 8, w // 16, w // 2), bf16) for w in wide),
        *(pltpu.VMEM((2, 8, w // 16, w // 2), bf16) for w in wide),
        *(pltpu.VMEM((4, r, w // 2), bf16) for r, w in zip(rows, wide)),
        *(pltpu.VMEM((4, r, w // 2), bf16) for r, w in zip(rows, wide)),
        *(pltpu.VMEM((16, r, n), bf16) for r, n in zip(rows, lanes)),
        *(pltpu.VMEM((3, 4, r, n), bf16) for r, n in zip(rows, lanes)),
        *(pltpu.VMEM((r, 4 * w), bf16) for r, w in zip(rows, wide)),
    ]
    n = len(PIECES)
    dma = pltpu.SemaphoreType.DMA
    sems = [
        dma((2,)), dma((n,)), dma((n,)), dma((2, n)), dma((2, n)), dma((4, n)), dma((4, n)),
        dma((2, 2, 16)), dma((2, 2, 16)), dma((2, 2, 8)), dma((2, 2, 8)),
        dma((2, 3)), dma((2, 3)), dma((2, 3)), dma((2,)),
        dma((2, 16)), dma((2, 3, 4)), dma((2,)),
    ]
    anywhere = pl.BlockSpec(memory_space=pl.ANY)
    return pl.pallas_call(
        kernel,
        out_shape=[jax.ShapeDtypeStruct((r, 4 * w), bf16) for r, w in zip(rows, wide)],
        in_specs=[pl.BlockSpec(memory_space=pltpu.HBM)] * 2,
        out_specs=[anywhere] * 2,
        scratch_shapes=[*vmem, *sems],
        compiler_params=pltpu.CompilerParams(
            collective_id=0, has_side_effects=True, vmem_limit_bytes=53_500_000
        ),
    )(activations, gradients)


def body(activations, gradients, old_inputs, old_gradients):
    tokens_all = activations.shape[0] * lax.axis_size(DP)
    sum_a, sum_g = sums(activations, gradients, old_inputs.shape[0], old_gradients.shape[0])
    scale = 0.5 / tokens_all
    return (
        0.5 * old_inputs + scale * sum_a.astype(jnp.float32),
        0.5 * old_gradients + scale * sum_g.astype(jnp.float32),
    )


def solution(mesh):
    finer = Mesh(mesh.devices.reshape(2, 4, 4, mesh.shape["tr"], mesh.shape["tc"]), AXES)
    return jax.shard_map(
        body,
        mesh=finer,
        in_specs=(P(DP, ("tr", "tc")), P(DP, ("tr", "tc")), P(DP_TR_TC, None), P(DP_TR_TC, None)),
        out_specs=(P(DP_TR_TC, None), P(DP_TR_TC, None)),
        check_vma=False,
    )
```

```python
import functools

import jax
import jax.numpy as jnp
from jax import lax
from jax.experimental import pallas as pl
from jax.experimental.pallas import tpu as pltpu
from jax.sharding import Mesh
from jax.sharding import PartitionSpec as P

MESH = pl.DeviceIdType.MESH
DP = ("dp_0", "dp_1", "dp_2")
DP_TR_TC = ("dp_0", "dp_1", "dp_2", "tr", "tc")
AXES = DP_TR_TC

ACT, GRAD = 0, 1
PIECES = (
    (GRAD, 0, 512, 0),
    (GRAD, 512, 384, 0),
    (GRAD, 0, 512, 1),
    (GRAD, 512, 384, 1),
    (ACT, 0, 512, 0),
    (ACT, 0, 512, 1),
)
AT_ONCE = (0, 1, 2)
AFTER = {1: (3,), 3: (4, 5)}


def pieces_of(m, half):
    return [i for i, p in enumerate(PIECES) if p[0] == m and p[3] == half]


def scoped(name, f):
    def g(*a):
        with jax.named_scope(name + "#" + "_".join(str(x) for x in a if isinstance(x, int))):
            return f(*a)

    return g


def kernel(
    act, grad, out_a, out_g,
    buf_a, buf_g, prod_a, prod_g, recv_a, recv_g, prox_a, prox_g, recx_a, recx_g,
    fin_a, fin_g, finx_a, finx_g, turn_a, turn_g, turx_a, turx_g,
    mir_a, mir_g, mirx_a, mirx_g, row_a, row_g,
    own_sem, a_send, a_recv, b_send, b_recv, d_send, d_recv,
    s_send, s_recv, x_send, x_recv, f_send, f_recv, g_send, g_recv,
    m_send, m_recv, n_send, n_recv, o_sem,
):
    h = lax.axis_index("dp_0")
    z = lax.axis_index("dp_1")
    y = lax.axis_index("dp_2")
    tr = lax.axis_index("tr")
    tc = lax.axis_index("tc")
    is_n = (tr + h) % 2
    odd = (h + tc) % 2
    shift = (is_n * odd, (1 - is_n) * odd + is_n * tc)

    src = (act, grad)
    out = (out_a, out_g)
    buf = (buf_a, buf_g)
    prod = (prod_a, prod_g)
    recv = (recv_a, recv_g)
    prox = (prox_a, prox_g)
    recx = (recx_a, recx_g)
    fin = (fin_a, fin_g)
    finx = (finx_a, finx_g)
    turn = (turn_a, turn_g)
    turx = (turx_a, turx_g)
    mir = (mir_a, mir_g)
    mirx = (mirx_a, mirx_g)
    row = (row_a, row_g)

    def flip1(v):
        return v + 1 - 2 * (v % 2)

    def flip3(v):
        return 3 - v

    x1 = (1 - h, z, y, tr, tc)
    x3 = (1 - h, z, y, tr, 1 - tc)
    core = (h, z, y, 1 - tr, tc)
    others = ((h, z, y, tr, 1 - tc), core, (h, z, y, 1 - tr, 1 - tc))
    y_a, y_b = (h, z, flip1(y), tr, tc), (h, z, flip3(y), tr, tc)
    z_a, z_b = (h, flip1(z), y, tr, tc), (h, flip3(z), y, tr, tc)

    def partner(d):
        f = flip1 if d % 2 == 0 else flip3
        on_y = (1 - tr) if d < 2 else tr
        return (
            h,
            on_y * z + (1 - on_y) * f(z),
            on_y * f(y) + (1 - on_y) * y,
            tr,
            tc,
        )

    half_z = z // 2
    c_mine = z % 2
    apart = (half_z + tc) % 2
    side = (c_mine + apart * shift[1] + (1 - apart) * shift[0]) % 2
    mirrors = 1 - (1 - is_n) * (1 - apart)
    kind = is_n * (1 + apart)
    turned_rows = (
        4 * h + 2 * (1 - half_z) + (c_mine + h + half_z) % 2,
        4 * (1 - h) + 2 * half_z + (c_mine + 1 + h + half_z) % 2,
        4 * (1 - h) + 2 * (1 - half_z) + (c_mine + half_z) % 2,
    )

    def quarters():
        for yy in range(4):
            for aa in range(2):
                for bb in range(2):
                    yield yy * 4 + aa * 2 + bb, (tr, 2 * tc + side, yy, aa, bb)

    barrier = pltpu.get_barrier_semaphore()
    peers = [x1, x3, *others, y_a, y_b, z_a, z_b]

    def greet(peer):
        pl.semaphore_signal(barrier, inc=1, device_id=peer, device_id_type=MESH)

    for peer in peers:
        greet(peer)

    own = [pltpu.make_async_copy(src[m], buf[m].at[0], own_sem.at[m]) for m in (ACT, GRAD)]
    for copy in own:
        copy.start()
    pl.semaphore_wait(barrier, len(peers))

    def cols(i, first):
        m, offset, size, later = PIECES[i]
        start = (first + later) % 2 * (buf[m].shape[2] // 2) + offset
        return pl.ds(pl.multiple_of(start, 128), size)

    def remote(a, b, ss, rs, to):
        return pltpu.make_async_remote_copy(
            src_ref=a, dst_ref=b, send_sem=ss, recv_sem=rs, device_id=to, device_id_type=MESH
        )

    def along_a(i):
        m = PIECES[i][0]
        to = (1 - is_n) * (1 - odd)
        return remote(
            src[m].at[:, cols(i, to)], buf[m].at[1, :, cols(i, to)], a_send.at[m], a_recv.at[i], x1
        )

    def along_b(k, i):
        m = PIECES[i][0]
        part = cols(i, odd)
        source = src[m].at[:, part] if k == 0 else buf[m].at[1, :, part]
        return remote(source, buf[m].at[3 - k, :, part], b_send.at[k, m], b_recv.at[k, i], x3)

    def to_core(k, i):
        m = PIECES[i][0]
        part = cols(i, 0 if k < 2 else odd)
        source = src[m].at[:, part] if k == 0 else buf[m].at[k, :, part]
        slot = k + 4 if k < 2 else k
        return remote(source, buf[m].at[slot, :, part], d_send.at[k, m], d_recv.at[k, i], core)

    every = range(len(PIECES))
    for i in every:
        along_a(i).start()

    @pl.when(is_n == 1)
    def _():
        for i in AT_ONCE:
            along_b(0, i).start()

    @pl.when(is_n == 0)
    def _():
        for i in every:
            to_core(0, i).start()

    def step_a(m, half):
        for i in pieces_of(m, half):
            along_a(i).wait_recv()

            @pl.when(is_n == 1)
            def _(i=i):
                along_b(1, i).start()
                for j in AFTER.get(i, ()):
                    along_b(0, j).start()

            @pl.when(is_n == 0)
            def _(i=i):
                to_core(1, i).start()

        @pl.when(is_n == 1)
        def _():
            for i in pieces_of(m, half):
                to_core(0, i).wait_recv()
                to_core(1, i).wait_recv()

    def step_b(m, half):
        @pl.when(is_n == 0)
        def _():
            for i in pieces_of(m, half):
                along_b(0, i).wait_recv()
                to_core(3, i).start()
            for i in pieces_of(m, half):
                along_b(1, i).wait_recv()
                to_core(2, i).start()

        @pl.when(is_n == 1)
        def _():
            for i in pieces_of(m, half):
                to_core(3, i).wait_recv()
                to_core(2, i).wait_recv()

    zb = z // 2
    za = (z + zb) % 2
    yb = y // 2
    ya = (y + yb) % 2

    def weight(d0, d1, k):
        on0, on1 = 2 ** ((d0 - k) % 4), 2 ** ((d1 - k) % 4)
        return on0 + tr * (on1 - on0)

    def stream_copy(m, k, q, to):
        return remote(
            prod[m].at[k, q], recv[m].at[k, q], s_send.at[m, k], s_recv.at[m, k, q], to
        )

    def lanes_of(m, k):
        tiles = buf[m].shape[2] // 256
        first = (tiles + 1) // 2 * 128
        return pl.ds(0, first) if k == 0 else pl.ds(first, tiles * 128 - first)

    def extra_copy(m, k, q, to):
        return remote(
            prox[m].at[q, :, lanes_of(m, k)],
            recx[m].at[q, :, lanes_of(m, k)],
            x_send.at[m, k],
            x_recv.at[m, k, q],
            to,
        )

    def dot(m, e, c, s):
        half = buf[m].shape[2] // 2
        tokens = 2 * buf[m].shape[1]
        base = e * 2 + (1 - e) * 4 * is_n
        left = buf[m][pl.ds(base, 2), :, pl.ds(pl.multiple_of(c * half, 128), half)]
        right = buf[m][pl.ds(0, 2), :, pl.ds(pl.multiple_of(s * half, 128), half)]
        return lax.dot_general(
            left.reshape(tokens, half),
            right.reshape(tokens, half),
            (((0,), (0,)), ((), ())),
            preferred_element_type=jnp.float32,
        )

    def bits_of(yy):
        return ((yy ^ (yy >> 1)) % 2 + ya) % 2, (yy // 2 + yb) % 2

    def product(m, e, order):
        c = (order + odd) % 2 if e else order
        value = dot(m, e, c, (c + shift[e]) % 2)
        rows = value.shape[0] // 8
        block = (tc + e) % 2
        rza = (c + block + za) % 2
        rzb = (block + zb) % 2
        for yy in range(4):
            rya, ryb = bits_of(yy)
            for k in range(2):
                q = rza * weight(2, 0, k) + rzb * weight(3, 1, k)
                q = q + rya * weight(0, 2, k) + ryb * weight(1, 3, k)
                first = (2 * yy + k) * rows
                prod[m][k, q] = value[first : first + rows].astype(jnp.bfloat16)

                @pl.when(q % 2 == 1)
                def _(k=k, q=q):
                    stream_copy(m, k, q, partner(k)).start()

    EXTRA = ((y_a, y_b, z_a, z_b), (z_b, z_a, y_b, y_a))

    def product_extra(m):
        value = dot(m, 0, 0, 1)
        rows = value.shape[0] // 16
        for yy in range(4):
            rya, ryb = bits_of(yy)
            for zz in range(4):
                rza = ((zz ^ (zz >> 1)) % 2 + za) % 2
                rzb = (zz // 2 + zb) % 2
                first = (4 * yy + zz) * rows
                part = value[first : first + rows].astype(jnp.bfloat16)
                for k in range(2):
                    if k == 0:
                        q = rya + 2 * ryb + 4 * rza + 8 * rzb
                    else:
                        q = rzb + 2 * rza + 4 * ryb + 8 * rya
                    lanes = lanes_of(m, k)
                    prox[m][q, :, lanes] = part[:, lanes.start : lanes.start + lanes.size]

                    @pl.when(q % 2 == 1)
                    def _(k=k, q=q):
                        extra_copy(m, k, q, EXTRA[k][0]).start()

    def total(own_ref, got_ref, k, q, parts):
        value = own_ref[k, q].astype(jnp.float32)
        for p in parts:
            value = value + got_ref[k, p].astype(jnp.float32)
        return value

    early_0 = 1
    early_1 = 1 - is_n * tc

    def is_early(k, q):
        def bit(d0, d1):
            at0, at1 = 2 ** ((d0 - k) % 4), 2 ** ((d1 - k) % 4)
            return (1 - tr) * (q // at0 % 2) + tr * (q // at1 % 2)

        block = (bit(3, 1) + zb) % 2
        c = (bit(2, 0) + za + block) % 2
        e = (block + tc) % 2
        return (1 - e) * (1 - c) + e * ((c + odd + 1) % 2) * early_1

    def stage(m, j, early=None):
        def move(k, q, parts):
            for p in parts:
                stream_copy(m, k, p, core).wait_recv()
            prod[m][k, q] = total(prod[m], recv[m], k, q, parts).astype(jnp.bfloat16)
            stream_copy(m, k, q, partner((j + k) % 4)).start()

        def one(i, carry):
            q = i * 2 ** (j + 1) + 2**j
            parts = [q + 2**b for b in range(j)]
            for k in range(2):
                if early is None:
                    move(k, q, parts)
                else:
                    pl.when(is_early(k, q) == early)(functools.partial(move, k, q, parts))
            return carry

        lax.fori_loop(0, 2 ** (3 - j), one, 0)

    def total_extra(m, k, q, parts):
        for p in parts:
            extra_copy(m, k, p, core).wait_recv()
        value = prox[m][q, :, lanes_of(m, k)].astype(jnp.float32)
        for p in parts:
            value = value + recx[m][p, :, lanes_of(m, k)].astype(jnp.float32)
        return value

    def stage_extra(m, j):
        def one(i, carry):
            q = i * 2 ** (j + 1) + 2**j
            parts = [q + 2**b for b in range(j)]
            for k in range(2):
                prox[m][q, :, lanes_of(m, k)] = total_extra(m, k, q, parts).astype(jnp.bfloat16)
                extra_copy(m, k, q, EXTRA[k][j]).start()
            return carry

        @pl.when(is_n == 0)
        def _():
            lax.fori_loop(0, 2 ** (3 - j), one, 0)

    def at(m, block, s):
        width = buf[m].shape[2]
        half = width // 2
        first = pl.multiple_of(block * width + s * half, 128)
        return pl.ds(first, half)

    def last_copy(m, k):
        to = others[k]
        return remote(
            fin[m].at[2 * to[3] + to[4]],
            row[m].at[:, at(m, 2 * tr + tc, side)],
            f_send.at[m],
            f_recv.at[m, k],
            to,
        )

    extra_to = (h, 2 * tc, y, half_z, c_mine)
    keeps = (1 - is_n) * (1 - apart) * (1 - c_mine) * (1 - tr) * (1 - tc)
    keeps_turned = (1 - is_n) * (1 - apart) * c_mine

    def last_extra(m):
        return remote(
            finx[m], row[m].at[:, at(m, 2 * tr + tc, 1)], g_send.at[m], g_recv.at[m], extra_to
        )

    def turned_extra(m, i):
        to = (h, 2 * tc + 1, i // 4, i // 2 % 2, i % 2)
        return remote(
            turx[m].at[i], mirx[m].at[4 * y + z], n_send.at[m], n_recv.at[m], to
        )

    def is_self(i):
        return keeps_turned * (i == 4 * y + 2 * tr + tc).astype(jnp.int32)

    def turned_copy(m, i, to):
        return remote(
            turn[m].at[i], mir[m].at[kind, y], m_send.at[m], m_recv.at[m, kind], to
        )

    def by_quarter(m, ref, value, s):
        rows = value.shape[0] // 4
        for i in range(4):
            ref[m][i] = value[i * rows : (i + 1) * rows].astype(jnp.bfloat16)
        row[m][:, at(m, 2 * tr + tc, s)] = ref[m][2 * tr + tc]

    def finish(m):
        parts = (1, 2, 4, 8)
        for k in range(2):
            for p in parts:
                stream_copy(m, k, p, core).wait_recv()
        value = jnp.concatenate(
            [total(prod[m], recv[m], k, 0, parts) for k in range(2)], axis=0
        )
        by_quarter(m, fin, value, side)
        for k in range(3):
            last_copy(m, k).start()

        @pl.when(mirrors == 1)
        def _():
            lanes = turn[m].shape[2]
            tall = value
            if lanes != value.shape[0]:
                fill = jnp.zeros((lanes - value.shape[0], value.shape[1]), jnp.float32)
                tall = jnp.concatenate([value, fill], axis=0)
            turned = tall.T
            rows = turned.shape[0] // 16
            for i, to in quarters():
                turn[m][i] = turned[i * rows : (i + 1) * rows].astype(jnp.bfloat16)
                turned_copy(m, i, to).start()

    def finish_extra(m):
        @pl.when(is_n == 0)
        def _():
            value = jnp.concatenate(
                [total_extra(m, k, 0, (1, 2, 4, 8)) for k in range(2)], axis=1
            )
            finx[m][...] = value.astype(jnp.bfloat16)

            @pl.when(keeps == 0)
            def _():
                last_extra(m).start()

            @pl.when(keeps == 1)
            def _():
                row[m][:, at(m, 2 * tr + tc, 1)] = finx[m][...]

            rows = value.shape[0]
            fill = jnp.zeros((128 - rows, value.shape[1]), jnp.float32)
            turned = jnp.concatenate([value, fill], axis=0).T
            for i in range(16):
                turx[m][i] = turned[i * rows : (i + 1) * rows].astype(jnp.bfloat16)

                @pl.when(is_self(i) == 0)
                def _(i=i):
                    turned_extra(m, i).start()

                @pl.when(is_self(i) == 1)
                def _(i=i):
                    mirx[m][4 * y + z] = turx[m][i]

    def gather_rows(m):
        width = buf[m].shape[2]
        rows = width // 8
        for t in range(3):
            pieces = mir[m].at[t]
            remote(pieces, pieces, m_send.at[m], m_recv.at[m, t], core).wait_recv()
            value = jnp.concatenate(
                [mir[m][t, yy].astype(jnp.float32)[:, :rows] for yy in range(4)], axis=1
            )
            chunk = turned_rows[t]
            row[m][:, at(m, chunk // 2, chunk % 2)] = value.astype(jnp.bfloat16)
        for k in range(3):
            last_copy(m, k).wait_recv()

        @pl.when(c_mine * (1 - keeps) + (1 - c_mine) * keeps == 0)
        def _():
            last_extra(m).wait_recv()

        @pl.when(c_mine == 1)
        def _():
            rows = width // 32
            for count in (15, 16):

                @pl.when(keeps_turned == 16 - count)
                def _(count=count):
                    pieces = mirx[m].at[pl.ds(0, count)]
                    remote(pieces, pieces, n_send.at[m], n_recv.at[m], core).wait_recv()

            value = jnp.concatenate(
                [mirx[m][i].astype(jnp.float32)[:, :rows] for i in range(16)], axis=1
            )
            row[m][:, at(m, 2 * h + half_z, 0)] = value.astype(jnp.bfloat16)

        own_out(m).start()

    def own_out(m):
        return pltpu.make_async_copy(row[m], out[m], o_sem.at[m])

    def products(m, e, first, last):
        def one(c, carry):
            product(m, e, c)
            return carry

        lax.fori_loop(first, last, one, 0)

    def extras(m):
        @pl.when(is_n == 0)
        def _():
            product_extra(m)

    step_a = scoped("step_a", step_a)
    step_b = scoped("step_b", step_b)
    products = scoped("products", products)
    extras = scoped("extras", extras)
    stage = scoped("stage", stage)
    stage_extra = scoped("stage_extra", stage_extra)
    finish = scoped("finish", finish)
    finish_extra = scoped("finish_extra", finish_extra)
    gather_rows = scoped("gather_rows", gather_rows)

    for copy in own:
        copy.wait()
    step_a(GRAD, 0)
    products(GRAD, 0, 0, early_0)
    step_b(GRAD, 0)
    products(GRAD, 1, 0, early_1)
    step_a(GRAD, 1)
    products(GRAD, 0, early_0, 2)
    products(GRAD, 1, early_1, 1)
    extras(GRAD)
    stage(GRAD, 1, 1)
    step_b(GRAD, 1)
    products(GRAD, 1, 1, 2)
    step_a(ACT, 0)
    step_a(ACT, 1)
    products(ACT, 0, 0, 2)
    extras(ACT)
    stage(GRAD, 1, 0)
    stage_extra(GRAD, 1)
    step_b(ACT, 0)
    step_b(ACT, 1)
    products(ACT, 1, 0, 2)
    stage(GRAD, 2)
    stage_extra(GRAD, 2)
    stage(ACT, 1)
    stage_extra(ACT, 1)
    stage(GRAD, 3)
    stage_extra(GRAD, 3)
    finish(GRAD)
    stage(ACT, 2)
    stage_extra(ACT, 2)
    finish_extra(GRAD)
    stage(ACT, 3)
    stage_extra(ACT, 3)
    finish(ACT)
    finish_extra(ACT)
    gather_rows(GRAD)
    gather_rows(ACT)

    with jax.named_scope("drain"):
        def sent(ref, sem):
            pltpu.make_async_copy(ref, ref, sem).wait()

        for m in (ACT, GRAD):
            block = buf[m].at[1]
            sent(block, a_send.at[m])

            @pl.when(is_n == 1)
            def _(m=m, block=block):
                for k in (0, 1):
                    sent(block, b_send.at[k, m])

            @pl.when(is_n == 0)
            def _(m=m, block=block):
                for k in range(4):
                    sent(block, d_send.at[k, m])
                for k in range(2):
                    sent(prox[m].at[pl.ds(1, 15), :, lanes_of(m, k)], x_send.at[m, k])

                @pl.when(keeps == 0)
                def _():
                    last_extra(m).wait_send()

                for count in (15, 16):

                    @pl.when(keeps_turned == 16 - count)
                    def _(count=count):
                        sent(turx[m].at[pl.ds(0, count)], n_send.at[m])

            for k in range(2):
                sent(prod[m].at[k, pl.ds(1, 15)], s_send.at[m, k])
            sent(fin[m].at[pl.ds(0, 3)], f_send.at[m])

            @pl.when(mirrors == 1)
            def _(m=m):
                sent(turn[m], m_send.at[m])

            own_out(m).wait()


def sums(activations, gradients, rows_a, rows_g):
    tokens = activations.shape[0]
    wide = (activations.shape[1], gradients.shape[1])
    rows = (rows_a, rows_g)
    bf16 = jnp.bfloat16
    lanes = [-(-w // 1024) * 128 for w in wide]
    vmem = [
        *(pltpu.VMEM((6, tokens, w), bf16) for w in wide),
        *(pltpu.VMEM((2, 16, w // 16, w // 2), bf16) for w in wide),
        *(pltpu.VMEM((2, 16, w // 16, w // 2), bf16) for w in wide),
        *(pltpu.VMEM((16, r, w // 2), bf16) for r, w in zip(rows, wide)),
        *(pltpu.VMEM((16, r, w // 2), bf16) for r, w in zip(rows, wide)),
        *(pltpu.VMEM((4, r, w // 2), bf16) for r, w in zip(rows, wide)),
        *(pltpu.VMEM((r, w // 2), bf16) for r, w in zip(rows, wide)),
        *(pltpu.VMEM((16, r, n), bf16) for r, n in zip(rows, lanes)),
        *(pltpu.VMEM((16, r, 128), bf16) for r in rows),
        *(pltpu.VMEM((3, 4, r, n), bf16) for r, n in zip(rows, lanes)),
        *(pltpu.VMEM((16, r, 128), bf16) for r in rows),
        *(pltpu.VMEM((r, 4 * w), bf16) for r, w in zip(rows, wide)),
    ]
    n = len(PIECES)
    dma = pltpu.SemaphoreType.DMA
    sems = [
        dma((2,)), dma((2,)), dma((n,)), dma((2, 2)), dma((2, n)), dma((4, 2)), dma((4, n)),
        dma((2, 2)), dma((2, 2, 16)), dma((2, 2)), dma((2, 2, 16)),
        dma((2,)), dma((2, 3)), dma((2,)), dma((2,)),
        dma((2,)), dma((2, 3)), dma((2,)), dma((2,)), dma((2,)),
    ]
    anywhere = pl.BlockSpec(memory_space=pl.ANY)
    return pl.pallas_call(
        kernel,
        out_shape=[jax.ShapeDtypeStruct((r, 4 * w), bf16) for r, w in zip(rows, wide)],
        in_specs=[pl.BlockSpec(memory_space=pltpu.HBM)] * 2,
        out_specs=[anywhere] * 2,
        scratch_shapes=[*vmem, *sems],
        compiler_params=pltpu.CompilerParams(
            collective_id=0, has_side_effects=True, vmem_limit_bytes=54_800_000
        ),
    )(activations, gradients)


def body(activations, gradients, old_inputs, old_gradients):
    tokens_all = activations.shape[0] * lax.axis_size(DP)
    sum_a, sum_g = sums(activations, gradients, old_inputs.shape[0], old_gradients.shape[0])
    scale = 0.5 / tokens_all
    return (
        0.5 * old_inputs + scale * sum_a.astype(jnp.float32),
        0.5 * old_gradients + scale * sum_g.astype(jnp.float32),
    )


def solution(mesh):
    finer = Mesh(mesh.devices.reshape(2, 4, 4, mesh.shape["tr"], mesh.shape["tc"]), AXES)
    return jax.shard_map(
        body,
        mesh=finer,
        in_specs=(P(DP, ("tr", "tc")), P(DP, ("tr", "tc")), P(DP_TR_TC, None), P(DP_TR_TC, None)),
        out_specs=(P(DP_TR_TC, None), P(DP_TR_TC, None)),
        check_vma=False,
    )
```

```python
import functools

import jax
import jax.numpy as jnp
from jax import lax
from jax.experimental import pallas as pl
from jax.experimental.pallas import tpu as pltpu
from jax.sharding import Mesh
from jax.sharding import PartitionSpec as P

MESH = pl.DeviceIdType.MESH
DP = ("dp_0", "dp_1", "dp_2")
DP_TR_TC = ("dp_0", "dp_1", "dp_2", "tr", "tc")
AXES = DP_TR_TC

ACT, GRAD = 0, 1
PIECES = (
    (GRAD, 0, 512, 0),
    (GRAD, 512, 384, 0),
    (GRAD, 0, 384, 1),
    (GRAD, 384, 256, 1),
    (GRAD, 640, 256, 1),
    (ACT, 0, 512, 0),
    (ACT, 0, 512, 1),
)
AT_ONCE = (0, 1, 2)
AFTER = {1: (3, 4), 4: (5, 6)}


def pieces_of(m, half):
    return [i for i, p in enumerate(PIECES) if p[0] == m and p[3] == half]


def scoped(name, f):
    def g(*a):
        with jax.named_scope(name + "#" + "_".join(str(x) for x in a if isinstance(x, int))):
            return f(*a)

    return g


def kernel(
    act, grad, out_a, out_g,
    buf_a, buf_g, prod_a, prod_g, recv_a, recv_g, prox_a, prox_g, recx_a, recx_g,
    fin_a, fin_g, finx_a, finx_g, turn_a, turn_g, turx_a, turx_g,
    mir_a, mir_g, mirx_a, mirx_g, row_a, row_g,
    own_sem, a_send, a_recv, b_send, b_recv, d_send, d_recv,
    s_send, s_recv, x_send, x_recv, f_send, f_recv, g_send, g_recv,
    m_send, m_recv, n_send, n_recv, o_sem,
):
    h = lax.axis_index("dp_0")
    z = lax.axis_index("dp_1")
    y = lax.axis_index("dp_2")
    tr = lax.axis_index("tr")
    tc = lax.axis_index("tc")
    is_n = (tr + h) % 2
    odd = (h + tc) % 2
    shift = (is_n * odd, (1 - is_n) * odd + is_n * h)

    src = (act, grad)
    out = (out_a, out_g)
    buf = (buf_a, buf_g)
    prod = (prod_a, prod_g)
    recv = (recv_a, recv_g)
    prox = (prox_a, prox_g)
    recx = (recx_a, recx_g)
    fin = (fin_a, fin_g)
    finx = (finx_a, finx_g)
    turn = (turn_a, turn_g)
    turx = (turx_a, turx_g)
    mir = (mir_a, mir_g)
    mirx = (mirx_a, mirx_g)
    row = (row_a, row_g)

    def flip1(v):
        return v + 1 - 2 * (v % 2)

    def flip3(v):
        return 3 - v

    x1 = (1 - h, z, y, tr, tc)
    x3 = (1 - h, z, y, tr, 1 - tc)
    core = (h, z, y, 1 - tr, tc)
    others = ((h, z, y, tr, 1 - tc), core, (h, z, y, 1 - tr, 1 - tc))
    y_a, y_b = (h, z, flip1(y), tr, tc), (h, z, flip3(y), tr, tc)
    z_a, z_b = (h, flip1(z), y, tr, tc), (h, flip3(z), y, tr, tc)

    def partner(d):
        f = flip1 if d % 2 == 0 else flip3
        on_y = is_n if d < 2 else 1 - is_n
        return (
            h,
            on_y * z + (1 - on_y) * f(z),
            on_y * f(y) + (1 - on_y) * y,
            tr,
            tc,
        )

    half_z = z // 2
    c_mine = z % 2
    apart = (half_z + tc) % 2
    side = (c_mine + apart * shift[1] + (1 - apart) * shift[0]) % 2
    mirrors = 1 - (1 - is_n) * (1 - apart)
    kind = is_n * (1 + apart)
    turned_rows = (
        4 * h + 2 * (1 - half_z) + (c_mine + h + half_z) % 2,
        4 * (1 - h) + 2 * half_z + (c_mine + 1 + h + half_z) % 2,
        4 * (1 - h) + 2 * (1 - half_z) + (c_mine + 1 + h) % 2,
    )

    def quarters():
        for yy in range(4):
            for aa in range(2):
                for bb in range(2):
                    yield yy * 4 + aa * 2 + bb, (tr, 2 * tc + side, yy, aa, bb)

    barrier = pltpu.get_barrier_semaphore()
    peers = [x1, x3, *others, y_a, y_b, z_a, z_b]

    def greet(peer):
        pl.semaphore_signal(barrier, inc=1, device_id=peer, device_id_type=MESH)

    for peer in peers:
        greet(peer)

    own = [pltpu.make_async_copy(src[m], buf[m].at[0], own_sem.at[m]) for m in (ACT, GRAD)]
    for copy in own:
        copy.start()
    pl.semaphore_wait(barrier, len(peers))

    def cols(i, first):
        m, offset, size, later = PIECES[i]
        start = (first + later) % 2 * (buf[m].shape[2] // 2) + offset
        return pl.ds(pl.multiple_of(start, 128), size)

    def remote(a, b, ss, rs, to):
        return pltpu.make_async_remote_copy(
            src_ref=a, dst_ref=b, send_sem=ss, recv_sem=rs, device_id=to, device_id_type=MESH
        )

    def along_a(i):
        m = PIECES[i][0]
        to = (1 - is_n) * (1 - odd)
        return remote(
            src[m].at[:, cols(i, to)], buf[m].at[1, :, cols(i, to)], a_send.at[m], a_recv.at[i], x1
        )

    def along_b(k, i):
        m = PIECES[i][0]
        part = cols(i, odd)
        source = src[m].at[:, part] if k == 0 else buf[m].at[1, :, part]
        return remote(source, buf[m].at[3 - k, :, part], b_send.at[k, m], b_recv.at[k, i], x3)

    def to_core(k, i):
        m = PIECES[i][0]
        part = cols(i, 0 if k < 2 else odd)
        source = src[m].at[:, part] if k == 0 else buf[m].at[k, :, part]
        slot = k + 4 if k < 2 else k
        return remote(source, buf[m].at[slot, :, part], d_send.at[k, m], d_recv.at[k, i], core)

    every = range(len(PIECES))
    for i in every:
        along_a(i).start()

    @pl.when(is_n == 1)
    def _():
        for i in AT_ONCE:
            along_b(0, i).start()

    @pl.when(is_n == 0)
    def _():
        for i in every:
            to_core(0, i).start()

    def step_a(m, half):
        for i in pieces_of(m, half):
            along_a(i).wait_recv()

            @pl.when(is_n == 1)
            def _(i=i):
                along_b(1, i).start()
                for j in AFTER.get(i, ()):
                    along_b(0, j).start()

            @pl.when(is_n == 0)
            def _(i=i):
                to_core(1, i).start()

        @pl.when(is_n == 1)
        def _():
            for i in pieces_of(m, half):
                to_core(0, i).wait_recv()
                to_core(1, i).wait_recv()

    def step_b(m, half):
        @pl.when(is_n == 0)
        def _():
            for i in pieces_of(m, half):
                along_b(0, i).wait_recv()
                to_core(3, i).start()
            for i in pieces_of(m, half):
                along_b(1, i).wait_recv()
                to_core(2, i).start()

        @pl.when(is_n == 1)
        def _():
            for i in pieces_of(m, half):
                to_core(3, i).wait_recv()
                to_core(2, i).wait_recv()

    zb = z // 2
    za = (z + zb) % 2
    yb = y // 2
    ya = (y + yb) % 2

    def weight(d0, d1, k):
        on0, on1 = 2 ** ((d0 - k) % 4), 2 ** ((d1 - k) % 4)
        return on0 + (1 - is_n) * (on1 - on0)

    def stream_copy(m, k, q, to):
        return remote(
            prod[m].at[k, q], recv[m].at[k, q], s_send.at[m, k], s_recv.at[m, k, q], to
        )

    def lanes_of(m, k):
        tiles = buf[m].shape[2] // 256
        first = (tiles + 1) // 2 * 128
        return pl.ds(0, first) if k == 0 else pl.ds(first, tiles * 128 - first)

    def extra_copy(m, k, q, to):
        return remote(
            prox[m].at[q, :, lanes_of(m, k)],
            recx[m].at[q, :, lanes_of(m, k)],
            x_send.at[m, k],
            x_recv.at[m, k, q],
            to,
        )

    def dot(m, e, c, s):
        half = buf[m].shape[2] // 2
        tokens = 2 * buf[m].shape[1]
        base = e * 2 + (1 - e) * 4 * is_n
        left = buf[m][pl.ds(base, 2), :, pl.ds(pl.multiple_of(c * half, 128), half)]
        right = buf[m][pl.ds(0, 2), :, pl.ds(pl.multiple_of(s * half, 128), half)]
        return lax.dot_general(
            left.reshape(tokens, half),
            right.reshape(tokens, half),
            (((0,), (0,)), ((), ())),
            preferred_element_type=jnp.float32,
        )

    def bits_of(yy):
        return ((yy ^ (yy >> 1)) % 2 + ya) % 2, (yy // 2 + yb) % 2

    def product(m, e, order):
        c = (order + odd) % 2 if e else order
        value = dot(m, e, c, (c + shift[e]) % 2)
        rows = value.shape[0] // 8
        block = (tc + e) % 2
        rza = (c + block + za) % 2
        rzb = (block + zb) % 2
        for yy in range(4):
            rya, ryb = bits_of(yy)
            for k in range(2):
                q = rza * weight(2, 0, k) + rzb * weight(3, 1, k)
                q = q + rya * weight(0, 2, k) + ryb * weight(1, 3, k)
                first = (2 * yy + k) * rows
                prod[m][k, q] = value[first : first + rows].astype(jnp.bfloat16)

                @pl.when(q % 2 == 1)
                def _(k=k, q=q):
                    stream_copy(m, k, q, partner(k)).start()

    EXTRA = ((y_a, y_b, z_a, z_b), (z_b, z_a, y_b, y_a))

    def product_extra(m):
        value = dot(m, 0, 0, 1)
        rows = value.shape[0] // 16
        for yy in range(4):
            rya, ryb = bits_of(yy)
            for zz in range(4):
                rza = ((zz ^ (zz >> 1)) % 2 + za) % 2
                rzb = (zz // 2 + zb) % 2
                first = (4 * yy + zz) * rows
                part = value[first : first + rows].astype(jnp.bfloat16)
                for k in range(2):
                    if k == 0:
                        q = rya + 2 * ryb + 4 * rza + 8 * rzb
                    else:
                        q = rzb + 2 * rza + 4 * ryb + 8 * rya
                    lanes = lanes_of(m, k)
                    prox[m][q, :, lanes] = part[:, lanes.start : lanes.start + lanes.size]

                    @pl.when(q % 2 == 1)
                    def _(k=k, q=q):
                        extra_copy(m, k, q, EXTRA[k][0]).start()

    def total(own_ref, got_ref, k, q, parts):
        value = own_ref[k, q].astype(jnp.float32)
        for p in parts:
            value = value + got_ref[k, p].astype(jnp.float32)
        return value

    early_0 = 1
    early_1 = 1 - is_n * h

    def group_of(k, q):
        def bit(d0, d1):
            at0, at1 = 2 ** ((d0 - k) % 4), 2 ** ((d1 - k) % 4)
            return is_n * (q // at0 % 2) + (1 - is_n) * (q // at1 % 2)

        block = (bit(3, 1) + zb) % 2
        c = (bit(2, 0) + za + block) % 2
        e = (block + tc) % 2
        second = (c + odd) % 2
        return (1 - e) * c + e * (2 * second + (1 - second) * (1 - early_1))

    def stage(m, j, group=None):
        def move(k, q, parts):
            for p in parts:
                stream_copy(m, k, p, core).wait_recv()
            prod[m][k, q] = total(prod[m], recv[m], k, q, parts).astype(jnp.bfloat16)
            stream_copy(m, k, q, partner((j + k) % 4)).start()

        def one(i, carry):
            q = i * 2 ** (j + 1) + 2**j
            parts = [q + 2**b for b in range(j)]
            for k in range(2):
                if group is None:
                    move(k, q, parts)
                else:
                    pl.when(group_of(k, q) == group)(functools.partial(move, k, q, parts))
            return carry

        lax.fori_loop(0, 2 ** (3 - j), one, 0)

    def total_extra(m, k, q, parts):
        for p in parts:
            extra_copy(m, k, p, core).wait_recv()
        value = prox[m][q, :, lanes_of(m, k)].astype(jnp.float32)
        for p in parts:
            value = value + recx[m][p, :, lanes_of(m, k)].astype(jnp.float32)
        return value

    def stage_extra(m, j):
        def one(i, carry):
            q = i * 2 ** (j + 1) + 2**j
            parts = [q + 2**b for b in range(j)]
            for k in range(2):
                prox[m][q, :, lanes_of(m, k)] = total_extra(m, k, q, parts).astype(jnp.bfloat16)
                extra_copy(m, k, q, EXTRA[k][j]).start()
            return carry

        @pl.when(is_n == 0)
        def _():
            lax.fori_loop(0, 2 ** (3 - j), one, 0)

    def at(m, block, s):
        width = buf[m].shape[2]
        half = width // 2
        first = pl.multiple_of(block * width + s * half, 128)
        return pl.ds(first, half)

    def last_copy(m, k):
        to = others[k]
        return remote(
            fin[m].at[2 * to[3] + to[4]],
            row[m].at[:, at(m, 2 * tr + tc, side)],
            f_send.at[m],
            f_recv.at[m, k],
            to,
        )

    extra_to = (h, 2 * tc, y, half_z, c_mine)
    keeps = (1 - is_n) * (1 - apart) * (1 - c_mine) * (1 - tr) * (1 - tc)
    keeps_turned = (1 - is_n) * (1 - apart) * c_mine

    def last_extra(m):
        return remote(
            finx[m], row[m].at[:, at(m, 2 * tr + tc, 1)], g_send.at[m], g_recv.at[m], extra_to
        )

    def turned_extra(m, i):
        to = (h, 2 * tc + 1, i // 4, i // 2 % 2, i % 2)
        return remote(
            turx[m].at[i], mirx[m].at[4 * y + z], n_send.at[m], n_recv.at[m], to
        )

    def is_self(i):
        return keeps_turned * (i == 4 * y + 2 * tr + tc).astype(jnp.int32)

    def turned_copy(m, i, to):
        return remote(
            turn[m].at[i], mir[m].at[kind, y], m_send.at[m], m_recv.at[m, kind], to
        )

    def by_quarter(m, ref, value, s):
        rows = value.shape[0] // 4
        for i in range(4):
            ref[m][i] = value[i * rows : (i + 1) * rows].astype(jnp.bfloat16)
        row[m][:, at(m, 2 * tr + tc, s)] = ref[m][2 * tr + tc]

    def finish(m):
        parts = (1, 2, 4, 8)
        for k in range(2):
            for p in parts:
                stream_copy(m, k, p, core).wait_recv()
        value = jnp.concatenate(
            [total(prod[m], recv[m], k, 0, parts) for k in range(2)], axis=0
        )
        by_quarter(m, fin, value, side)
        for k in range(3):
            last_copy(m, k).start()

        @pl.when(mirrors == 1)
        def _():
            lanes = turn[m].shape[2]
            tall = value
            if lanes != value.shape[0]:
                fill = jnp.zeros((lanes - value.shape[0], value.shape[1]), jnp.float32)
                tall = jnp.concatenate([value, fill], axis=0)
            turned = tall.T
            rows = turned.shape[0] // 16
            for i, to in quarters():
                turn[m][i] = turned[i * rows : (i + 1) * rows].astype(jnp.bfloat16)

    def send_turned(m):
        @pl.when(mirrors == 1)
        def _():
            for i, to in quarters():
                turned_copy(m, i, to).start()

    def finish_extra(m):
        @pl.when(is_n == 0)
        def _():
            value = jnp.concatenate(
                [total_extra(m, k, 0, (1, 2, 4, 8)) for k in range(2)], axis=1
            )
            finx[m][...] = value.astype(jnp.bfloat16)

            @pl.when(keeps == 0)
            def _():
                last_extra(m).start()

            @pl.when(keeps == 1)
            def _():
                row[m][:, at(m, 2 * tr + tc, 1)] = finx[m][...]

            rows = value.shape[0]
            fill = jnp.zeros((128 - rows, value.shape[1]), jnp.float32)
            turned = jnp.concatenate([value, fill], axis=0).T
            for i in range(16):
                turx[m][i] = turned[i * rows : (i + 1) * rows].astype(jnp.bfloat16)

                @pl.when(is_self(i) == 0)
                def _(i=i):
                    turned_extra(m, i).start()

                @pl.when(is_self(i) == 1)
                def _(i=i):
                    mirx[m][4 * y + z] = turx[m][i]

    def gather_rows(m):
        width = buf[m].shape[2]
        rows = width // 8
        for t in range(3):
            pieces = mir[m].at[t]
            remote(pieces, pieces, m_send.at[m], m_recv.at[m, t], core).wait_recv()
            value = jnp.concatenate(
                [mir[m][t, yy].astype(jnp.float32)[:, :rows] for yy in range(4)], axis=1
            )
            chunk = turned_rows[t]
            row[m][:, at(m, chunk // 2, chunk % 2)] = value.astype(jnp.bfloat16)
        for k in range(3):
            last_copy(m, k).wait_recv()

        @pl.when(c_mine * (1 - keeps) + (1 - c_mine) * keeps == 0)
        def _():
            last_extra(m).wait_recv()

        @pl.when(c_mine == 1)
        def _():
            rows = width // 32
            for count in (15, 16):

                @pl.when(keeps_turned == 16 - count)
                def _(count=count):
                    pieces = mirx[m].at[pl.ds(0, count)]
                    remote(pieces, pieces, n_send.at[m], n_recv.at[m], core).wait_recv()

            value = jnp.concatenate(
                [mirx[m][i].astype(jnp.float32)[:, :rows] for i in range(16)], axis=1
            )
            row[m][:, at(m, 2 * h + half_z, 0)] = value.astype(jnp.bfloat16)

        own_out(m).start()

    def own_out(m):
        return pltpu.make_async_copy(row[m], out[m], o_sem.at[m])

    def products(m, e, first, last):
        def one(c, carry):
            product(m, e, c)
            return carry

        lax.fori_loop(first, last, one, 0)

    def extras(m):
        @pl.when(is_n == 0)
        def _():
            product_extra(m)

    step_a = scoped("step_a", step_a)
    step_b = scoped("step_b", step_b)
    products = scoped("products", products)
    extras = scoped("extras", extras)
    stage = scoped("stage", stage)
    stage_extra = scoped("stage_extra", stage_extra)
    finish = scoped("finish", finish)
    finish_extra = scoped("finish_extra", finish_extra)
    gather_rows = scoped("gather_rows", gather_rows)
    send_turned = scoped("send_turned", send_turned)

    for copy in own:
        copy.wait()
    step_a(GRAD, 0)
    products(GRAD, 0, 0, early_0)
    step_b(GRAD, 0)
    products(GRAD, 1, 0, early_1)
    step_a(GRAD, 1)
    products(GRAD, 0, early_0, 2)
    products(GRAD, 1, early_1, 1)
    extras(GRAD)
    stage(GRAD, 1, 0)
    step_b(GRAD, 1)
    products(GRAD, 1, 1, 2)
    step_a(ACT, 0)
    products(ACT, 0, 0, 1)
    stage(GRAD, 1, 1)
    stage_extra(GRAD, 1)
    step_a(ACT, 1)
    products(ACT, 0, 1, 2)
    extras(ACT)
    stage(GRAD, 1, 2)
    step_b(ACT, 0)
    step_b(ACT, 1)
    products(ACT, 1, 0, 2)
    stage(GRAD, 2)
    stage_extra(GRAD, 2)
    stage(ACT, 1)
    stage_extra(ACT, 1)
    stage(GRAD, 3)
    stage_extra(GRAD, 3)
    stage(ACT, 2)
    stage_extra(ACT, 2)
    finish(GRAD)
    stage(ACT, 3)
    stage_extra(ACT, 3)
    send_turned(GRAD)
    finish_extra(GRAD)
    finish(ACT)
    send_turned(ACT)
    finish_extra(ACT)
    gather_rows(GRAD)
    gather_rows(ACT)

    with jax.named_scope("drain"):
        def sent(ref, sem):
            pltpu.make_async_copy(ref, ref, sem).wait()

        for m in (ACT, GRAD):
            block = buf[m].at[1]
            sent(block, a_send.at[m])

            @pl.when(is_n == 1)
            def _(m=m, block=block):
                for k in (0, 1):
                    sent(block, b_send.at[k, m])

            @pl.when(is_n == 0)
            def _(m=m, block=block):
                for k in range(4):
                    sent(block, d_send.at[k, m])
                for k in range(2):
                    sent(prox[m].at[pl.ds(1, 15), :, lanes_of(m, k)], x_send.at[m, k])

                @pl.when(keeps == 0)
                def _():
                    last_extra(m).wait_send()

                for count in (15, 16):

                    @pl.when(keeps_turned == 16 - count)
                    def _(count=count):
                        sent(turx[m].at[pl.ds(0, count)], n_send.at[m])

            for k in range(2):
                sent(prod[m].at[k, pl.ds(1, 15)], s_send.at[m, k])
            sent(fin[m].at[pl.ds(0, 3)], f_send.at[m])

            @pl.when(mirrors == 1)
            def _(m=m):
                sent(turn[m], m_send.at[m])

            own_out(m).wait()


def sums(activations, gradients, rows_a, rows_g):
    tokens = activations.shape[0]
    wide = (activations.shape[1], gradients.shape[1])
    rows = (rows_a, rows_g)
    bf16 = jnp.bfloat16
    lanes = [-(-w // 1024) * 128 for w in wide]
    vmem = [
        *(pltpu.VMEM((6, tokens, w), bf16) for w in wide),
        *(pltpu.VMEM((2, 16, w // 16, w // 2), bf16) for w in wide),
        *(pltpu.VMEM((2, 16, w // 16, w // 2), bf16) for w in wide),
        *(pltpu.VMEM((16, r, w // 2), bf16) for r, w in zip(rows, wide)),
        *(pltpu.VMEM((16, r, w // 2), bf16) for r, w in zip(rows, wide)),
        *(pltpu.VMEM((4, r, w // 2), bf16) for r, w in zip(rows, wide)),
        *(pltpu.VMEM((r, w // 2), bf16) for r, w in zip(rows, wide)),
        *(pltpu.VMEM((16, r, n), bf16) for r, n in zip(rows, lanes)),
        *(pltpu.VMEM((16, r, 128), bf16) for r in rows),
        *(pltpu.VMEM((3, 4, r, n), bf16) for r, n in zip(rows, lanes)),
        *(pltpu.VMEM((16, r, 128), bf16) for r in rows),
        *(pltpu.VMEM((r, 4 * w), bf16) for r, w in zip(rows, wide)),
    ]
    n = len(PIECES)
    dma = pltpu.SemaphoreType.DMA
    sems = [
        dma((2,)), dma((2,)), dma((n,)), dma((2, 2)), dma((2, n)), dma((4, 2)), dma((4, n)),
        dma((2, 2)), dma((2, 2, 16)), dma((2, 2)), dma((2, 2, 16)),
        dma((2,)), dma((2, 3)), dma((2,)), dma((2,)),
        dma((2,)), dma((2, 3)), dma((2,)), dma((2,)), dma((2,)),
    ]
    anywhere = pl.BlockSpec(memory_space=pl.ANY)
    return pl.pallas_call(
        kernel,
        out_shape=[jax.ShapeDtypeStruct((r, 4 * w), bf16) for r, w in zip(rows, wide)],
        in_specs=[pl.BlockSpec(memory_space=pltpu.HBM)] * 2,
        out_specs=[anywhere] * 2,
        scratch_shapes=[*vmem, *sems],
        compiler_params=pltpu.CompilerParams(
            collective_id=0, has_side_effects=True, vmem_limit_bytes=54_800_000
        ),
    )(activations, gradients)


def body(activations, gradients, old_inputs, old_gradients):
    tokens_all = activations.shape[0] * lax.axis_size(DP)
    sum_a, sum_g = sums(activations, gradients, old_inputs.shape[0], old_gradients.shape[0])
    scale = 0.5 / tokens_all
    return (
        0.5 * old_inputs + scale * sum_a.astype(jnp.float32),
        0.5 * old_gradients + scale * sum_g.astype(jnp.float32),
    )


def solution(mesh):
    finer = Mesh(mesh.devices.reshape(2, 4, 4, mesh.shape["tr"], mesh.shape["tc"]), AXES)
    return jax.shard_map(
        body,
        mesh=finer,
        in_specs=(P(DP, ("tr", "tc")), P(DP, ("tr", "tc")), P(DP_TR_TC, None), P(DP_TR_TC, None)),
        out_specs=(P(DP_TR_TC, None), P(DP_TR_TC, None)),
        check_vma=False,
    )
```

```python
import functools

import jax
import jax.numpy as jnp
from jax import lax
from jax.experimental import pallas as pl
from jax.experimental.pallas import tpu as pltpu
from jax.sharding import Mesh
from jax.sharding import PartitionSpec as P

MESH = pl.DeviceIdType.MESH
DP = ("dp_0", "dp_1", "dp_2")
DP_TR_TC = ("dp_0", "dp_1", "dp_2", "tr", "tc")
AXES = DP_TR_TC

ACT, GRAD = 0, 1
PIECES = (
    (GRAD, 0, 512, 0),
    (GRAD, 512, 384, 0),
    (GRAD, 0, 384, 1),
    (GRAD, 384, 256, 1),
    (GRAD, 640, 256, 1),
    (ACT, 0, 512, 0),
    (ACT, 0, 512, 1),
)
AT_ONCE = (0, 1, 2)
AFTER = {1: (3, 4), 4: (5, 6)}


def pieces_of(m, half):
    return [i for i, p in enumerate(PIECES) if p[0] == m and p[3] == half]


def kernel(
    act, grad, out_a, out_g,
    buf_a, buf_g, prod_a, prod_g, recv_a, recv_g, prox_a, prox_g, recx_a, recx_g,
    fin_a, fin_g, finx_a, finx_g, turn_a, turn_g, turx_a, turx_g,
    mir_a, mir_g, mirx_a, mirx_g, row_a, row_g,
    own_sem, a_send, a_recv, b_send, b_recv, d_send, d_recv,
    s_send, s_recv, x_send, x_recv, f_send, f_recv, g_send, g_recv,
    m_send, m_recv, n_send, n_recv, o_sem,
):
    h = lax.axis_index("dp_0")
    z = lax.axis_index("dp_1")
    y = lax.axis_index("dp_2")
    tr = lax.axis_index("tr")
    tc = lax.axis_index("tc")
    is_n = (tr + h) % 2
    odd = (h + tc) % 2
    shift = (is_n * odd, (1 - is_n) * odd + is_n * h)

    src = (act, grad)
    out = (out_a, out_g)
    buf = (buf_a, buf_g)
    prod = (prod_a, prod_g)
    recv = (recv_a, recv_g)
    prox = (prox_a, prox_g)
    recx = (recx_a, recx_g)
    fin = (fin_a, fin_g)
    finx = (finx_a, finx_g)
    turn = (turn_a, turn_g)
    turx = (turx_a, turx_g)
    mir = (mir_a, mir_g)
    mirx = (mirx_a, mirx_g)
    row = (row_a, row_g)

    def flip1(v):
        return v + 1 - 2 * (v % 2)

    def flip3(v):
        return 3 - v

    x1 = (1 - h, z, y, tr, tc)
    x3 = (1 - h, z, y, tr, 1 - tc)
    core = (h, z, y, 1 - tr, tc)
    others = ((h, z, y, tr, 1 - tc), core, (h, z, y, 1 - tr, 1 - tc))
    y_a, y_b = (h, z, flip1(y), tr, tc), (h, z, flip3(y), tr, tc)
    z_a, z_b = (h, flip1(z), y, tr, tc), (h, flip3(z), y, tr, tc)

    ORDER_N = ((0, 1, 2, 3), (1, 0, 3, 2))
    ORDER_R = ((2, 3, 0, 1), (3, 2, 1, 0))
    along = (y_a, y_b, z_a, z_b)

    def partner(k, j):
        pair = zip(along[ORDER_N[k][j]], along[ORDER_R[k][j]])
        return tuple(b + is_n * (a - b) for a, b in pair)

    half_z = z // 2
    c_mine = z % 2
    apart = (half_z + tc) % 2
    place = is_n * (1 - shift[1])
    side = (c_mine + apart * (place + shift[1]) + (1 - apart) * shift[0]) % 2
    moved = apart * place
    mirrors = 1 - (1 - is_n) * (1 - apart)
    kind = is_n * (1 + apart)
    turned_rows = (
        4 * h + 2 * (1 - half_z) + (c_mine + h + half_z) % 2,
        4 * (1 - h) + 2 * half_z + (c_mine + 1 + h + half_z) % 2,
        4 * (1 - h) + 2 * (1 - half_z) + (c_mine + 1 + h) % 2,
    )

    def quarters():
        for yy in range(4):
            for aa in range(2):
                for bb in range(2):
                    yield yy * 4 + aa * 2 + bb, (tr, 2 * tc + side, yy, aa, bb)

    barrier = pltpu.get_barrier_semaphore()
    peers = [x1, x3, *others, y_a, y_b, z_a, z_b]

    def greet(peer):
        pl.semaphore_signal(barrier, inc=1, device_id=peer, device_id_type=MESH)

    for peer in peers:
        greet(peer)

    own = [pltpu.make_async_copy(src[m], buf[m].at[0], own_sem.at[m]) for m in (ACT, GRAD)]
    for copy in own:
        copy.start()
    pl.semaphore_wait(barrier, len(peers))

    def cols(i, first):
        m, offset, size, later = PIECES[i]
        start = (first + later) % 2 * (buf[m].shape[2] // 2) + offset
        return pl.ds(pl.multiple_of(start, 128), size)

    def remote(a, b, ss, rs, to):
        return pltpu.make_async_remote_copy(
            src_ref=a, dst_ref=b, send_sem=ss, recv_sem=rs, device_id=to, device_id_type=MESH
        )

    def along_a(i):
        m = PIECES[i][0]
        to = (1 - is_n) * (1 - odd)
        return remote(
            src[m].at[:, cols(i, to)], buf[m].at[1, :, cols(i, to)], a_send.at[m], a_recv.at[i], x1
        )

    def along_b(k, i):
        m = PIECES[i][0]
        part = cols(i, odd)
        source = src[m].at[:, part] if k == 0 else buf[m].at[1, :, part]
        return remote(source, buf[m].at[3 - k, :, part], b_send.at[k, m], b_recv.at[k, i], x3)

    def to_core(k, i):
        m = PIECES[i][0]
        part = cols(i, 0 if k < 2 else odd)
        source = src[m].at[:, part] if k == 0 else buf[m].at[k, :, part]
        slot = k + 4 if k < 2 else k
        return remote(source, buf[m].at[slot, :, part], d_send.at[k, m], d_recv.at[k, i], core)

    every = range(len(PIECES))
    for i in every:
        along_a(i).start()

    @pl.when(is_n == 1)
    def _():
        for i in AT_ONCE:
            along_b(0, i).start()

    @pl.when(is_n == 0)
    def _():
        for i in every:
            to_core(0, i).start()

    def step_a(m, half):
        for i in pieces_of(m, half):
            along_a(i).wait_recv()

            @pl.when(is_n == 1)
            def _(i=i):
                along_b(1, i).start()
                for j in AFTER.get(i, ()):
                    along_b(0, j).start()

            @pl.when(is_n == 0)
            def _(i=i):
                to_core(1, i).start()

        @pl.when(is_n == 1)
        def _():
            for i in pieces_of(m, half):
                to_core(0, i).wait_recv()
                to_core(1, i).wait_recv()

    def step_b(m, half):
        @pl.when(is_n == 0)
        def _():
            for i in pieces_of(m, half):
                along_b(0, i).wait_recv()
                to_core(3, i).start()
            for i in pieces_of(m, half):
                along_b(1, i).wait_recv()
                to_core(2, i).start()

        @pl.when(is_n == 1)
        def _():
            for i in pieces_of(m, half):
                to_core(3, i).wait_recv()
                to_core(2, i).wait_recv()

    zb = z // 2
    za = (z + zb) % 2
    yb = y // 2
    ya = (y + yb) % 2

    def weight(d, k):
        at_n, at_r = 2 ** ORDER_N[k].index(d), 2 ** ORDER_R[k].index(d)
        return at_r + is_n * (at_n - at_r)

    def stream_copy(m, k, q, to):
        return remote(
            prod[m].at[k, q], recv[m].at[k, q], s_send.at[m, k], s_recv.at[m, k, q], to
        )

    def lanes_of(m, k):
        tiles = buf[m].shape[2] // 256
        first = (tiles + 1) // 2 * 128
        return pl.ds(0, first) if k == 0 else pl.ds(first, tiles * 128 - first)

    def extra_copy(m, k, q, to):
        return remote(
            prox[m].at[q, :, lanes_of(m, k)],
            recx[m].at[q, :, lanes_of(m, k)],
            x_send.at[m, k],
            x_recv.at[m, q],
            to,
        )

    def dot(m, e, c, s):
        half = buf[m].shape[2] // 2
        tokens = 2 * buf[m].shape[1]
        base = e * 2 + (1 - e) * 4 * is_n
        left = buf[m][pl.ds(base, 2), :, pl.ds(pl.multiple_of(c * half, 128), half)]
        right = buf[m][pl.ds(0, 2), :, pl.ds(pl.multiple_of(s * half, 128), half)]
        return lax.dot_general(
            left.reshape(tokens, half),
            right.reshape(tokens, half),
            (((0,), (0,)), ((), ())),
            preferred_element_type=jnp.float32,
        )

    def bits_of(yy):
        return ((yy ^ (yy >> 1)) % 2 + ya) % 2, (yy // 2 + yb) % 2

    def product(m, e, order):
        c = (order + odd) % 2 if e else order
        s = (c + shift[e]) % 2
        value = dot(m, e, c, s)
        rows = value.shape[0] // 8
        block = (tc + e) % 2
        rza = (c + (place if e else 0) + block + za) % 2
        rzb = (block + zb) % 2
        for yy in range(4):
            rya, ryb = bits_of(yy)
            for k in range(2):
                q = rza * weight(2, k) + rzb * weight(3, k)
                q = q + rya * weight(0, k) + ryb * weight(1, k)
                first = (2 * yy + k) * rows
                prod[m][k, q] = value[first : first + rows].astype(jnp.bfloat16)

                @pl.when(q % 2 == 1)
                def _(k=k, q=q):
                    stream_copy(m, k, q, partner(k, 0)).start()

    EXTRA = ((y_a, y_b, z_a, z_b), (z_b, z_a, y_b, y_a))

    def product_extra(m):
        value = dot(m, 0, 0, 1)
        rows = value.shape[0] // 16
        for yy in range(4):
            rya, ryb = bits_of(yy)
            for zz in range(4):
                rza = ((zz ^ (zz >> 1)) % 2 + za) % 2
                rzb = (zz // 2 + zb) % 2
                first = (4 * yy + zz) * rows
                part = value[first : first + rows].astype(jnp.bfloat16)
                for k in range(2):
                    if k == 0:
                        q = rya + 2 * ryb + 4 * rza + 8 * rzb
                    else:
                        q = rzb + 2 * rza + 4 * ryb + 8 * rya
                    lanes = lanes_of(m, k)
                    prox[m][q, :, lanes] = part[:, lanes.start : lanes.start + lanes.size]

                    @pl.when(q % 2 == 1)
                    def _(k=k, q=q):
                        extra_copy(m, k, q, EXTRA[k][0]).start()

    def total(own_ref, got_ref, k, q, parts):
        value = own_ref[k, q].astype(jnp.float32)
        for p in parts:
            value = value + got_ref[k, p].astype(jnp.float32)
        return value

    early_0 = 1
    early_1 = 1 - is_n * h

    def group_of(k, q):
        def bit(d):
            at_n, at_r = 2 ** ORDER_N[k].index(d), 2 ** ORDER_R[k].index(d)
            return is_n * (q // at_n % 2) + (1 - is_n) * (q // at_r % 2)

        block = (bit(3) + zb) % 2
        c = (bit(2) + za + block) % 2
        e = (block + tc) % 2
        c = (c + e * place) % 2
        second = (c + odd) % 2
        return (1 - e) * c + e * (2 * second + (1 - second) * (1 - early_1))

    def stage(m, j, group=None):
        def move(k, q, parts):
            for p in parts:
                stream_copy(m, k, p, core).wait_recv()
            prod[m][k, q] = total(prod[m], recv[m], k, q, parts).astype(jnp.bfloat16)
            stream_copy(m, k, q, partner(k, j)).start()

        def one(i, carry):
            q = i * 2 ** (j + 1) + 2**j
            parts = [q + 2**b for b in range(j)]
            for k in range(2):
                if group is None:
                    move(k, q, parts)
                else:
                    pl.when(group_of(k, q) == group)(functools.partial(move, k, q, parts))
            return carry

        lax.fori_loop(0, 2 ** (3 - j), one, 0)

    def extra_arrived(m, parts):
        for p in parts:
            slot = recx[m].at[p]
            remote(slot, slot, x_send.at[m, 0], x_recv.at[m, p], core).wait_recv()

    def total_extra(m, k, q, parts):
        value = prox[m][q, :, lanes_of(m, k)].astype(jnp.float32)
        for p in parts:
            value = value + recx[m][p, :, lanes_of(m, k)].astype(jnp.float32)
        return value

    def stage_extra(m, j):
        def one(i, carry):
            q = i * 2 ** (j + 1) + 2**j
            parts = [q + 2**b for b in range(j)]
            extra_arrived(m, parts)
            for k in range(2):
                prox[m][q, :, lanes_of(m, k)] = total_extra(m, k, q, parts).astype(jnp.bfloat16)
                extra_copy(m, k, q, EXTRA[k][j]).start()
            return carry

        @pl.when(is_n == 0)
        def _():
            lax.fori_loop(0, 2 ** (3 - j), one, 0)

    def at(m, block, s):
        width = buf[m].shape[2]
        half = width // 2
        first = pl.multiple_of(block * width + s * half, 128)
        return pl.ds(first, half)

    def last_copy(m, k):
        _, _, _, a, b = (*others, x1)[k]
        to = (h, z + moved * (flip1(z) - z), y, a, b)
        return remote(
            fin[m].at[2 * to[3] + to[4]],
            row[m].at[:, at(m, 2 * tr + tc, side)],
            f_send.at[m],
            f_recv.at[m, k],
            to,
        )

    extra_to = (h, 2 * tc, y, half_z, c_mine)
    keeps = (1 - is_n) * (1 - apart) * (1 - c_mine) * (1 - tr) * (1 - tc)
    keeps_turned = (1 - is_n) * (1 - apart) * c_mine

    def last_extra(m):
        return remote(
            finx[m], row[m].at[:, at(m, 2 * tr + tc, 1)], g_send.at[m], g_recv.at[m], extra_to
        )

    def turned_extra(m, i):
        to = (h, 2 * tc + 1, i // 4, i // 2 % 2, i % 2)
        return remote(
            turx[m].at[i], mirx[m].at[4 * y + z], n_send.at[m], n_recv.at[m], to
        )

    def is_self(i):
        return keeps_turned * (i == 4 * y + 2 * tr + tc).astype(jnp.int32)

    def turned_copy(m, i, to):
        return remote(
            turn[m].at[i], mir[m].at[kind, y], m_send.at[m], m_recv.at[m, kind], to
        )

    def by_quarter(m, ref, value):
        rows = value.shape[0] // 4
        for i in range(4):
            ref[m][i] = value[i * rows : (i + 1) * rows].astype(jnp.bfloat16)

    def finish(m):
        parts = (1, 2, 4, 8)
        for k in range(2):
            for p in parts:
                stream_copy(m, k, p, core).wait_recv()
        value = jnp.concatenate(
            [total(prod[m], recv[m], k, 0, parts) for k in range(2)], axis=0
        )
        by_quarter(m, fin, value)
        for k in range(3):
            last_copy(m, k).start()

        @pl.when(moved == 1)
        def _():
            last_copy(m, 3).start()

        @pl.when(moved == 0)
        def _():
            row[m][:, at(m, 2 * tr + tc, side)] = fin[m][2 * tr + tc]

        @pl.when(mirrors == 1)
        def _():
            lanes = turn[m].shape[2]
            tall = value
            if lanes != value.shape[0]:
                fill = jnp.zeros((lanes - value.shape[0], value.shape[1]), jnp.float32)
                tall = jnp.concatenate([value, fill], axis=0)
            turned = tall.T
            rows = turned.shape[0] // 16
            for i, to in quarters():
                turn[m][i] = turned[i * rows : (i + 1) * rows].astype(jnp.bfloat16)

    def send_turned(m):
        @pl.when(mirrors == 1)
        def _():
            for i, to in quarters():
                turned_copy(m, i, to).start()

    def finish_extra(m):
        @pl.when(is_n == 0)
        def _():
            extra_arrived(m, (1, 2, 4, 8))
            value = jnp.concatenate(
                [total_extra(m, k, 0, (1, 2, 4, 8)) for k in range(2)], axis=1
            )
            finx[m][...] = value.astype(jnp.bfloat16)

            @pl.when(keeps == 0)
            def _():
                last_extra(m).start()

            @pl.when(keeps == 1)
            def _():
                row[m][:, at(m, 2 * tr + tc, 1)] = finx[m][...]

            rows = value.shape[0]
            fill = jnp.zeros((128 - rows, value.shape[1]), jnp.float32)
            turned = jnp.concatenate([value, fill], axis=0).T
            for i in range(16):
                turx[m][i] = turned[i * rows : (i + 1) * rows].astype(jnp.bfloat16)

                @pl.when(is_self(i) == 0)
                def _(i=i):
                    turned_extra(m, i).start()

                @pl.when(is_self(i) == 1)
                def _(i=i):
                    mirx[m][4 * y + z] = turx[m][i]

    def gather_rows(m):
        width = buf[m].shape[2]
        rows = width // 8
        for t in range(3):
            pieces = mir[m].at[t]
            remote(pieces, pieces, m_send.at[m], m_recv.at[m, t], core).wait_recv()
            value = jnp.concatenate(
                [mir[m][t, yy].astype(jnp.float32)[:, :rows] for yy in range(4)], axis=1
            )
            chunk = turned_rows[t]
            row[m][:, at(m, chunk // 2, chunk % 2)] = value.astype(jnp.bfloat16)
        for k in range(3):
            last_copy(m, k).wait_recv()

        @pl.when(moved == 1)
        def _():
            last_copy(m, 3).wait_recv()

        @pl.when(c_mine * (1 - keeps) + (1 - c_mine) * keeps == 0)
        def _():
            last_extra(m).wait_recv()

        @pl.when(c_mine == 1)
        def _():
            rows = width // 32
            for count in (15, 16):

                @pl.when(keeps_turned == 16 - count)
                def _(count=count):
                    pieces = mirx[m].at[pl.ds(0, count)]
                    remote(pieces, pieces, n_send.at[m], n_recv.at[m], core).wait_recv()

            value = jnp.concatenate(
                [mirx[m][i].astype(jnp.float32)[:, :rows] for i in range(16)], axis=1
            )
            row[m][:, at(m, 2 * h + half_z, 0)] = value.astype(jnp.bfloat16)

        own_out(m).start()

    def own_out(m):
        return pltpu.make_async_copy(row[m], out[m], o_sem.at[m])

    def products(m, e, first, last):
        def one(c, carry):
            product(m, e, c)
            return carry

        lax.fori_loop(first, last, one, 0)

    def extras(m):
        @pl.when(is_n == 0)
        def _():
            product_extra(m)

    for copy in own:
        copy.wait()
    step_a(GRAD, 0)
    products(GRAD, 0, 0, early_0)
    step_b(GRAD, 0)
    products(GRAD, 1, 0, early_1)
    step_a(GRAD, 1)
    products(GRAD, 0, early_0, 2)
    products(GRAD, 1, early_1, 1)
    extras(GRAD)
    stage(GRAD, 1, 0)
    step_b(GRAD, 1)
    products(GRAD, 1, 1, 2)
    step_a(ACT, 0)
    products(ACT, 0, 0, 1)
    stage(GRAD, 1, 1)
    stage_extra(GRAD, 1)
    step_a(ACT, 1)
    products(ACT, 0, 1, 2)
    extras(ACT)
    stage(GRAD, 1, 2)
    step_b(ACT, 0)
    step_b(ACT, 1)
    products(ACT, 1, 0, 2)
    stage(GRAD, 2)
    stage_extra(GRAD, 2)
    stage(ACT, 1)
    stage_extra(ACT, 1)
    stage(GRAD, 3)
    stage_extra(GRAD, 3)
    stage(ACT, 2)
    finish(GRAD)
    send_turned(GRAD)
    stage_extra(ACT, 2)
    stage(ACT, 3)
    stage_extra(ACT, 3)
    finish_extra(GRAD)
    finish(ACT)
    send_turned(ACT)
    finish_extra(ACT)
    gather_rows(GRAD)
    gather_rows(ACT)

    def sent(ref, sem):
        pltpu.make_async_copy(ref, ref, sem).wait()

    for m in (ACT, GRAD):
        block = buf[m].at[1]
        sent(block, a_send.at[m])

        @pl.when(is_n == 1)
        def _(m=m, block=block):
            for k in (0, 1):
                sent(block, b_send.at[k, m])

        @pl.when(is_n == 0)
        def _(m=m, block=block):
            for k in range(4):
                sent(block, d_send.at[k, m])
            for k in range(2):
                sent(prox[m].at[pl.ds(1, 15), :, lanes_of(m, k)], x_send.at[m, k])

            @pl.when(keeps == 0)
            def _():
                last_extra(m).wait_send()

            for count in (15, 16):

                @pl.when(keeps_turned == 16 - count)
                def _(count=count):
                    sent(turx[m].at[pl.ds(0, count)], n_send.at[m])

        for k in range(2):
            sent(prod[m].at[k, pl.ds(1, 15)], s_send.at[m, k])
        for count in (3, 4):

            @pl.when(moved == count - 3)
            def _(m=m, count=count):
                sent(fin[m].at[pl.ds(0, count)], f_send.at[m])


        @pl.when(mirrors == 1)
        def _(m=m):
            sent(turn[m], m_send.at[m])

        own_out(m).wait()


def sums(activations, gradients, rows_a, rows_g):
    tokens = activations.shape[0]
    wide = (activations.shape[1], gradients.shape[1])
    rows = (rows_a, rows_g)
    bf16 = jnp.bfloat16
    lanes = [-(-w // 1024) * 128 for w in wide]
    vmem = [
        *(pltpu.VMEM((6, tokens, w), bf16) for w in wide),
        *(pltpu.VMEM((2, 16, w // 16, w // 2), bf16) for w in wide),
        *(pltpu.VMEM((2, 16, w // 16, w // 2), bf16) for w in wide),
        *(pltpu.VMEM((16, r, w // 2), bf16) for r, w in zip(rows, wide)),
        *(pltpu.VMEM((16, r, w // 2), bf16) for r, w in zip(rows, wide)),
        *(pltpu.VMEM((4, r, w // 2), bf16) for r, w in zip(rows, wide)),
        *(pltpu.VMEM((r, w // 2), bf16) for r, w in zip(rows, wide)),
        *(pltpu.VMEM((16, r, n), bf16) for r, n in zip(rows, lanes)),
        *(pltpu.VMEM((16, r, 128), bf16) for r in rows),
        *(pltpu.VMEM((3, 4, r, n), bf16) for r, n in zip(rows, lanes)),
        *(pltpu.VMEM((16, r, 128), bf16) for r in rows),
        *(pltpu.VMEM((r, 4 * w), bf16) for r, w in zip(rows, wide)),
    ]
    n = len(PIECES)
    dma = pltpu.SemaphoreType.DMA
    sems = [
        dma((2,)), dma((2,)), dma((n,)), dma((2, 2)), dma((2, n)), dma((4, 2)), dma((4, n)),
        dma((2, 2)), dma((2, 2, 16)), dma((2, 2)), dma((2, 16)),
        dma((2,)), dma((2, 4)), dma((2,)), dma((2,)),
        dma((2,)), dma((2, 3)), dma((2,)), dma((2,)), dma((2,)),
    ]
    anywhere = pl.BlockSpec(memory_space=pl.ANY)
    return pl.pallas_call(
        kernel,
        out_shape=[jax.ShapeDtypeStruct((r, 4 * w), bf16) for r, w in zip(rows, wide)],
        in_specs=[pl.BlockSpec(memory_space=pltpu.HBM)] * 2,
        out_specs=[anywhere] * 2,
        scratch_shapes=[*vmem, *sems],
        compiler_params=pltpu.CompilerParams(
            collective_id=0, has_side_effects=True, vmem_limit_bytes=54_800_000
        ),
    )(activations, gradients)


def body(activations, gradients, old_inputs, old_gradients):
    tokens_all = activations.shape[0] * lax.axis_size(DP)
    sum_a, sum_g = sums(activations, gradients, old_inputs.shape[0], old_gradients.shape[0])
    scale = 0.5 / tokens_all
    return (
        0.5 * old_inputs + scale * sum_a.astype(jnp.float32),
        0.5 * old_gradients + scale * sum_g.astype(jnp.float32),
    )


def solution(mesh):
    finer = Mesh(mesh.devices.reshape(2, 4, 4, mesh.shape["tr"], mesh.shape["tc"]), AXES)
    return jax.shard_map(
        body,
        mesh=finer,
        in_specs=(P(DP, ("tr", "tc")), P(DP, ("tr", "tc")), P(DP_TR_TC, None), P(DP_TR_TC, None)),
        out_specs=(P(DP_TR_TC, None), P(DP_TR_TC, None)),
        check_vma=False,
    )
```

```python
import functools

import jax
import jax.numpy as jnp
from jax import lax
from jax.experimental import pallas as pl
from jax.experimental.pallas import tpu as pltpu
from jax.sharding import Mesh
from jax.sharding import PartitionSpec as P

MESH = pl.DeviceIdType.MESH
DP = ("dp_0", "dp_1", "dp_2")
DP_TR_TC = ("dp_0", "dp_1", "dp_2", "tr", "tc")
AXES = DP_TR_TC

ACT, GRAD = 0, 1
PIECES = (
    (GRAD, 0, 512, 0),
    (GRAD, 512, 384, 0),
    (GRAD, 0, 384, 1),
    (GRAD, 384, 256, 1),
    (GRAD, 640, 256, 1),
    (ACT, 0, 512, 0),
    (ACT, 0, 256, 1),
    (ACT, 256, 256, 1),
)
AT_ONCE = (0, 1, 2)
AFTER = {1: (3, 4), 4: (5, 6, 7)}


def pieces_of(m, half):
    return [i for i, p in enumerate(PIECES) if p[0] == m and p[3] == half]


def kernel(
    act, grad, out_a, out_g,
    buf_a, buf_g, prod_a, prod_g, recv_a, recv_g, prox_a, prox_g, recx_a, recx_g,
    fin_a, fin_g, finx_a, finx_g, turn_a, turn_g, turx_a, turx_g,
    mir_a, mir_g, mirx_a, mirx_g, row_a, row_g,
    own_sem, a_send, a_recv, b_send, b_recv, d_send, d_recv,
    s_send, s_recv, x_send, x_recv, f_send, f_recv, g_send, g_recv,
    m_send, m_recv, n_send, n_recv, o_sem,
):
    h = lax.axis_index("dp_0")
    z = lax.axis_index("dp_1")
    y = lax.axis_index("dp_2")
    tr = lax.axis_index("tr")
    tc = lax.axis_index("tc")
    is_n = (tr + h) % 2
    odd = (h + tc) % 2
    shift = (is_n * odd, (1 - is_n) * odd + is_n * h)

    src = (act, grad)
    out = (out_a, out_g)
    buf = (buf_a, buf_g)
    prod = (prod_a, prod_g)
    recv = (recv_a, recv_g)
    prox = (prox_a, prox_g)
    recx = (recx_a, recx_g)
    fin = (fin_a, fin_g)
    finx = (finx_a, finx_g)
    turn = (turn_a, turn_g)
    turx = (turx_a, turx_g)
    mir = (mir_a, mir_g)
    mirx = (mirx_a, mirx_g)
    row = (row_a, row_g)

    def flip1(v):
        return v + 1 - 2 * (v % 2)

    def flip3(v):
        return 3 - v

    x1 = (1 - h, z, y, tr, tc)
    x3 = (1 - h, z, y, tr, 1 - tc)
    core = (h, z, y, 1 - tr, tc)
    others = ((h, z, y, tr, 1 - tc), core, (h, z, y, 1 - tr, 1 - tc))
    y_a, y_b = (h, z, flip1(y), tr, tc), (h, z, flip3(y), tr, tc)
    z_a, z_b = (h, flip1(z), y, tr, tc), (h, flip3(z), y, tr, tc)

    ORDER_N = ((0, 1, 2, 3), (1, 0, 3, 2))
    ORDER_R = ((2, 3, 0, 1), (3, 2, 1, 0))
    along = (y_a, y_b, z_a, z_b)

    def partner(k, j):
        pair = zip(along[ORDER_N[k][j]], along[ORDER_R[k][j]])
        return tuple(b + is_n * (a - b) for a, b in pair)

    half_z = z // 2
    c_mine = z % 2
    apart = (half_z + tc) % 2
    place = is_n * (1 - shift[1])
    side = (c_mine + apart * (place + shift[1]) + (1 - apart) * shift[0]) % 2
    moved = apart * place
    mirrors = 1 - (1 - is_n) * (1 - apart)
    kind = is_n * (1 + apart)
    turned_rows = (
        4 * h + 2 * (1 - half_z) + (c_mine + h + half_z) % 2,
        4 * (1 - h) + 2 * half_z + (c_mine + 1 + h + half_z) % 2,
        4 * (1 - h) + 2 * (1 - half_z) + (c_mine + 1 + h) % 2,
    )

    def quarters():
        for yy in range(4):
            for aa in range(2):
                for bb in range(2):
                    yield yy * 4 + aa * 2 + bb, (tr, 2 * tc + side, yy, aa, bb)

    barrier = pltpu.get_barrier_semaphore()
    peers = [x1, x3, *others, y_a, y_b, z_a, z_b]

    def greet(peer):
        pl.semaphore_signal(barrier, inc=1, device_id=peer, device_id_type=MESH)

    for peer in peers:
        greet(peer)

    own = [pltpu.make_async_copy(src[m], buf[m].at[0], own_sem.at[m]) for m in (ACT, GRAD)]
    for copy in own:
        copy.start()
    pl.semaphore_wait(barrier, len(peers))

    def cols(i, first):
        m, offset, size, later = PIECES[i]
        start = (first + later) % 2 * (buf[m].shape[2] // 2) + offset
        return pl.ds(pl.multiple_of(start, 128), size)

    def remote(a, b, ss, rs, to):
        return pltpu.make_async_remote_copy(
            src_ref=a, dst_ref=b, send_sem=ss, recv_sem=rs, device_id=to, device_id_type=MESH
        )

    def along_a(i):
        m = PIECES[i][0]
        to = (1 - is_n) * (1 - odd)
        return remote(
            src[m].at[:, cols(i, to)], buf[m].at[1, :, cols(i, to)], a_send.at[m], a_recv.at[i], x1
        )

    def along_b(k, i):
        m = PIECES[i][0]
        part = cols(i, odd)
        source = src[m].at[:, part] if k == 0 else buf[m].at[1, :, part]
        return remote(source, buf[m].at[3 - k, :, part], b_send.at[k, m], b_recv.at[k, i], x3)

    def to_core(k, i):
        m = PIECES[i][0]
        part = cols(i, 0 if k < 2 else odd)
        source = src[m].at[:, part] if k == 0 else buf[m].at[k, :, part]
        slot = k + 4 if k < 2 else k
        return remote(source, buf[m].at[slot, :, part], d_send.at[k, m], d_recv.at[k, i], core)

    every = range(len(PIECES))
    for i in every:
        along_a(i).start()

    @pl.when(is_n == 1)
    def _():
        for i in AT_ONCE:
            along_b(0, i).start()

    @pl.when(is_n == 0)
    def _():
        for i in every:
            to_core(0, i).start()

    def step_a(m, half):
        for i in pieces_of(m, half):
            along_a(i).wait_recv()

            @pl.when(is_n == 1)
            def _(i=i):
                along_b(1, i).start()
                for j in AFTER.get(i, ()):
                    along_b(0, j).start()

            @pl.when(is_n == 0)
            def _(i=i):
                to_core(1, i).start()

        @pl.when(is_n == 1)
        def _():
            for i in pieces_of(m, half):
                to_core(0, i).wait_recv()
                to_core(1, i).wait_recv()

    def step_b(m, half):
        @pl.when(is_n == 0)
        def _():
            for i in pieces_of(m, half):
                along_b(0, i).wait_recv()
                to_core(3, i).start()
            for i in pieces_of(m, half):
                along_b(1, i).wait_recv()
                to_core(2, i).start()

        @pl.when(is_n == 1)
        def _():
            for i in pieces_of(m, half):
                to_core(3, i).wait_recv()
                to_core(2, i).wait_recv()

    zb = z // 2
    za = (z + zb) % 2
    yb = y // 2
    ya = (y + yb) % 2

    def weight(d, k):
        at_n, at_r = 2 ** ORDER_N[k].index(d), 2 ** ORDER_R[k].index(d)
        return at_r + is_n * (at_n - at_r)

    def stream_copy(m, k, q, to):
        return remote(
            prod[m].at[k, q], recv[m].at[k, q], s_send.at[m, k], s_recv.at[m, k, q], to
        )

    def lanes_of(m, k):
        tiles = buf[m].shape[2] // 256
        first = (tiles + 1) // 2 * 128
        return pl.ds(0, first) if k == 0 else pl.ds(first, tiles * 128 - first)

    def extra_copy(m, k, q, to):
        return remote(
            prox[m].at[q, :, lanes_of(m, k)],
            recx[m].at[q, :, lanes_of(m, k)],
            x_send.at[m, k],
            x_recv.at[m, q],
            to,
        )

    def dot(m, e, c, s):
        half = buf[m].shape[2] // 2
        tokens = 2 * buf[m].shape[1]
        base = e * 2 + (1 - e) * 4 * is_n
        left = buf[m][pl.ds(base, 2), :, pl.ds(pl.multiple_of(c * half, 128), half)]
        right = buf[m][pl.ds(0, 2), :, pl.ds(pl.multiple_of(s * half, 128), half)]
        return lax.dot_general(
            left.reshape(tokens, half),
            right.reshape(tokens, half),
            (((0,), (0,)), ((), ())),
            preferred_element_type=jnp.float32,
        )

    def bits_of(yy):
        return ((yy ^ (yy >> 1)) % 2 + ya) % 2, (yy // 2 + yb) % 2

    def product(m, e, order):
        c = (order + odd) % 2 if e else order
        s = (c + shift[e]) % 2
        value = dot(m, e, c, s)
        rows = value.shape[0] // 8
        block = (tc + e) % 2
        rza = (c + (place if e else 0) + block + za) % 2
        rzb = (block + zb) % 2
        for yy in range(4):
            rya, ryb = bits_of(yy)
            for k in range(2):
                q = rza * weight(2, k) + rzb * weight(3, k)
                q = q + rya * weight(0, k) + ryb * weight(1, k)
                first = (2 * yy + k) * rows
                prod[m][k, q] = value[first : first + rows].astype(jnp.bfloat16)

                @pl.when(q % 2 == 1)
                def _(k=k, q=q):
                    stream_copy(m, k, q, partner(k, 0)).start()

    EXTRA = ((y_a, y_b, z_a, z_b), (z_b, z_a, y_b, y_a))

    def product_extra(m):
        value = dot(m, 0, 0, 1)
        rows = value.shape[0] // 16
        for yy in range(4):
            rya, ryb = bits_of(yy)
            for zz in range(4):
                rza = ((zz ^ (zz >> 1)) % 2 + za) % 2
                rzb = (zz // 2 + zb) % 2
                first = (4 * yy + zz) * rows
                part = value[first : first + rows].astype(jnp.bfloat16)
                for k in range(2):
                    if k == 0:
                        q = rya + 2 * ryb + 4 * rza + 8 * rzb
                    else:
                        q = rzb + 2 * rza + 4 * ryb + 8 * rya
                    lanes = lanes_of(m, k)
                    prox[m][q, :, lanes] = part[:, lanes.start : lanes.start + lanes.size]

                    @pl.when(q % 2 == 1)
                    def _(k=k, q=q):
                        extra_copy(m, k, q, EXTRA[k][0]).start()

    def total(own_ref, got_ref, k, q, parts):
        value = own_ref[k, q].astype(jnp.float32)
        for p in parts:
            value = value + got_ref[k, p].astype(jnp.float32)
        return value

    early_0 = 1
    early_1 = 1 - is_n * h

    def group_of(k, q):
        def bit(d):
            at_n, at_r = 2 ** ORDER_N[k].index(d), 2 ** ORDER_R[k].index(d)
            return is_n * (q // at_n % 2) + (1 - is_n) * (q // at_r % 2)

        block = (bit(3) + zb) % 2
        c = (bit(2) + za + block) % 2
        e = (block + tc) % 2
        c = (c + e * place) % 2
        second = (c + odd) % 2
        return (1 - e) * c + e * (2 * second + (1 - second) * (1 - early_1))

    def stage(m, j, group=None):
        def move(k, q, parts):
            for p in parts:
                stream_copy(m, k, p, core).wait_recv()
            prod[m][k, q] = total(prod[m], recv[m], k, q, parts).astype(jnp.bfloat16)
            stream_copy(m, k, q, partner(k, j)).start()

        def one(i, carry):
            q = i * 2 ** (j + 1) + 2**j
            parts = [q + 2**b for b in range(j)]
            for k in range(2):
                if group is None:
                    move(k, q, parts)
                else:
                    pl.when(group_of(k, q) == group)(functools.partial(move, k, q, parts))
            return carry

        lax.fori_loop(0, 2 ** (3 - j), one, 0)

    def extra_arrived(m, parts):
        for p in parts:
            slot = recx[m].at[p]
            remote(slot, slot, x_send.at[m, 0], x_recv.at[m, p], core).wait_recv()

    def total_extra(m, k, q, parts):
        value = prox[m][q, :, lanes_of(m, k)].astype(jnp.float32)
        for p in parts:
            value = value + recx[m][p, :, lanes_of(m, k)].astype(jnp.float32)
        return value

    def stage_extra(m, j):
        def one(i, carry):
            q = i * 2 ** (j + 1) + 2**j
            parts = [q + 2**b for b in range(j)]
            extra_arrived(m, parts)
            for k in range(2):
                prox[m][q, :, lanes_of(m, k)] = total_extra(m, k, q, parts).astype(jnp.bfloat16)
                extra_copy(m, k, q, EXTRA[k][j]).start()
            return carry

        @pl.when(is_n == 0)
        def _():
            lax.fori_loop(0, 2 ** (3 - j), one, 0)

    def at(m, block, s):
        width = buf[m].shape[2]
        half = width // 2
        first = pl.multiple_of(block * width + s * half, 128)
        return pl.ds(first, half)

    def last_copy(m, k):
        _, _, _, a, b = (*others, x1)[k]
        to = (h, z + moved * (flip1(z) - z), y, a, b)
        return remote(
            fin[m].at[2 * to[3] + to[4]],
            row[m].at[:, at(m, 2 * tr + tc, side)],
            f_send.at[m],
            f_recv.at[m, k],
            to,
        )

    extra_to = (h, 2 * tc, y, half_z, c_mine)
    keeps = (1 - is_n) * (1 - apart) * (1 - c_mine) * (1 - tr) * (1 - tc)
    keeps_turned = (1 - is_n) * (1 - apart) * c_mine

    def last_extra(m):
        return remote(
            finx[m], row[m].at[:, at(m, 2 * tr + tc, 1)], g_send.at[m], g_recv.at[m], extra_to
        )

    def turned_extra(m, i):
        to = (h, 2 * tc + 1, i // 4, i // 2 % 2, i % 2)
        return remote(
            turx[m].at[i], mirx[m].at[4 * y + z], n_send.at[m], n_recv.at[m], to
        )

    def is_self(i):
        return keeps_turned * (i == 4 * y + 2 * tr + tc).astype(jnp.int32)

    def turned_copy(m, i, to):
        return remote(
            turn[m].at[i], mir[m].at[kind, y], m_send.at[m], m_recv.at[m, kind], to
        )

    def by_quarter(m, ref, value):
        rows = value.shape[0] // 4
        for i in range(4):
            ref[m][i] = value[i * rows : (i + 1) * rows].astype(jnp.bfloat16)

    def finish(m):
        parts = (1, 2, 4, 8)
        for k in range(2):
            for p in parts:
                stream_copy(m, k, p, core).wait_recv()
        value = jnp.concatenate(
            [total(prod[m], recv[m], k, 0, parts) for k in range(2)], axis=0
        )
        by_quarter(m, fin, value)
        for k in range(3):
            last_copy(m, k).start()

        @pl.when(moved == 1)
        def _():
            last_copy(m, 3).start()

        @pl.when(moved == 0)
        def _():
            row[m][:, at(m, 2 * tr + tc, side)] = fin[m][2 * tr + tc]

        @pl.when(mirrors == 1)
        def _():
            lanes = turn[m].shape[2]
            tall = value
            if lanes != value.shape[0]:
                fill = jnp.zeros((lanes - value.shape[0], value.shape[1]), jnp.float32)
                tall = jnp.concatenate([value, fill], axis=0)
            turned = tall.T
            rows = turned.shape[0] // 16
            for i, to in quarters():
                turn[m][i] = turned[i * rows : (i + 1) * rows].astype(jnp.bfloat16)

    def send_turned(m):
        @pl.when(mirrors == 1)
        def _():
            for i, to in quarters():
                turned_copy(m, i, to).start()

    def finish_extra(m):
        @pl.when(is_n == 0)
        def _():
            extra_arrived(m, (1, 2, 4, 8))
            value = jnp.concatenate(
                [total_extra(m, k, 0, (1, 2, 4, 8)) for k in range(2)], axis=1
            )
            finx[m][...] = value.astype(jnp.bfloat16)

            @pl.when(keeps == 0)
            def _():
                last_extra(m).start()

            @pl.when(keeps == 1)
            def _():
                row[m][:, at(m, 2 * tr + tc, 1)] = finx[m][...]

            rows = value.shape[0]
            fill = jnp.zeros((128 - rows, value.shape[1]), jnp.float32)
            turned = jnp.concatenate([value, fill], axis=0).T
            for i in range(16):
                turx[m][i] = turned[i * rows : (i + 1) * rows].astype(jnp.bfloat16)

                @pl.when(is_self(i) == 0)
                def _(i=i):
                    turned_extra(m, i).start()

                @pl.when(is_self(i) == 1)
                def _(i=i):
                    mirx[m][4 * y + z] = turx[m][i]

    def gather_rows(m):
        width = buf[m].shape[2]
        rows = width // 8
        for t in range(3):
            pieces = mir[m].at[t]
            remote(pieces, pieces, m_send.at[m], m_recv.at[m, t], core).wait_recv()
            value = jnp.concatenate(
                [mir[m][t, yy].astype(jnp.float32)[:, :rows] for yy in range(4)], axis=1
            )
            chunk = turned_rows[t]
            row[m][:, at(m, chunk // 2, chunk % 2)] = value.astype(jnp.bfloat16)
        for k in range(3):
            last_copy(m, k).wait_recv()

        @pl.when(moved == 1)
        def _():
            last_copy(m, 3).wait_recv()

        @pl.when(c_mine * (1 - keeps) + (1 - c_mine) * keeps == 0)
        def _():
            last_extra(m).wait_recv()

        @pl.when(c_mine == 1)
        def _():
            rows = width // 32
            for count in (15, 16):

                @pl.when(keeps_turned == 16 - count)
                def _(count=count):
                    pieces = mirx[m].at[pl.ds(0, count)]
                    remote(pieces, pieces, n_send.at[m], n_recv.at[m], core).wait_recv()

            value = jnp.concatenate(
                [mirx[m][i].astype(jnp.float32)[:, :rows] for i in range(16)], axis=1
            )
            row[m][:, at(m, 2 * h + half_z, 0)] = value.astype(jnp.bfloat16)

        own_out(m).start()

    def own_out(m):
        return pltpu.make_async_copy(row[m], out[m], o_sem.at[m])

    def products(m, e, first, last):
        def one(c, carry):
            product(m, e, c)
            return carry

        lax.fori_loop(first, last, one, 0)

    def extras(m):
        @pl.when(is_n == 0)
        def _():
            product_extra(m)

    for copy in own:
        copy.wait()
    step_a(GRAD, 0)
    products(GRAD, 0, 0, early_0)
    step_b(GRAD, 0)
    products(GRAD, 1, 0, early_1)
    step_a(GRAD, 1)
    products(GRAD, 0, early_0, 2)
    products(GRAD, 1, early_1, 1)
    extras(GRAD)
    stage(GRAD, 1, 0)
    step_b(GRAD, 1)
    products(GRAD, 1, 1, 2)
    step_a(ACT, 0)
    products(ACT, 0, 0, 1)
    stage(GRAD, 1, 1)
    stage_extra(GRAD, 1)
    step_a(ACT, 1)
    products(ACT, 0, 1, 2)
    extras(ACT)
    stage(GRAD, 1, 2)
    step_b(ACT, 0)
    step_b(ACT, 1)
    products(ACT, 1, 0, 2)
    stage(GRAD, 2)
    stage_extra(GRAD, 2)
    stage(ACT, 1)
    stage_extra(ACT, 1)
    stage(GRAD, 3)
    stage_extra(GRAD, 3)
    stage(ACT, 2)
    finish(GRAD)
    send_turned(GRAD)
    stage_extra(ACT, 2)
    stage(ACT, 3)
    stage_extra(ACT, 3)
    finish_extra(GRAD)
    finish(ACT)
    send_turned(ACT)
    finish_extra(ACT)
    gather_rows(GRAD)
    gather_rows(ACT)

    def sent(ref, sem):
        pltpu.make_async_copy(ref, ref, sem).wait()

    for m in (ACT, GRAD):
        block = buf[m].at[1]
        sent(block, a_send.at[m])

        @pl.when(is_n == 1)
        def _(m=m, block=block):
            for k in (0, 1):
                sent(block, b_send.at[k, m])

        @pl.when(is_n == 0)
        def _(m=m, block=block):
            for k in range(4):
                sent(block, d_send.at[k, m])
            for k in range(2):
                sent(prox[m].at[pl.ds(1, 15), :, lanes_of(m, k)], x_send.at[m, k])

            @pl.when(keeps == 0)
            def _():
                last_extra(m).wait_send()

            for count in (15, 16):

                @pl.when(keeps_turned == 16 - count)
                def _(count=count):
                    sent(turx[m].at[pl.ds(0, count)], n_send.at[m])

        for k in range(2):
            sent(prod[m].at[k, pl.ds(1, 15)], s_send.at[m, k])
        for count in (3, 4):

            @pl.when(moved == count - 3)
            def _(m=m, count=count):
                sent(fin[m].at[pl.ds(0, count)], f_send.at[m])


        @pl.when(mirrors == 1)
        def _(m=m):
            sent(turn[m], m_send.at[m])

        own_out(m).wait()


def sums(activations, gradients, rows_a, rows_g):
    tokens = activations.shape[0]
    wide = (activations.shape[1], gradients.shape[1])
    rows = (rows_a, rows_g)
    bf16 = jnp.bfloat16
    lanes = [-(-w // 1024) * 128 for w in wide]
    vmem = [
        *(pltpu.VMEM((6, tokens, w), bf16) for w in wide),
        *(pltpu.VMEM((2, 16, w // 16, w // 2), bf16) for w in wide),
        *(pltpu.VMEM((2, 16, w // 16, w // 2), bf16) for w in wide),
        *(pltpu.VMEM((16, r, w // 2), bf16) for r, w in zip(rows, wide)),
        *(pltpu.VMEM((16, r, w // 2), bf16) for r, w in zip(rows, wide)),
        *(pltpu.VMEM((4, r, w // 2), bf16) for r, w in zip(rows, wide)),
        *(pltpu.VMEM((r, w // 2), bf16) for r, w in zip(rows, wide)),
        *(pltpu.VMEM((16, r, n), bf16) for r, n in zip(rows, lanes)),
        *(pltpu.VMEM((16, r, 128), bf16) for r in rows),
        *(pltpu.VMEM((3, 4, r, n), bf16) for r, n in zip(rows, lanes)),
        *(pltpu.VMEM((16, r, 128), bf16) for r in rows),
        *(pltpu.VMEM((r, 4 * w), bf16) for r, w in zip(rows, wide)),
    ]
    n = len(PIECES)
    dma = pltpu.SemaphoreType.DMA
    sems = [
        dma((2,)), dma((2,)), dma((n,)), dma((2, 2)), dma((2, n)), dma((4, 2)), dma((4, n)),
        dma((2, 2)), dma((2, 2, 16)), dma((2, 2)), dma((2, 16)),
        dma((2,)), dma((2, 4)), dma((2,)), dma((2,)),
        dma((2,)), dma((2, 3)), dma((2,)), dma((2,)), dma((2,)),
    ]
    anywhere = pl.BlockSpec(memory_space=pl.ANY)
    return pl.pallas_call(
        kernel,
        out_shape=[jax.ShapeDtypeStruct((r, 4 * w), bf16) for r, w in zip(rows, wide)],
        in_specs=[pl.BlockSpec(memory_space=pltpu.HBM)] * 2,
        out_specs=[anywhere] * 2,
        scratch_shapes=[*vmem, *sems],
        compiler_params=pltpu.CompilerParams(
            collective_id=0, has_side_effects=True, vmem_limit_bytes=54_800_000
        ),
    )(activations, gradients)


def body(activations, gradients, old_inputs, old_gradients):
    tokens_all = activations.shape[0] * lax.axis_size(DP)
    sum_a, sum_g = sums(activations, gradients, old_inputs.shape[0], old_gradients.shape[0])
    scale = 0.5 / tokens_all
    return (
        0.5 * old_inputs + scale * sum_a.astype(jnp.float32),
        0.5 * old_gradients + scale * sum_g.astype(jnp.float32),
    )


def solution(mesh):
    finer = Mesh(mesh.devices.reshape(2, 4, 4, mesh.shape["tr"], mesh.shape["tc"]), AXES)
    return jax.shard_map(
        body,
        mesh=finer,
        in_specs=(P(DP, ("tr", "tc")), P(DP, ("tr", "tc")), P(DP_TR_TC, None), P(DP_TR_TC, None)),
        out_specs=(P(DP_TR_TC, None), P(DP_TR_TC, None)),
        check_vma=False,
    )
```

```python
import functools

import jax
import jax.numpy as jnp
from jax import lax
from jax.experimental import pallas as pl
from jax.experimental.pallas import tpu as pltpu
from jax.sharding import Mesh
from jax.sharding import PartitionSpec as P

MESH = pl.DeviceIdType.MESH
DP = ("dp_0", "dp_1", "dp_2")
DP_TR_TC = ("dp_0", "dp_1", "dp_2", "tr", "tc")
AXES = DP_TR_TC

ACT, GRAD = 0, 1
PIECES = (
    (GRAD, 0, 512, 0),
    (GRAD, 512, 384, 0),
    (GRAD, 0, 512, 1),
    (GRAD, 512, 256, 1),
    (GRAD, 768, 128, 1),
    (ACT, 0, 512, 0),
    (ACT, 0, 256, 1),
    (ACT, 256, 256, 1),
)
AT_ONCE = (0, 1, 2)
AFTER = {1: (3, 4), 4: (5, 6, 7)}


def pieces_of(m, half):
    return [i for i, p in enumerate(PIECES) if p[0] == m and p[3] == half]


def kernel(
    act, grad, out_a, out_g,
    buf_a, buf_g, prod_a, prod_g, recv_a, recv_g, prox_a, prox_g, recx_a, recx_g,
    fin_a, fin_g, finx_a, finx_g, turn_a, turn_g, turx_a, turx_g,
    mir_a, mir_g, mirx_a, mirx_g, row_a, row_g,
    own_sem, a_send, a_recv, b_send, b_recv, d_send, d_recv,
    s_send, s_recv, x_send, x_recv, f_send, f_recv, g_send, g_recv,
    m_send, m_recv, n_send, n_recv, o_sem,
):
    h = lax.axis_index("dp_0")
    z = lax.axis_index("dp_1")
    y = lax.axis_index("dp_2")
    tr = lax.axis_index("tr")
    tc = lax.axis_index("tc")
    is_n = (tr + h) % 2
    odd = (h + tc) % 2
    shift = (is_n * odd, (1 - is_n) * odd + is_n * h)

    src = (act, grad)
    out = (out_a, out_g)
    buf = (buf_a, buf_g)
    prod = (prod_a, prod_g)
    recv = (recv_a, recv_g)
    prox = (prox_a, prox_g)
    recx = (recx_a, recx_g)
    fin = (fin_a, fin_g)
    finx = (finx_a, finx_g)
    turn = (turn_a, turn_g)
    turx = (turx_a, turx_g)
    mir = (mir_a, mir_g)
    mirx = (mirx_a, mirx_g)
    row = (row_a, row_g)

    def flip1(v):
        return v + 1 - 2 * (v % 2)

    def flip3(v):
        return 3 - v

    x1 = (1 - h, z, y, tr, tc)
    x3 = (1 - h, z, y, tr, 1 - tc)
    core = (h, z, y, 1 - tr, tc)
    others = ((h, z, y, tr, 1 - tc), core, (h, z, y, 1 - tr, 1 - tc))
    y_a, y_b = (h, z, flip1(y), tr, tc), (h, z, flip3(y), tr, tc)
    z_a, z_b = (h, flip1(z), y, tr, tc), (h, flip3(z), y, tr, tc)

    ORDER_N = ((0, 1, 2, 3), (1, 0, 3, 2))
    ORDER_R = ((2, 3, 0, 1), (3, 2, 1, 0))
    along = (y_a, y_b, z_a, z_b)

    def partner(k, j):
        pair = zip(along[ORDER_N[k][j]], along[ORDER_R[k][j]])
        return tuple(b + is_n * (a - b) for a, b in pair)

    half_z = z // 2
    c_mine = z % 2
    apart = (half_z + tc) % 2
    place = is_n * (1 - shift[1])
    side = (c_mine + apart * (place + shift[1]) + (1 - apart) * shift[0]) % 2
    moved = apart * place
    mirrors = 1 - (1 - is_n) * (1 - apart)
    kind = is_n * (1 + apart)
    turned_rows = (
        4 * h + 2 * (1 - half_z) + (c_mine + h + half_z) % 2,
        4 * (1 - h) + 2 * half_z + (c_mine + 1 + h + half_z) % 2,
        4 * (1 - h) + 2 * (1 - half_z) + (c_mine + 1 + h) % 2,
    )

    def quarters():
        for yy in range(4):
            for aa in range(2):
                for bb in range(2):
                    yield yy * 4 + aa * 2 + bb, (tr, 2 * tc + side, yy, aa, bb)

    barrier = pltpu.get_barrier_semaphore()
    peers = [x1, x3, *others, y_a, y_b, z_a, z_b]

    def greet(peer):
        pl.semaphore_signal(barrier, inc=1, device_id=peer, device_id_type=MESH)

    for peer in peers:
        greet(peer)

    own = [pltpu.make_async_copy(src[m], buf[m].at[0], own_sem.at[m]) for m in (ACT, GRAD)]
    for copy in own:
        copy.start()
    pl.semaphore_wait(barrier, len(peers))

    def cols(i, first):
        m, offset, size, later = PIECES[i]
        start = (first + later) % 2 * (buf[m].shape[2] // 2) + offset
        return pl.ds(pl.multiple_of(start, 128), size)

    def remote(a, b, ss, rs, to):
        return pltpu.make_async_remote_copy(
            src_ref=a, dst_ref=b, send_sem=ss, recv_sem=rs, device_id=to, device_id_type=MESH
        )

    def along_a(i):
        m = PIECES[i][0]
        to = (1 - is_n) * (1 - odd)
        return remote(
            src[m].at[:, cols(i, to)], buf[m].at[1, :, cols(i, to)], a_send.at[m], a_recv.at[i], x1
        )

    def along_b(k, i):
        m = PIECES[i][0]
        part = cols(i, odd)
        source = src[m].at[:, part] if k == 0 else buf[m].at[1, :, part]
        return remote(source, buf[m].at[3 - k, :, part], b_send.at[k, m], b_recv.at[k, i], x3)

    def to_core(k, i):
        m = PIECES[i][0]
        part = cols(i, 0 if k < 2 else odd)
        source = src[m].at[:, part] if k == 0 else buf[m].at[k, :, part]
        slot = k + 4 if k < 2 else k
        return remote(source, buf[m].at[slot, :, part], d_send.at[k, m], d_recv.at[k, i], core)

    every = range(len(PIECES))
    for i in every:
        along_a(i).start()

    @pl.when(is_n == 1)
    def _():
        for i in AT_ONCE:
            along_b(0, i).start()

    @pl.when(is_n == 0)
    def _():
        for i in every:
            to_core(0, i).start()

    def step_a(m, half):
        for i in pieces_of(m, half):
            along_a(i).wait_recv()

            @pl.when(is_n == 1)
            def _(i=i):
                along_b(1, i).start()
                for j in AFTER.get(i, ()):
                    along_b(0, j).start()

            @pl.when(is_n == 0)
            def _(i=i):
                to_core(1, i).start()

        @pl.when(is_n == 1)
        def _():
            for i in pieces_of(m, half):
                to_core(0, i).wait_recv()
                to_core(1, i).wait_recv()

    def step_b(m, half):
        @pl.when(is_n == 0)
        def _():
            for i in pieces_of(m, half):
                along_b(0, i).wait_recv()
                to_core(3, i).start()
            for i in pieces_of(m, half):
                along_b(1, i).wait_recv()
                to_core(2, i).start()

        @pl.when(is_n == 1)
        def _():
            for i in pieces_of(m, half):
                to_core(3, i).wait_recv()
                to_core(2, i).wait_recv()

    zb = z // 2
    za = (z + zb) % 2
    yb = y // 2
    ya = (y + yb) % 2

    def weight(d, k):
        at_n, at_r = 2 ** ORDER_N[k].index(d), 2 ** ORDER_R[k].index(d)
        return at_r + is_n * (at_n - at_r)

    def stream_copy(m, k, q, to):
        return remote(
            prod[m].at[k, q], recv[m].at[k, q], s_send.at[m, k], s_recv.at[m, k, q], to
        )

    def lanes_of(m, k):
        tiles = buf[m].shape[2] // 256
        first = (tiles + 1) // 2 * 128
        return pl.ds(0, first) if k == 0 else pl.ds(first, tiles * 128 - first)

    def extra_copy(m, k, q, to):
        return remote(
            prox[m].at[q, :, lanes_of(m, k)],
            recx[m].at[q, :, lanes_of(m, k)],
            x_send.at[m, k],
            x_recv.at[m, q],
            to,
        )

    def dot(m, e, c, s):
        half = buf[m].shape[2] // 2
        tokens = 2 * buf[m].shape[1]
        base = e * 2 + (1 - e) * 4 * is_n
        left = buf[m][pl.ds(base, 2), :, pl.ds(pl.multiple_of(c * half, 128), half)]
        right = buf[m][pl.ds(0, 2), :, pl.ds(pl.multiple_of(s * half, 128), half)]
        return lax.dot_general(
            left.reshape(tokens, half),
            right.reshape(tokens, half),
            (((0,), (0,)), ((), ())),
            preferred_element_type=jnp.float32,
        )

    def bits_of(yy):
        return ((yy ^ (yy >> 1)) % 2 + ya) % 2, (yy // 2 + yb) % 2

    def product(m, e, order):
        c = (order + odd) % 2 if e else order
        s = (c + shift[e]) % 2
        value = dot(m, e, c, s)
        rows = value.shape[0] // 8
        block = (tc + e) % 2
        rza = (c + (place if e else 0) + block + za) % 2
        rzb = (block + zb) % 2
        for yy in range(4):
            rya, ryb = bits_of(yy)
            for k in range(2):
                q = rza * weight(2, k) + rzb * weight(3, k)
                q = q + rya * weight(0, k) + ryb * weight(1, k)
                first = (2 * yy + k) * rows
                prod[m][k, q] = value[first : first + rows].astype(jnp.bfloat16)

                @pl.when(q % 2 == 1)
                def _(k=k, q=q):
                    stream_copy(m, k, q, partner(k, 0)).start()

    EXTRA = ((y_a, y_b, z_a, z_b), (z_b, z_a, y_b, y_a))

    def product_extra(m):
        value = dot(m, 0, 0, 1)
        rows = value.shape[0] // 16
        for yy in range(4):
            rya, ryb = bits_of(yy)
            for zz in range(4):
                rza = ((zz ^ (zz >> 1)) % 2 + za) % 2
                rzb = (zz // 2 + zb) % 2
                first = (4 * yy + zz) * rows
                part = value[first : first + rows].astype(jnp.bfloat16)
                for k in range(2):
                    if k == 0:
                        q = rya + 2 * ryb + 4 * rza + 8 * rzb
                    else:
                        q = rzb + 2 * rza + 4 * ryb + 8 * rya
                    lanes = lanes_of(m, k)
                    prox[m][q, :, lanes] = part[:, lanes.start : lanes.start + lanes.size]

                    @pl.when(q % 2 == 1)
                    def _(k=k, q=q):
                        extra_copy(m, k, q, EXTRA[k][0]).start()

    def total(own_ref, got_ref, k, q, parts):
        value = own_ref[k, q].astype(jnp.float32)
        for p in parts:
            value = value + got_ref[k, p].astype(jnp.float32)
        return value

    early_0 = 1
    early_1 = 1 - is_n * h

    def group_of(k, q):
        def bit(d):
            at_n, at_r = 2 ** ORDER_N[k].index(d), 2 ** ORDER_R[k].index(d)
            return is_n * (q // at_n % 2) + (1 - is_n) * (q // at_r % 2)

        block = (bit(3) + zb) % 2
        c = (bit(2) + za + block) % 2
        e = (block + tc) % 2
        c = (c + e * place) % 2
        second = (c + odd) % 2
        return (1 - e) * c + e * (2 * second + (1 - second) * (1 - early_1))

    def stage(m, j, group=None):
        def move(k, q, parts):
            for p in parts:
                stream_copy(m, k, p, core).wait_recv()
            prod[m][k, q] = total(prod[m], recv[m], k, q, parts).astype(jnp.bfloat16)
            stream_copy(m, k, q, partner(k, j)).start()

        def one(i, carry):
            q = i * 2 ** (j + 1) + 2**j
            parts = [q + 2**b for b in range(j)]
            for k in range(2):
                if group is None:
                    move(k, q, parts)
                else:
                    pl.when(group_of(k, q) == group)(functools.partial(move, k, q, parts))
            return carry

        lax.fori_loop(0, 2 ** (3 - j), one, 0)

    def extra_arrived(m, parts):
        for p in parts:
            slot = recx[m].at[p]
            remote(slot, slot, x_send.at[m, 0], x_recv.at[m, p], core).wait_recv()

    def total_extra(m, k, q, parts):
        value = prox[m][q, :, lanes_of(m, k)].astype(jnp.float32)
        for p in parts:
            value = value + recx[m][p, :, lanes_of(m, k)].astype(jnp.float32)
        return value

    def stage_extra(m, j):
        def one(i, carry):
            q = i * 2 ** (j + 1) + 2**j
            parts = [q + 2**b for b in range(j)]
            extra_arrived(m, parts)
            for k in range(2):
                prox[m][q, :, lanes_of(m, k)] = total_extra(m, k, q, parts).astype(jnp.bfloat16)
                extra_copy(m, k, q, EXTRA[k][j]).start()
            return carry

        @pl.when(is_n == 0)
        def _():
            lax.fori_loop(0, 2 ** (3 - j), one, 0)

    def at(m, block, s):
        width = buf[m].shape[2]
        half = width // 2
        first = pl.multiple_of(block * width + s * half, 128)
        return pl.ds(first, half)

    def last_copy(m, k):
        _, _, _, a, b = (*others, x1)[k]
        to = (h, z + moved * (flip1(z) - z), y, a, b)
        return remote(
            fin[m].at[2 * to[3] + to[4]],
            row[m].at[:, at(m, 2 * tr + tc, side)],
            f_send.at[m],
            f_recv.at[m, k],
            to,
        )

    extra_to = (h, 2 * tc, y, half_z, c_mine)
    keeps = (1 - is_n) * (1 - apart) * (1 - c_mine) * (1 - tr) * (1 - tc)
    keeps_turned = (1 - is_n) * (1 - apart) * c_mine

    def last_extra(m):
        return remote(
            finx[m], row[m].at[:, at(m, 2 * tr + tc, 1)], g_send.at[m], g_recv.at[m], extra_to
        )

    def turned_extra(m, i):
        to = (h, 2 * tc + 1, i // 4, i // 2 % 2, i % 2)
        return remote(
            turx[m].at[i], mirx[m].at[4 * y + z], n_send.at[m], n_recv.at[m], to
        )

    def is_self(i):
        return keeps_turned * (i == 4 * y + 2 * tr + tc).astype(jnp.int32)

    def turned_copy(m, i, to):
        return remote(
            turn[m].at[i], mir[m].at[kind, y], m_send.at[m], m_recv.at[m, kind], to
        )

    def by_quarter(m, ref, value):
        rows = value.shape[0] // 4
        for i in range(4):
            ref[m][i] = value[i * rows : (i + 1) * rows].astype(jnp.bfloat16)

    def finish(m):
        parts = (1, 2, 4, 8)
        for k in range(2):
            for p in parts:
                stream_copy(m, k, p, core).wait_recv()
        value = jnp.concatenate(
            [total(prod[m], recv[m], k, 0, parts) for k in range(2)], axis=0
        )
        by_quarter(m, fin, value)
        for k in range(3):
            last_copy(m, k).start()

        @pl.when(moved == 1)
        def _():
            last_copy(m, 3).start()

        @pl.when(moved == 0)
        def _():
            row[m][:, at(m, 2 * tr + tc, side)] = fin[m][2 * tr + tc]

        @pl.when(mirrors == 1)
        def _():
            lanes = turn[m].shape[2]
            tall = value
            if lanes != value.shape[0]:
                fill = jnp.zeros((lanes - value.shape[0], value.shape[1]), jnp.float32)
                tall = jnp.concatenate([value, fill], axis=0)
            turned = tall.T
            rows = turned.shape[0] // 16
            for i, to in quarters():
                turn[m][i] = turned[i * rows : (i + 1) * rows].astype(jnp.bfloat16)

    def send_turned(m):
        @pl.when(mirrors == 1)
        def _():
            for i, to in quarters():
                turned_copy(m, i, to).start()

    def finish_extra(m):
        @pl.when(is_n == 0)
        def _():
            extra_arrived(m, (1, 2, 4, 8))
            value = jnp.concatenate(
                [total_extra(m, k, 0, (1, 2, 4, 8)) for k in range(2)], axis=1
            )
            finx[m][...] = value.astype(jnp.bfloat16)

            @pl.when(keeps == 0)
            def _():
                last_extra(m).start()

            @pl.when(keeps == 1)
            def _():
                row[m][:, at(m, 2 * tr + tc, 1)] = finx[m][...]

            rows = value.shape[0]
            fill = jnp.zeros((128 - rows, value.shape[1]), jnp.float32)
            turned = jnp.concatenate([value, fill], axis=0).T
            for i in range(16):
                turx[m][i] = turned[i * rows : (i + 1) * rows].astype(jnp.bfloat16)

                @pl.when(is_self(i) == 0)
                def _(i=i):
                    turned_extra(m, i).start()

                @pl.when(is_self(i) == 1)
                def _(i=i):
                    mirx[m][4 * y + z] = turx[m][i]

    def gather_rows(m):
        width = buf[m].shape[2]
        rows = width // 8
        for t in range(3):
            pieces = mir[m].at[t]
            remote(pieces, pieces, m_send.at[m], m_recv.at[m, t], core).wait_recv()
            value = jnp.concatenate(
                [mir[m][t, yy].astype(jnp.float32)[:, :rows] for yy in range(4)], axis=1
            )
            chunk = turned_rows[t]
            row[m][:, at(m, chunk // 2, chunk % 2)] = value.astype(jnp.bfloat16)
        for k in range(3):
            last_copy(m, k).wait_recv()

        @pl.when(moved == 1)
        def _():
            last_copy(m, 3).wait_recv()

        @pl.when(c_mine * (1 - keeps) + (1 - c_mine) * keeps == 0)
        def _():
            last_extra(m).wait_recv()

        @pl.when(c_mine == 1)
        def _():
            rows = width // 32
            for count in (15, 16):

                @pl.when(keeps_turned == 16 - count)
                def _(count=count):
                    pieces = mirx[m].at[pl.ds(0, count)]
                    remote(pieces, pieces, n_send.at[m], n_recv.at[m], core).wait_recv()

            value = jnp.concatenate(
                [mirx[m][i].astype(jnp.float32)[:, :rows] for i in range(16)], axis=1
            )
            row[m][:, at(m, 2 * h + half_z, 0)] = value.astype(jnp.bfloat16)

        own_out(m).start()

    def own_out(m):
        return pltpu.make_async_copy(row[m], out[m], o_sem.at[m])

    def products(m, e, first, last):
        def one(c, carry):
            product(m, e, c)
            return carry

        lax.fori_loop(first, last, one, 0)

    def extras(m):
        @pl.when(is_n == 0)
        def _():
            product_extra(m)

    for copy in own:
        copy.wait()
    step_a(GRAD, 0)
    products(GRAD, 0, 0, early_0)
    step_b(GRAD, 0)
    products(GRAD, 1, 0, early_1)
    step_a(GRAD, 1)
    products(GRAD, 0, early_0, 2)
    products(GRAD, 1, early_1, 1)
    extras(GRAD)
    stage(GRAD, 1, 0)
    step_b(GRAD, 1)
    products(GRAD, 1, 1, 2)
    step_a(ACT, 0)
    products(ACT, 0, 0, 1)
    stage(GRAD, 1, 1)
    stage_extra(GRAD, 1)
    step_a(ACT, 1)
    products(ACT, 0, 1, 2)
    extras(ACT)
    stage(GRAD, 1, 2)
    step_b(ACT, 0)
    step_b(ACT, 1)
    products(ACT, 1, 0, 2)
    stage(GRAD, 2)
    stage_extra(GRAD, 2)
    stage(ACT, 1)
    stage_extra(ACT, 1)
    stage(GRAD, 3)
    stage_extra(GRAD, 3)
    stage(ACT, 2)
    finish(GRAD)
    send_turned(GRAD)
    stage_extra(ACT, 2)
    stage(ACT, 3)
    stage_extra(ACT, 3)
    finish_extra(GRAD)
    finish(ACT)
    send_turned(ACT)
    finish_extra(ACT)
    gather_rows(GRAD)
    gather_rows(ACT)

    def sent(ref, sem):
        pltpu.make_async_copy(ref, ref, sem).wait()

    for m in (ACT, GRAD):
        block = buf[m].at[1]
        sent(block, a_send.at[m])

        @pl.when(is_n == 1)
        def _(m=m, block=block):
            for k in (0, 1):
                sent(block, b_send.at[k, m])

        @pl.when(is_n == 0)
        def _(m=m, block=block):
            for k in range(4):
                sent(block, d_send.at[k, m])
            for k in range(2):
                sent(prox[m].at[pl.ds(1, 15), :, lanes_of(m, k)], x_send.at[m, k])

            @pl.when(keeps == 0)
            def _():
                last_extra(m).wait_send()

            for count in (15, 16):

                @pl.when(keeps_turned == 16 - count)
                def _(count=count):
                    sent(turx[m].at[pl.ds(0, count)], n_send.at[m])

        for k in range(2):
            sent(prod[m].at[k, pl.ds(1, 15)], s_send.at[m, k])
        for count in (3, 4):

            @pl.when(moved == count - 3)
            def _(m=m, count=count):
                sent(fin[m].at[pl.ds(0, count)], f_send.at[m])


        @pl.when(mirrors == 1)
        def _(m=m):
            sent(turn[m], m_send.at[m])

        own_out(m).wait()


def sums(activations, gradients, rows_a, rows_g):
    tokens = activations.shape[0]
    wide = (activations.shape[1], gradients.shape[1])
    rows = (rows_a, rows_g)
    bf16 = jnp.bfloat16
    lanes = [-(-w // 1024) * 128 for w in wide]
    vmem = [
        *(pltpu.VMEM((6, tokens, w), bf16) for w in wide),
        *(pltpu.VMEM((2, 16, w // 16, w // 2), bf16) for w in wide),
        *(pltpu.VMEM((2, 16, w // 16, w // 2), bf16) for w in wide),
        *(pltpu.VMEM((16, r, w // 2), bf16) for r, w in zip(rows, wide)),
        *(pltpu.VMEM((16, r, w // 2), bf16) for r, w in zip(rows, wide)),
        *(pltpu.VMEM((4, r, w // 2), bf16) for r, w in zip(rows, wide)),
        *(pltpu.VMEM((r, w // 2), bf16) for r, w in zip(rows, wide)),
        *(pltpu.VMEM((16, r, n), bf16) for r, n in zip(rows, lanes)),
        *(pltpu.VMEM((16, r, 128), bf16) for r in rows),
        *(pltpu.VMEM((3, 4, r, n), bf16) for r, n in zip(rows, lanes)),
        *(pltpu.VMEM((16, r, 128), bf16) for r in rows),
        *(pltpu.VMEM((r, 4 * w), bf16) for r, w in zip(rows, wide)),
    ]
    n = len(PIECES)
    dma = pltpu.SemaphoreType.DMA
    sems = [
        dma((2,)), dma((2,)), dma((n,)), dma((2, 2)), dma((2, n)), dma((4, 2)), dma((4, n)),
        dma((2, 2)), dma((2, 2, 16)), dma((2, 2)), dma((2, 16)),
        dma((2,)), dma((2, 4)), dma((2,)), dma((2,)),
        dma((2,)), dma((2, 3)), dma((2,)), dma((2,)), dma((2,)),
    ]
    anywhere = pl.BlockSpec(memory_space=pl.ANY)
    return pl.pallas_call(
        kernel,
        out_shape=[jax.ShapeDtypeStruct((r, 4 * w), bf16) for r, w in zip(rows, wide)],
        in_specs=[pl.BlockSpec(memory_space=pltpu.HBM)] * 2,
        out_specs=[anywhere] * 2,
        scratch_shapes=[*vmem, *sems],
        compiler_params=pltpu.CompilerParams(
            collective_id=0, has_side_effects=True, vmem_limit_bytes=54_800_000
        ),
    )(activations, gradients)


def body(activations, gradients, old_inputs, old_gradients):
    tokens_all = activations.shape[0] * lax.axis_size(DP)
    sum_a, sum_g = sums(activations, gradients, old_inputs.shape[0], old_gradients.shape[0])
    scale = 0.5 / tokens_all
    return (
        0.5 * old_inputs + scale * sum_a.astype(jnp.float32),
        0.5 * old_gradients + scale * sum_g.astype(jnp.float32),
    )


def solution(mesh):
    finer = Mesh(mesh.devices.reshape(2, 4, 4, mesh.shape["tr"], mesh.shape["tc"]), AXES)
    return jax.shard_map(
        body,
        mesh=finer,
        in_specs=(P(DP, ("tr", "tc")), P(DP, ("tr", "tc")), P(DP_TR_TC, None), P(DP_TR_TC, None)),
        out_specs=(P(DP_TR_TC, None), P(DP_TR_TC, None)),
        check_vma=False,
    )
```
